32 devices in a mesh: dp: 2 (over x), tp: 4 (over z), cp: 4 (over y, core).
Axes of the slice: x: 2, y: 2, z: 4, core: 2. Of those that a mesh axis runs over, the one named last changes fastest.
Arguments:
- x_in: bfloat16 [16384, 4096], P(('dp', 'cp')), parts along dimension 0
- positions: int32 [16384], P(('dp', 'cp')), parts along dimension 0
- norm_gain: bfloat16 [4096], replicated
- w_q: bfloat16 [4096, 4096], P(None, 'tp')
- w_k: bfloat16 [4096, 1024], P(None, 'tp')
- w_v: bfloat16 [4096, 1024], P(None, 'tp')
- w_o: bfloat16 [4096, 4096], P('tp')
Outputs:
- output 1: bfloat16 [16384, 4096], P(('dp', 'cp')), parts along dimension 0
- output 2: bfloat16 [16384, 8, 128], P(('dp', 'cp'), 'tp'), parts along dimension 0
- output 3: bfloat16 [16384, 8, 128], P(('dp', 'cp'), 'tp'), parts along dimension 0
There are 2 independent parts. The reference program is written for one: setup_inputs(seed, part) draws one part's arguments, and reference() takes and returns one part's arrays. A program takes and returns all parts, laid end to end along the dimension named above; an argument that names none is the same for every part.
All inputs are finite; a program needn't handle non-finite values.
Results may differ from the reference program's by a relative error of at most 0.00580332.
Values are sent between devices in bfloat16 or wider.
A program may use at most 1 GiB of HBM per device.

```python
import math
import jax
import jax.numpy as jnp
from jax import lax

MODEL_DIM = 4096
Q_HEADS = 32
KV_HEADS = 8
HEAD_DIM = 128
SEQ_LEN = 8192
CP_SIZE = 4


def rope_freqs():
    exponent = jnp.arange(0, HEAD_DIM, 2).astype(jnp.float32) / HEAD_DIM
    base_freq = 1.0 / (500000.0 ** exponent)
    wave_len = 2.0 * math.pi / base_freq
    smooth = (8192.0 / wave_len - 1.0) / 3.0
    blended = (1.0 - smooth) * base_freq / 8.0 + smooth * base_freq
    return jnp.where(wave_len < 2048.0, base_freq, jnp.where(wave_len > 8192.0, base_freq / 8.0, blended))


def apply_rope(vecs, positions, freqs):
    half_dim = HEAD_DIM // 2
    angles = positions.astype(jnp.float32)[:, None] * freqs[None, :]
    cosine = jnp.cos(angles)[:, None, :]
    sine_val = jnp.sin(angles)[:, None, :]
    vec_f32 = vecs.astype(jnp.float32)
    first_half = vec_f32[..., :half_dim]
    second_half = vec_f32[..., half_dim:]
    return jnp.concatenate([first_half * cosine - second_half * sine_val, second_half * cosine + first_half * sine_val], axis=-1).astype(jnp.bfloat16)


def setup_inputs(seed: int = 0, part: int = 0) -> dict:
    base_key = jax.random.key(seed)
    part_key = jax.random.fold_in(base_key, part)
    key_off, key_mean, key_noise = jax.random.split(part_key, 3)
    key_gain, key_q, key_k, key_v, key_o = jax.random.split(base_key, 5)
    seg_len = SEQ_LEN // (2 * CP_SIZE)
    dev_ids = jnp.arange(CP_SIZE)[:, None]
    seg_ids = jnp.concatenate([dev_ids, 2 * CP_SIZE - 1 - dev_ids], axis=1).reshape(2 * CP_SIZE)
    glob_idx = (seg_ids[:, None] * seg_len + jnp.arange(seg_len)[None, :]).reshape(SEQ_LEN)
    offset = jax.random.randint(key_off, (), 0, 4096)
    positions = (glob_idx + offset).astype(jnp.int32)
    seg_means = jax.random.normal(key_mean, (2 * CP_SIZE, MODEL_DIM), jnp.float32)
    row_means = jnp.repeat(seg_means[seg_ids], seg_len, axis=0)
    tok_noise = jax.random.normal(key_noise, (SEQ_LEN, MODEL_DIM), jnp.float32)
    x_in = (0.5 * (row_means + 0.5 * tok_noise)).astype(jnp.bfloat16)
    norm_gain = (1.0 + 0.3 * jax.random.normal(key_gain, (MODEL_DIM,), jnp.float32)).astype(jnp.bfloat16)
    in_scale = 1.0 / math.sqrt(MODEL_DIM)
    w_q = (jax.random.normal(key_q, (MODEL_DIM, Q_HEADS * HEAD_DIM), jnp.float32) * (2.0 * in_scale)).astype(jnp.bfloat16)
    w_k = (jax.random.normal(key_k, (MODEL_DIM, KV_HEADS * HEAD_DIM), jnp.float32) * in_scale).astype(jnp.bfloat16)
    w_v = (jax.random.normal(key_v, (MODEL_DIM, KV_HEADS * HEAD_DIM), jnp.float32) * in_scale).astype(jnp.bfloat16)
    w_o = (jax.random.normal(key_o, (Q_HEADS * HEAD_DIM, MODEL_DIM), jnp.float32) * (2.0 / math.sqrt(Q_HEADS * HEAD_DIM))).astype(jnp.bfloat16)
    return dict(x_in=x_in, positions=positions, norm_gain=norm_gain, w_q=w_q, w_k=w_k, w_v=w_v, w_o=w_o)


def reference(x_in, positions, norm_gain, w_q, w_k, w_v, w_o):
    seq_rows = x_in.shape[0]
    group_size = Q_HEADS // KV_HEADS
    x_f32 = x_in.astype(jnp.float32)
    normed = x_f32 * lax.rsqrt(jnp.mean(x_f32 * x_f32, axis=-1, keepdims=True) + 1e-5)
    hidden = (normed * norm_gain.astype(jnp.float32)[None, :]).astype(jnp.bfloat16)
    freqs = rope_freqs()
    queries = jnp.dot(hidden, w_q, preferred_element_type=jnp.float32).astype(jnp.bfloat16).reshape(seq_rows, Q_HEADS, HEAD_DIM)
    keys = jnp.dot(hidden, w_k, preferred_element_type=jnp.float32).astype(jnp.bfloat16).reshape(seq_rows, KV_HEADS, HEAD_DIM)
    values = jnp.dot(hidden, w_v, preferred_element_type=jnp.float32).astype(jnp.bfloat16).reshape(seq_rows, KV_HEADS, HEAD_DIM)
    queries = apply_rope(queries, positions, freqs)
    keys = apply_rope(keys, positions, freqs)
    q_blk = seq_rows
    while q_blk % 2 == 0 and q_blk > 8 and q_blk * seq_rows * Q_HEADS > 2 ** 24:
        q_blk = q_blk // 2
    n_blocks = seq_rows // q_blk
    q_grouped = queries.reshape(n_blocks, q_blk, KV_HEADS, group_size, HEAD_DIM)
    q_pos = positions.reshape(n_blocks, q_blk)
    keys_f32 = keys.astype(jnp.float32)
    values_f32 = values.astype(jnp.float32)
    score_scale = 1.0 / math.sqrt(HEAD_DIM)

    def attend(block):
        q_part, pos_part = block
        scores = jnp.einsum('qhgd,thd->qhgt', q_part.astype(jnp.float32), keys_f32) * score_scale
        keep_mask = positions[None, None, None, :] <= pos_part[:, None, None, None]
        scores = jnp.where(keep_mask, scores, -jnp.inf)
        prob_bf = jax.nn.softmax(scores, axis=-1).astype(jnp.bfloat16)
        attn_out = jnp.einsum('qhgt,thd->qhgd', prob_bf.astype(jnp.float32), values_f32)
        return attn_out.astype(jnp.bfloat16)

    o_blocks = lax.map(attend, (q_grouped, q_pos))
    attn = o_blocks.reshape(seq_rows, Q_HEADS * HEAD_DIM)
    y_out = (x_f32 + jnp.dot(attn, w_o, preferred_element_type=jnp.float32)).astype(jnp.bfloat16)
    return y_out, keys, values
```

```python
import math
import jax
import jax.numpy as jnp
from jax import lax
from jax.experimental import pallas as pl
from jax.experimental.pallas import tpu as pltpu
from jax.sharding import PartitionSpec as P

HEAD_DIM = 128
NORM_EPS = 1e-5
NEG = -0.7 * float(jnp.finfo(jnp.float32).max)
SCALE2 = (1.0 / math.sqrt(HEAD_DIM)) * math.log2(math.e)
BF16 = jnp.bfloat16
F32 = jnp.float32
VMEM_LIMIT = 56 * 2 ** 20


def rope_freqs():
    exponent = jnp.arange(0, HEAD_DIM, 2).astype(jnp.float32) / HEAD_DIM
    base_freq = 1.0 / (500000.0 ** exponent)
    wave_len = 2.0 * math.pi / base_freq
    smooth = (8192.0 / wave_len - 1.0) / 3.0
    blended = (1.0 - smooth) * base_freq / 8.0 + smooth * base_freq
    return jnp.where(wave_len < 2048.0, base_freq, jnp.where(wave_len > 8192.0, base_freq / 8.0, blended))


def rotate(vec_bf, cos, sin):
    vec = vec_bf.astype(F32)
    return (vec * cos + pltpu.roll(vec, HEAD_DIM // 2, axis=1) * sin).astype(BF16)


def norm_kv(x, gain, w_k, w_v, cos, sin, half, rows):
    width = x.shape[1]
    kv_width = w_k.shape[1]
    blk = 256
    base = half * rows // blk

    def kernel(x_ref, g_ref, wk_ref, wv_ref, c_ref, s_ref, h_ref, k_ref, v_ref, vt_ref):
        xf = x_ref[...].astype(F32)
        inv = lax.rsqrt(jnp.mean(xf * xf, axis=-1, keepdims=True) + NORM_EPS)
        h_ref[...] = ((xf * inv) * g_ref[...].astype(F32)).astype(BF16)
        h = h_ref[...]
        k = jnp.dot(h, wk_ref[...], preferred_element_type=F32).astype(BF16)
        cos, sin = c_ref[...], s_ref[...]
        for j in range(kv_width // HEAD_DIM):
            cols = slice(j * HEAD_DIM, (j + 1) * HEAD_DIM)
            k_ref[:, cols] = rotate(k[:, cols], cos, sin)
        v = jnp.dot(h, wv_ref[...], preferred_element_type=F32).astype(BF16)
        v_ref[...] = v
        vt_ref[...] = v.T

    row_blk = lambda i: (base + i, 0)
    full = lambda i: (0, 0)
    return pl.pallas_call(
        kernel,
        grid=(rows // blk,),
        in_specs=[
            pl.BlockSpec((blk, width), row_blk),
            pl.BlockSpec((1, width), full),
            pl.BlockSpec((width, kv_width), full),
            pl.BlockSpec((width, kv_width), full),
            pl.BlockSpec((blk, HEAD_DIM), row_blk),
            pl.BlockSpec((blk, HEAD_DIM), row_blk),
        ],
        out_specs=[
            pl.BlockSpec((blk, width), lambda i: (i, 0)),
            pl.BlockSpec((blk, kv_width), lambda i: (i, 0)),
            pl.BlockSpec((blk, kv_width), lambda i: (i, 0)),
            pl.BlockSpec((kv_width, blk), lambda i: (0, i)),
        ],
        out_shape=[
            jax.ShapeDtypeStruct((rows, width), BF16),
            jax.ShapeDtypeStruct((rows, kv_width), BF16),
            jax.ShapeDtypeStruct((rows, kv_width), BF16),
            jax.ShapeDtypeStruct((kv_width, rows), BF16),
        ],
        compiler_params=pltpu.CompilerParams(vmem_limit_bytes=40 * 2 ** 20),
        cost_estimate=pl.CostEstimate(flops=2 * rows * width * 2 * kv_width, bytes_accessed=4 * rows * width, transcendentals=0),
        name="norm_kv",
    )(x, gain, w_k, w_v, cos, sin)


def project_q(h, w_q, cos, sin, half):
    rows, width = h.shape
    q_width = w_q.shape[1]
    blk = 256
    base = half * rows // blk

    def kernel(h_ref, w_ref, c_ref, s_ref, q_ref):
        q = jnp.dot(h_ref[...], w_ref[...], preferred_element_type=F32).astype(BF16)
        cos, sin = c_ref[...], s_ref[...]
        for j in range(q_width // HEAD_DIM):
            cols = slice(j * HEAD_DIM, (j + 1) * HEAD_DIM)
            q_ref[:, cols] = rotate(q[:, cols], cos, sin)

    full = lambda i: (0, 0)
    return pl.pallas_call(
        kernel,
        grid=(rows // blk,),
        in_specs=[
            pl.BlockSpec((blk, width), lambda i: (i, 0)),
            pl.BlockSpec((width, q_width), full),
            pl.BlockSpec((blk, HEAD_DIM), lambda i: (base + i, 0)),
            pl.BlockSpec((blk, HEAD_DIM), lambda i: (base + i, 0)),
        ],
        out_specs=pl.BlockSpec((blk, q_width), lambda i: (i, 0)),
        out_shape=jax.ShapeDtypeStruct((rows, q_width), BF16),
        compiler_params=pltpu.CompilerParams(vmem_limit_bytes=40 * 2 ** 20),
        cost_estimate=pl.CostEstimate(flops=2 * rows * width * q_width, bytes_accessed=2 * rows * width, transcendentals=0),
        name="project_q",
    )(h, w_q, cos, sin)


def attend(q, k_lo, vt_lo, k_hi, vt_hi, row0, n_rows, hi, kv_heads, group):
    n_cp, seg = k_lo.shape[0], k_lo.shape[1]
    blk_q = 128 if n_rows % 512 else 256
    blk_k = 512
    cols = blk_q * group
    n_sub = n_rows // (2 * blk_q)
    n_seg = 2 * n_cp if hi else n_cp
    d = HEAD_DIM

    def kernel(q_ref, *refs):
        kv_refs = refs[:4 if hi else 2]
        o_ref, kb, vb, qt, s_a, s_b, acc_a, acc_b, m_run, l_run, m_tile, sem = refs[len(kv_refs):]
        cp = lax.axis_index("cp")
        head, sub = pl.program_id(0), pl.program_id(1)

        def copies(h):
            out = []
            for i in range(n_cp):
                pairs = [(kv_refs[0], kv_refs[1], i)]
                if hi:
                    pairs.append((kv_refs[2], kv_refs[3], n_seg - 1 - i))
                for k_src, v_src, s in pairs:
                    part = k_src.at[i, :, pl.ds(h * d, d)]
                    out.append(pltpu.make_async_copy(part, kb.at[h, pl.ds(s * seg, seg), pl.ds(0, d)], sem.at[h]))
                    out.append(pltpu.make_async_copy(part, kb.at[h, pl.ds(s * seg, seg), pl.ds(d, d)], sem.at[h]))
                    out.append(pltpu.make_async_copy(v_src.at[i, pl.ds(h * d, d), :], vb.at[h, :, pl.ds(s * seg, seg)], sem.at[h]))
            return out

        for h in range(kv_heads):
            @pl.when((head == 0) & (sub == 0))
            def _():
                for c in copies(h):
                    c.start()
        for h in range(kv_heads):
            @pl.when((head == h) & (sub == 0))
            def _():
                for c in copies(h):
                    c.wait()

        r0 = row0 + sub * 2 * blk_q
        g0 = ((2 * n_cp - 1 - cp) if hi else cp) * seg + r0
        for st in range(2):
            for j in range(group):
                qs = q_ref[st * blk_q:(st + 1) * blk_q, j * d:(j + 1) * d].T.astype(F32) * SCALE2
                top = qs.astype(BF16)
                span = slice(j * blk_q, (j + 1) * blk_q)
                qt[st, 0:d, span] = top
                qt[st, d:2 * d, span] = (qs - top.astype(F32)).astype(BF16)
        scores = (s_a, s_b)
        accs = (acc_a, acc_b)
        k_idx = lax.broadcasted_iota(jnp.int32, (blk_k, cols), 0)
        q_idx = lax.broadcasted_iota(jnp.int32, (blk_k, cols), 1) % blk_q

        def qk(st, t, mask=None):
            s = jnp.dot(kb[head, pl.ds(pl.multiple_of(t * blk_k, blk_k), blk_k), :], qt[st], preferred_element_type=F32)
            if mask is not None:
                s = jnp.where(mask, s, NEG)
            scores[st][...] = s
            m_tile[st] = jnp.max(s, axis=0, keepdims=True)

        def soft(st, t):
            m_old = m_run[st]
            m_new = jnp.maximum(m_old, m_tile[st])
            m_run[st] = m_new
            alpha = jnp.exp2(m_old - m_new)
            p = jnp.exp2(scores[st][...] - m_new)
            l_run[st] = l_run[st] * alpha + jnp.sum(p, axis=0, keepdims=True)
            pv = jnp.dot(vb[head, :, pl.ds(pl.multiple_of(t * blk_k, blk_k), blk_k)], p.astype(BF16), preferred_element_type=F32)
            accs[st][...] = accs[st][...] * alpha + pv

        m_run[...] = jnp.full_like(m_run, NEG)
        l_run[...] = jnp.zeros_like(l_run)
        acc_a[...] = jnp.zeros_like(acc_a)
        acc_b[...] = jnp.zeros_like(acc_b)
        n_full = g0 // blk_k
        off = g0 - n_full * blk_k

        @pl.when(n_full > 0)
        def _():
            qk(0, 0)

        @pl.when(n_full == 0)
        def _():
            qk(0, 0, k_idx <= q_idx + off)

        def body(t, carry):
            qk(1, t)
            soft(0, t)
            qk(0, t + 1)
            soft(1, t)
            return carry

        lax.fori_loop(0, n_full - 1, body, 0)

        @pl.when(n_full > 0)
        def _():
            qk(1, n_full - 1)
            soft(0, n_full - 1)
            qk(0, n_full, k_idx <= q_idx + off)
            soft(1, n_full - 1)

        qk(1, n_full, k_idx <= q_idx + (off + blk_q))
        soft(0, n_full)
        soft(1, n_full)
        for st in range(2):
            o = accs[st][...] * (1.0 / l_run[st])
            for j in range(group):
                o_ref[st * blk_q:(st + 1) * blk_q, j * d:(j + 1) * d] = o[:, j * blk_q:(j + 1) * blk_q].T.astype(BF16)

    any_spec = pl.BlockSpec(memory_space=pl.ANY)
    kv = (k_lo, vt_lo, k_hi, vt_hi) if hi else (k_lo, vt_lo)
    blk0 = row0 // (2 * blk_q)
    pairs = n_rows * group * kv_heads * (6 if hi else 3) * seg
    return pl.pallas_call(
        kernel,
        grid=(kv_heads, n_sub),
        in_specs=[pl.BlockSpec((2 * blk_q, group * d), lambda h, s: (blk0 + s, h))] + [any_spec] * len(kv),
        out_specs=pl.BlockSpec((2 * blk_q, group * d), lambda h, s: (s, h)),
        out_shape=jax.ShapeDtypeStruct((n_rows, kv_heads * group * d), BF16),
        scratch_shapes=[
            pltpu.VMEM((kv_heads, n_seg * seg, 2 * d), BF16),
            pltpu.VMEM((kv_heads, d, n_seg * seg), BF16),
            pltpu.VMEM((2, 2 * d, cols), BF16),
            pltpu.VMEM((blk_k, cols), F32),
            pltpu.VMEM((blk_k, cols), F32),
            pltpu.VMEM((d, cols), F32),
            pltpu.VMEM((d, cols), F32),
            pltpu.VMEM((2, 1, cols), F32),
            pltpu.VMEM((2, 1, cols), F32),
            pltpu.VMEM((2, 1, cols), F32),
            pltpu.SemaphoreType.DMA((kv_heads,)),
        ],
        compiler_params=pltpu.CompilerParams(dimension_semantics=("arbitrary", "arbitrary"), vmem_limit_bytes=VMEM_LIMIT),
        cost_estimate=pl.CostEstimate(flops=4 * pairs * d, bytes_accessed=8 * 2 ** 20, transcendentals=pairs),
        name="attend_hi" if hi else "attend_lo",
    )(q, *kv)


def gather_w_o(w_o, n_dp, n_tp, n_cp):
    place = lax.axis_index("dp") * n_cp + lax.axis_index("cp")
    rows = w_o.shape[0] // (n_dp * n_cp)
    own = lax.dynamic_slice_in_dim(w_o, place * rows, rows, axis=0)
    swaps = {
        "x": lambda a: lax.ppermute(a, "dp", [(i, 1 - i) for i in range(2)]),
        "y": lambda a: lax.ppermute(a, "cp", [(i, i ^ 2) for i in range(4)]),
        "c": lambda a: lax.ppermute(a, "cp", [(i, i ^ 1) for i in range(4)]),
    }
    blocks = []
    for dz in range(n_tp):
        a = own if dz == 0 else lax.ppermute(own, "tp", [(i, (i + dz) % n_tp) for i in range(n_tp)])
        held = {(0, 0, 0): a}
        for axis in ("xyc" if dz % 2 == 0 else "yxc"):
            pos = "xyc".index(axis)
            for key, val in list(held.items()):
                new = tuple(1 if i == pos else k for i, k in enumerate(key))
                held[new] = swaps[axis](val)
        blocks += [held[(i >> 2, (i >> 1) & 1, i & 1)] for i in range(8)]
    return jnp.concatenate(blocks, axis=0)


def project_out(o_all, w_all, x, y_prev, row0):
    n_tp, rows, width = o_all.shape
    out_width = w_all.shape[1]
    n_heads = width // HEAD_DIM
    tile = 512
    blk0 = row0 // rows
    d = HEAD_DIM

    def kernel(o_ref, w_ref, x_ref, *refs):
        y_ref, o_rel = refs[-2:]

        @pl.when(pl.program_id(0) == 0)
        def _():
            t = lax.axis_index("tp")
            dp, cp = lax.axis_index("dp"), lax.axis_index("cp")
            for dz in range(n_tp):
                z = lax.rem(t + n_tp - dz, n_tp)
                for dj in range(n_heads):
                    dx, dy, dc = dj >> 2, (dj >> 1) & 1, dj & 1
                    px = 1 - dp if dx else dp
                    py = 1 - cp // 2 if dy else cp // 2
                    pc = 1 - cp % 2 if dc else cp % 2
                    j = px * 4 + py * 2 + pc
                    at = (dz * n_heads + dj) * d
                    o_rel[:, at:at + d] = o_ref[z, :, pl.ds(pl.multiple_of(j * d, d), d)]

        acc = jnp.dot(o_rel[...], w_ref[...], preferred_element_type=F32)
        y_ref[...] = (x_ref[...].astype(F32) + acc).astype(BF16)

    extra = [] if y_prev is None else [y_prev]
    return pl.pallas_call(
        kernel,
        grid=(out_width // tile,),
        in_specs=[
            pl.BlockSpec((n_tp, rows, width), lambda n: (0, 0, 0)),
            pl.BlockSpec((n_tp * width, tile), lambda n: (0, n)),
            pl.BlockSpec((rows, tile), lambda n: (blk0, n)),
        ] + [pl.BlockSpec(memory_space=pl.ANY)] * len(extra),
        out_specs=pl.BlockSpec((rows, tile), lambda n: (blk0, n)),
        out_shape=jax.ShapeDtypeStruct(x.shape, BF16),
        scratch_shapes=[pltpu.VMEM((rows, n_tp * width), BF16)],
        input_output_aliases={} if y_prev is None else {3: 0},
        compiler_params=pltpu.CompilerParams(vmem_limit_bytes=VMEM_LIMIT),
        cost_estimate=pl.CostEstimate(flops=2 * rows * n_tp * width * out_width, bytes_accessed=2 * n_tp * width * out_width, transcendentals=0),
        name="project_out",
    )(o_all, w_all, x, *extra)


def solution(mesh):
    n_dp, n_tp, n_cp = mesh.shape['dp'], mesh.shape['tp'], mesh.shape['cp']

    def device_fn(x_in, positions, norm_gain, w_q, w_k, w_v, w_o):
        local_rows = x_in.shape[0]
        seg = local_rows // 2
        kv_heads = w_k.shape[1] // HEAD_DIM
        group = w_q.shape[1] // w_k.shape[1]
        angles = positions.astype(F32)[:, None] * rope_freqs()[None, :]
        cos, sin = jnp.cos(angles), jnp.sin(angles)
        cos = jnp.concatenate([cos, cos], axis=1)
        sin = jnp.concatenate([-sin, sin], axis=1)
        gain = norm_gain[None, :]
        w_all = gather_w_o(w_o, n_dp, n_tp, n_cp)

        h, k, v, kg, vg, q = ([None, None] for _ in range(6))
        for half in range(2):
            h[half], k[half], v[half], vt = norm_kv(x_in, gain, w_k, w_v, cos, sin, half, seg)
            kg[half] = lax.all_gather(k[half], 'cp', axis=0)
            vg[half] = lax.all_gather(vt, 'cp', axis=0)
        for half in range(2):
            q[half] = project_q(h[half], w_q, cos, sin, half)

        rows = 256
        o_all = []
        for half in range(2):
            for row0 in range(0, seg, rows):
                o = attend(q[half], kg[0], vg[0], kg[1], vg[1], row0, rows, half == 1, kv_heads, group)
                o_all.append(lax.all_gather(o, 'tp', axis=0))
        y = None
        for i, o in enumerate(o_all):
            y = project_out(o, w_all, x_in, y, i * rows)
        keys = jnp.concatenate(k, axis=0).reshape(local_rows, kv_heads, HEAD_DIM)
        values = jnp.concatenate(v, axis=0).reshape(local_rows, kv_heads, HEAD_DIM)
        return y, keys, values

    row_spec = P(('dp', 'cp'), None)
    cache_spec = P(('dp', 'cp'), 'tp', None)
    return jax.shard_map(device_fn, mesh=mesh, in_specs=(row_spec, P(('dp', 'cp')), P(None), P(None, 'tp'), P(None, 'tp'), P(None, 'tp'), P('tp', None)), out_specs=(row_spec, cache_spec, cache_spec), check_vma=False)
```

```python
import math
import jax
import jax.numpy as jnp
from jax import lax
from jax.experimental import pallas as pl
from jax.experimental.pallas import tpu as pltpu
from jax.sharding import PartitionSpec as P

HEAD_DIM = 128
NORM_EPS = 1e-5
NEG = -0.7 * float(jnp.finfo(jnp.float32).max)
SCALE2 = (1.0 / math.sqrt(HEAD_DIM)) * math.log2(math.e)
BF16 = jnp.bfloat16
F32 = jnp.float32
MESH = pl.DeviceIdType.MESH


def rope_freqs():
    exponent = jnp.arange(0, HEAD_DIM, 2).astype(jnp.float32) / HEAD_DIM
    base_freq = 1.0 / (500000.0 ** exponent)
    wave_len = 2.0 * math.pi / base_freq
    smooth = (8192.0 / wave_len - 1.0) / 3.0
    blended = (1.0 - smooth) * base_freq / 8.0 + smooth * base_freq
    return jnp.where(wave_len < 2048.0, base_freq, jnp.where(wave_len > 8192.0, base_freq / 8.0, blended))


def rotate(vec_bf, cos, sin):
    vec = vec_bf.astype(F32)
    return (vec * cos + pltpu.roll(vec, HEAD_DIM // 2, axis=1) * sin).astype(BF16)


def layer(x, gain, w_q, w_k, w_v, w_o, positions, freqs):
    rows, width = x.shape
    seg = rows // 2
    d = HEAD_DIM
    kvh = w_k.shape[1] // d
    group = w_q.shape[1] // w_k.shape[1]
    gw = group * d
    qw = kvh * gw
    n_tp = width // qw
    n_seg = 8
    total = n_seg * seg
    blk = 256
    n_blk = rows // blk
    half_w = width // 2
    bq, bk = 256, 512
    cols = bq * group
    unit_rows = 2 * bq
    slice_rows = qw // 8
    y_cols = 512
    nr = 32

    def kernel(x_ref, gain_ref, wq_ref, wk_ref, wv_ref, wo_ref, pos_ref, freq_ref,
               y_ref, k_ref, v_ref, oall_ref, wall_ref,
               big, kb, vb, qb, xb, csb, vst, qt, s_a, s_b, acc_a, acc_b, m_run, l_run, m_tile, yb,
               ld_sem, x_sem, vst_sem, kout_sem,
               kv_s, kv_r, wz_s, wz_r, wp_s, wp_r, wc_s, wc_r,
               o_s, o_l, o_r, f_s, ob_sem, yb_sem, wl_sem):
        dp, z, cp = lax.axis_index("dp"), lax.axis_index("tp"), lax.axis_index("cp")
        cy, cc = cp // 2, cp % 2
        x_nb = {"dp": 1 - dp}
        y_nb = {"cp": (1 - cy) * 2 + cc}
        c_nb = {"cp": cy * 2 + 1 - cc}
        peer = lambda off: {"tp": lax.rem(z + off, n_tp)}

        def remote(src, dst, ss, rs, dev):
            return pltpu.make_async_remote_copy(src_ref=src, dst_ref=dst, send_sem=ss, recv_sem=rs, device_id=dev, device_id_type=MESH)

        def got(region, rs):
            remote(region, region, rs, rs, x_nb).wait_recv()

        barrier = pltpu.get_barrier_semaphore()
        for dev in (x_nb, y_nb, c_nb, peer(1), peer(2), peer(3)):
            pl.semaphore_signal(barrier, inc=1, device_id=dev, device_id_type=MESH)
        pl.semaphore_wait(barrier, 6)

        place = dp * 4 + cp

        def w_rows(zs, fx, fy, fc):
            px = 1 - dp if fx else dp
            py = 1 - cy if fy else cy
            pc = 1 - cc if fc else cc
            return pl.multiple_of(zs * qw + (px * 4 + py * 2 + pc) * slice_rows, slice_rows)

        def w_piece(zs, fx, fy, fc, lo=0, n=slice_rows):
            return wall_ref.at[pl.ds(pl.multiple_of(w_rows(zs, fx, fy, fc) + lo, 64), n), :]

        middle = (z == 1) | (z == 2)
        partner = z + 1 - 2 * (z % 2)
        other_mid = jnp.where(z < 2, 2, 1)
        other_end = jnp.where(z < 2, 3, 0)
        sources = (z, partner, other_mid, other_end)
        slot_out = jnp.where(middle, 1, 2)

        src_z = lambda o: sources[o + 1]

        def z_copy(o):
            src = wo_ref.at[pl.ds(pl.multiple_of(place * slice_rows, slice_rows), slice_rows), :]
            dst = w_piece(z, 0, 0, 0)
            return remote(src, dst, wz_s.at[o], wz_r.at[0 if o == 0 else slot_out], {"tp": sources[o + 1]})

        def z_forward():
            there = w_piece(other_end, 0, 0, 0)
            return remote(there, there, wz_s.at[3], wz_r.at[2], {"tp": partner})
        half_n = slice_rows // 2

        def w_send(kind, o):
            zs = src_z(o)
            if kind == 0:
                return remote(w_piece(zs, 0, 0, 0), w_piece(zs, 0, 0, 0), wp_s.at[0, o], wp_r.at[0, o], x_nb)
            if kind == 1:
                return remote(w_piece(zs, 0, 0, 0), w_piece(zs, 0, 0, 0), wp_s.at[1, o], wp_r.at[1, o], y_nb)
            if kind == 2:
                return remote(w_piece(zs, 1, 0, 0, 0, half_n), w_piece(zs, 1, 0, 0, 0, half_n), wp_s.at[2, o], wp_r.at[2, o], y_nb)
            return remote(w_piece(zs, 0, 1, 0, half_n, half_n), w_piece(zs, 0, 1, 0, half_n, half_n), wp_s.at[3, o], wp_r.at[3, o], x_nb)

        def c_send(i, o):
            zs = src_z(o)
            piece = w_piece(zs, i & 1, i >> 1, 0)
            return remote(piece, piece, wc_s.at[i, o], wc_r.at[i, o], c_nb)

        def w_stage1(o):
            zs = src_z(o)
            if o < 2:
                got(w_piece(zs, 0, 0, 0), wz_r.at[o])
            else:
                @pl.when(jnp.logical_not(middle))
                def _():
                    got(w_piece(zs, 0, 0, 0), wz_r.at[o])

            w_send(0, o).start()
            w_send(1, o).start()
            c_send(0, o).start()

        def w_stage2(o):
            zs = src_z(o)
            got(w_piece(zs, 1, 0, 0), wp_r.at[0, o])
            w_send(2, o).start()
            c_send(1, o).start()
            got(w_piece(zs, 0, 1, 0), wp_r.at[1, o])
            w_send(3, o).start()
            c_send(2, o).start()

        def w_stage3(o):
            zs = src_z(o)
            got(w_piece(zs, 1, 1, 0, 0, half_n), wp_r.at[2, o])
            got(w_piece(zs, 1, 1, 0, half_n, half_n), wp_r.at[3, o])
            c_send(3, o).start()

        def w_load(zs, src, i):
            out = []
            for n in range(2):
                out.append(pltpu.make_async_copy(
                    src.at[:, pl.ds(n * half_w, half_w)],
                    big.at[n, pl.ds(pl.multiple_of(zs * qw, qw), qw), :], wl_sem.at[i, n]))
            return out

        def w_load_own():
            return w_load(z, wo_ref, 3)

        def w_load_other(o):
            zs = src_z(o)
            return w_load(zs, wall_ref.at[pl.ds(pl.multiple_of(zs * qw, qw), qw), :], o)

        def w_stage4(o):
            zs = src_z(o)
            for i in range(4):
                got(w_piece(zs, i & 1, i >> 1, 1), wc_r.at[i, o])
            for c in w_load_other(o):
                c.start()

        load_k = pltpu.make_async_copy(wk_ref, big.at[0, :, pl.ds(qw, kvh * d)], ld_sem.at[0])
        load_v = pltpu.make_async_copy(wv_ref, big.at[0, :, pl.ds(qw + kvh * d, kvh * d)], ld_sem.at[1])
        load_q = pltpu.make_async_copy(wq_ref, big.at[0, :, pl.ds(0, qw)], ld_sem.at[2])

        def x_copy(b, slot):
            return pltpu.make_async_copy(x_ref.at[pl.ds(pl.multiple_of(b * blk, blk), blk), :], xb.at[slot], x_sem.at[slot])

        low_lanes = lax.broadcasted_iota(jnp.int32, (blk, d), 1) < d // 2

        def make_angles(b):
            first = pos_ref[b * blk]
            pos = (lax.broadcasted_iota(jnp.int32, (blk, d), 0) + first).astype(F32)
            angle = pos * freq_ref[...]
            csb[pl.ds(pl.multiple_of(b * blk, blk), blk), :] = jnp.where(low_lanes, jnp.cos(angle), jnp.sin(angle))

        def cos_sin(b):
            both = csb[pl.ds(pl.multiple_of(b * blk, blk), blk), :]
            turned = pltpu.roll(both, d // 2, axis=1)
            return jnp.where(low_lanes, both, turned), jnp.where(low_lanes, -turned, both)

        def v_copy(b, slot):
            return pltpu.make_async_copy(vst.at[slot], v_ref.at[pl.ds(pl.multiple_of(b * blk, blk), blk), :], vst_sem.at[slot])

        x_copy(0, 0).start()
        load_k.start()
        load_v.start()
        load_q.start()
        z_copy(0).start()
        z_copy(1).start()

        @pl.when(middle)
        def _():
            z_copy(2).start()

        seg_at = lambda half, c: jnp.where(half == 0, c, n_seg - 1 - c) * seg

        def kv_region(half, c, which):
            at = pl.multiple_of(seg_at(half, c), seg)
            return kb.at[:, pl.ds(at // blk, seg // blk)] if which == 0 else vb.at[:, :, pl.ds(at, seg)]

        y_cp = (1 - cy) * 2 + cc
        c_cp = cy * 2 + 1 - cc
        yc_cp = (1 - cy) * 2 + 1 - cc

        def kv_send(half, which, kind):
            c, dev = ((cp, c_nb), (cp, y_nb), (y_cp, c_nb))[kind]
            region = kv_region(half, c, which)
            i = half * 2 + which
            return remote(region, region, kv_s.at[kind, i], kv_r.at[kind, i], dev)

        def kv_relay(half):
            for which in range(2):
                got(kv_region(half, y_cp, which), kv_r.at[1, half * 2 + which])
                kv_send(half, which, 2).start()

        def kv_arrived(half):
            for which in range(2):
                got(kv_region(half, c_cp, which), kv_r.at[0, half * 2 + which])
                got(kv_region(half, yc_cp, which), kv_r.at[2, half * 2 + which])

        def k_copy(half, hh):
            at = pl.multiple_of(seg_at(half, cp), seg)
            n = seg // blk
            return pltpu.make_async_copy(kb.at[hh, pl.ds(at // blk, n)], k_ref.at[pl.ds(half * n, n), :, pl.ds(hh * d, d)], kout_sem.at[half, hh])

        load_k.wait()
        load_v.wait()

        def h_rows(b):
            h0 = big[1, pl.ds(pl.multiple_of(b * blk, blk), blk), :]
            h1 = big[1, pl.ds(pl.multiple_of(rows + b * blk, blk), blk), :]
            return jnp.concatenate([h0, h1], axis=1)

        def kv_block(b, carry):
            slot = b % 2
            x_copy(b, slot).wait()

            @pl.when(b + 1 < n_blk)
            def _():
                x_copy(b + 1, 1 - slot).start()

            def norm_rows(i, carry):
                at = pl.multiple_of(i * nr, nr)
                xf = xb[slot, pl.ds(at, nr), :].astype(F32)
                inv = lax.rsqrt(jnp.mean(xf * xf, axis=-1, keepdims=True) + NORM_EPS)
                for i in range(width // d):
                    lanes = slice(i * d, (i + 1) * d)
                    h = ((xf[:, lanes] * inv) * gain_ref[i:i + 1, :].astype(F32)).astype(BF16)
                    row = b * blk + (0 if i * d < half_w else rows)
                    lane = (i * d) % half_w
                    big[1, pl.ds(pl.multiple_of(row, blk) + at, nr), lane:lane + d] = h
                return carry

            lax.fori_loop(0, blk // nr, norm_rows, 0)
            h = h_rows(b)
            make_angles(b)
            kv = jnp.dot(h, big[0, :, qw:qw + 2 * kvh * d], preferred_element_type=F32).astype(BF16)
            cos, sin = cos_sin(b)
            at = pl.multiple_of(seg_at(b // 4, cp) + (b % 4) * blk, blk)

            @pl.when(b >= 2)
            def _():
                v_copy(b - 2, slot).wait()

            for hh in range(kvh):
                kb[hh, at // blk] = rotate(kv[:, hh * d:(hh + 1) * d], cos, sin)
                vb[hh, :, pl.ds(at, blk)] = kv[:, (kvh + hh) * d:(kvh + hh + 1) * d].T
            vst[slot] = kv[:, kvh * d:]
            v_copy(b, slot).start()
            for half in range(2):
                @pl.when(b == half * 4 + 3)
                def _():
                    for which in range(2):
                        kv_send(half, which, 1).start()
                        kv_send(half, which, 0).start()
                    for hh in range(kvh):
                        k_copy(half, hh).start()
            return carry

        lax.fori_loop(0, n_blk, kv_block, 0)
        v_copy(n_blk - 2, 0).wait()
        v_copy(n_blk - 1, 1).wait()
        load_q.wait()

        def q_half(half):
            def q_block(i, carry):
                b = half * 4 + i
                cos, sin = cos_sin(b)
                q = jnp.dot(h_rows(b), big[0, :, 0:qw], preferred_element_type=F32).astype(BF16)
                at = pl.multiple_of(b * blk, blk)
                for j in range(qw // d):
                    qb[j, pl.ds(at, blk), :] = rotate(q[:, j * d:(j + 1) * d], cos, sin)
                return carry

            lax.fori_loop(0, 4, q_block, 0)

        def o_region(zz, rb, hh):
            return oall_ref.at[pl.ds((zz * kvh + hh) * group, group), pl.ds(pl.multiple_of(rb * blk, blk), blk), :]

        def o_own(rb, hh):
            return qb.at[pl.ds(hh * group, group), pl.ds(pl.multiple_of(rb * blk, blk), blk), :]

        def o_local(rb, hh):
            return pltpu.make_async_copy(o_own(rb, hh), o_region(z, rb, hh), o_l.at[rb, hh])

        def o_send(kind, rb, hh):
            if kind == 0:
                return remote(o_own(rb, hh), o_region(z, rb, hh), o_s.at[0, rb, hh], o_r.at[0, rb, hh], {"tp": partner})
            return remote(o_own(rb, hh), o_region(z, rb, hh), o_s.at[1, rb, hh], o_r.at[slot_out, rb, hh], {"tp": other_mid})

        def o_fwd(kind, rb, hh):
            zz = other_mid if kind == 0 else other_end
            return remote(o_region(zz, rb, hh), o_region(zz, rb, hh), f_s.at[kind, rb, hh], o_r.at[1 + kind, rb, hh], {"tp": partner})

        scores = (s_a, s_b)
        accs = (acc_a, acc_b)

        def unit(u):
            half, c, hh = u // 4, (u // 2) % 2, u % 2
            r0 = pl.multiple_of(half * seg + c * unit_rows, unit_rows)
            g0 = seg_at(half, cp) + c * unit_rows
            for st in range(2):
                for j in range(group):
                    blk_q = qb[hh * group + j, pl.ds(r0 + st * bq, bq), :]
                    qs = blk_q.T.astype(F32) * SCALE2
                    top = qs.astype(BF16)
                    span = slice(j * bq, (j + 1) * bq)
                    qt[st, 0:d, span] = top
                    qt[st, d:2 * d, span] = (qs - top.astype(F32)).astype(BF16)
            k_idx = lax.broadcasted_iota(jnp.int32, (bk, cols), 0)
            q_idx = lax.broadcasted_iota(jnp.int32, (bk, cols), 1) % bq

            def qk(st, t, mask=None):
                kt = kb[hh, pl.ds(t * (bk // blk), bk // blk)].reshape(bk, d)
                s = jnp.dot(jnp.concatenate([kt, kt], axis=1), qt[st], preferred_element_type=F32)
                if mask is not None:
                    s = jnp.where(mask, s, NEG)
                scores[st][...] = s
                m_tile[st] = jnp.max(s, axis=0, keepdims=True)

            def soft(st, t):
                m_old = m_run[st]
                m_new = jnp.maximum(m_old, m_tile[st])
                m_run[st] = m_new
                alpha = jnp.exp2(m_old - m_new)
                p = jnp.exp2(scores[st][...] - m_new)
                l_run[st] = l_run[st] * alpha + jnp.sum(p, axis=0, keepdims=True)
                pv = jnp.dot(vb[hh, :, pl.ds(pl.multiple_of(t * bk, bk), bk)], p.astype(BF16), preferred_element_type=F32)
                accs[st][...] = accs[st][...] * alpha + pv

            m_run[...] = jnp.full_like(m_run, NEG)
            l_run[...] = jnp.zeros_like(l_run)
            acc_a[...] = jnp.zeros_like(acc_a)
            acc_b[...] = jnp.zeros_like(acc_b)
            n_full = g0 // bk

            @pl.when(n_full > 0)
            def _():
                qk(0, 0)

            @pl.when(n_full == 0)
            def _():
                qk(0, 0, k_idx <= q_idx)

            def body(t, carry):
                qk(1, t)
                soft(0, t)
                qk(0, t + 1)
                soft(1, t)
                return carry

            lax.fori_loop(0, n_full - 1, body, 0)

            @pl.when(n_full > 0)
            def _():
                qk(1, n_full - 1)
                soft(0, n_full - 1)
                qk(0, n_full, k_idx <= q_idx)
                soft(1, n_full - 1)

            qk(1, n_full, k_idx <= q_idx + bq)
            soft(0, n_full)
            soft(1, n_full)
            for st in range(2):
                o = accs[st][...] * (1.0 / l_run[st])
                for j in range(group):
                    qb[hh * group + j, pl.ds(r0 + st * bq, bq), :] = o[:, j * bq:(j + 1) * bq].T.astype(BF16)
            for st in range(2):
                rb = half * 4 + c * 2 + st
                o_send(0, rb, hh).start()
                o_send(1, rb, hh).start()
                o_local(rb, hh).start()

        q_half(0)
        kv_relay(0)
        kv_arrived(0)


        def o_forward(rb):
            @pl.when(middle)
            def _():
                for kind, zz in ((0, other_mid), (1, other_end)):
                    for hh in range(kvh):
                        got(o_region(zz, rb, hh), o_r.at[1 + kind, rb, hh])
                        o_fwd(kind, rb, hh).start()

        def unit_loop(u, carry):
            @pl.when(u == 4)
            def _():
                @pl.when(middle)
                def _():
                    got(w_piece(other_end, 0, 0, 0), wz_r.at[2])
                    z_forward().start()

                kv_relay(1)
                q_half(1)
                for c in w_load_own():
                    c.start()
                kv_arrived(1)
                w_stage1(0)
                w_stage1(1)

            unit(u)

            @pl.when((u == 4) & middle)
            def _():
                w_stage1(2)

            @pl.when(u == 5)
            def _():
                o_forward(0)

            @pl.when(u == 6)
            def _():
                w_stage2(0)
                w_stage2(1)
                o_forward(1)
            return carry

        lax.fori_loop(0, 8, unit_loop, 0)

        def o_landed(kind, rb):
            for hh in range(kvh):
                if kind == 0:
                    o_local(rb, hh).wait()
                elif kind == 1:
                    got(o_region(partner, rb, hh), o_r.at[0, rb, hh])
                else:
                    @pl.when(jnp.logical_not(middle))
                    def _():
                        got(o_region(sources[kind], rb, hh), o_r.at[kind - 1, rb, hh])

        heads = kvh * group

        def ob_copy(kind, rb, slot):
            zz = sources[kind]
            return pltpu.make_async_copy(
                oall_ref.at[pl.ds(zz * heads, heads), pl.ds(pl.multiple_of(rb * blk, blk), blk), :],
                kb.at[slot, pl.ds(zz * heads, heads)], ob_sem.at[slot, kind])

        def o_fetch(rb, slot, kinds):
            for kind in kinds:
                o_landed(kind, rb)
                ob_copy(kind, rb, slot).start()

        n_y = width // y_cols
        n_h = half_w // y_cols

        def y_copy(rb, n, slot):
            return pltpu.make_async_copy(
                yb.at[slot],
                y_ref.at[pl.ds(pl.multiple_of(rb * blk, blk), blk), pl.ds(pl.multiple_of(n * y_cols, y_cols), y_cols)], yb_sem.at[slot])

        x_copy(0, 0).start()

        @pl.when(jnp.logical_not(middle))
        def _():
            w_stage1(2)

        o_forward(2)
        w_stage3(0)
        w_stage3(1)
        w_stage4(0)
        w_stage2(2)
        o_forward(3)
        w_stage4(1)
        w_stage3(2)
        w_stage4(2)
        for half in range(2):
            for which in range(2):
                for kind in range(3):
                    kv_send(half, which, kind).wait_send()
            for hh in range(kvh):
                k_copy(half, hh).wait()
        o_fetch(0, 0, range(4))
        for c in w_load_own() + w_load_other(0) + w_load_other(1) + w_load_other(2):
            c.wait()

        def product(slot, kinds, n):
            acc = None
            lane = pl.multiple_of((n % n_h) * y_cols, y_cols)
            for kind in kinds:
                zz = sources[kind]
                o = jnp.concatenate([kb[slot, zz * heads + i] for i in range(heads)], axis=1)
                w = big[n // n_h, pl.ds(pl.multiple_of(zz * qw, qw), qw), pl.ds(lane, y_cols)]
                term = jnp.dot(o, w, preferred_element_type=F32)
                acc = term if acc is None else acc + term
            return acc

        def x_cols(slot, n):
            return xb[slot, :, pl.ds(pl.multiple_of(n * y_cols, y_cols), y_cols)].astype(F32)

        def out_block(rb, carry):
            slot = rb % 2
            x_copy(rb, slot).wait()
            for kind in range(4):
                ob_copy(kind, rb, slot).wait()
            x_copy(rb + 1, 1 - slot).start()

            def out_cols(n, carry):
                ys = n % 2

                @pl.when(rb * n_y + n >= 2)
                def _():
                    y_copy(rb, n, ys).wait()

                yb[ys] = (x_cols(slot, n) + product(slot, range(4), n)).astype(BF16)
                y_copy(rb, n, ys).start()
                return carry

            lax.fori_loop(0, n_y, out_cols, 0)

            @pl.when(rb + 4 < n_blk)
            def _():
                o_forward(rb + 4)

            @pl.when(rb + 2 < n_blk)
            def _():
                o_fetch(rb + 1, 1 - slot, range(4))
            return carry

        lax.fori_loop(0, n_blk - 1, out_block, 0)

        last, slot = n_blk - 1, (n_blk - 1) % 2
        o_fetch(last, slot, range(3))
        x_copy(last, slot).wait()
        for kind in range(3):
            ob_copy(kind, last, slot).wait()

        def part(n):
            return (pl.ds(pl.multiple_of((n % n_h) // 2 * blk, blk), blk), pl.ds(pl.multiple_of(n % 2 * y_cols, y_cols), y_cols))

        for i in range(2):
            def first_terms(n, carry):
                scores[i][part(n)] = x_cols(slot, n) + product(slot, range(3), n)
                return carry

            lax.fori_loop(i * n_h, (i + 1) * n_h, first_terms, 0)
        o_fetch(last, slot, (3,))
        ob_copy(3, last, slot).wait()
        for i in range(2):
            def last_terms(n, carry):
                ys = n % 2
                y_copy(last, n, ys).wait()
                yb[ys] = (scores[i][part(n)] + product(slot, (3,), n)).astype(BF16)
                y_copy(last, n, ys).start()
                return carry

            lax.fori_loop(i * n_h, (i + 1) * n_h, last_terms, 0)
        for n in (n_y - 2, n_y - 1):
            y_copy(n_blk - 1, n, n % 2).wait()

        def drain(i, carry):
            rb, hh = i // kvh, i % kvh
            o_send(0, rb, hh).wait_send()
            o_send(1, rb, hh).wait_send()

            @pl.when(middle)
            def _():
                o_fwd(0, rb, hh).wait_send()
                o_fwd(1, rb, hh).wait_send()
            return carry

        lax.fori_loop(0, n_blk * kvh, drain, 0)
        z_copy(0).wait_send()
        z_copy(1).wait_send()

        @pl.when(middle)
        def _():
            z_copy(2).wait_send()
            z_forward().wait_send()

        for o in range(3):
            for kind in range(4):
                w_send(kind, o).wait_send()
                c_send(kind, o).wait_send()

    any_spec = pl.BlockSpec(memory_space=pl.ANY)
    vmem_spec = pl.BlockSpec(memory_space=pltpu.VMEM)
    dma = pltpu.SemaphoreType.DMA
    outs = pl.pallas_call(
        kernel,
        in_specs=[any_spec, vmem_spec] + [any_spec] * 4 + [pl.BlockSpec(memory_space=pltpu.SMEM), vmem_spec],
        out_specs=[any_spec] * 5,
        out_shape=[
            jax.ShapeDtypeStruct((rows, width), BF16),
            jax.ShapeDtypeStruct((n_blk, blk, kvh * d), BF16),
            jax.ShapeDtypeStruct((rows, kvh * d), BF16),
            jax.ShapeDtypeStruct((n_tp * kvh * group, rows, d), BF16),
            jax.ShapeDtypeStruct((width, width), BF16),
        ],
        scratch_shapes=[
            pltpu.VMEM((2, width, half_w), BF16),
            pltpu.VMEM((kvh, total // blk, blk, d), BF16),
            pltpu.VMEM((kvh, d, total), BF16),
            pltpu.VMEM((qw // d, rows, d), BF16),
            pltpu.VMEM((2, blk, width), BF16),
            pltpu.VMEM((rows, d), F32),
            pltpu.VMEM((2, blk, kvh * d), BF16),
            pltpu.VMEM((2, 2 * d, cols), BF16),
            pltpu.VMEM((bk, cols), F32),
            pltpu.VMEM((bk, cols), F32),
            pltpu.VMEM((d, cols), F32),
            pltpu.VMEM((d, cols), F32),
            pltpu.VMEM((2, 1, cols), F32),
            pltpu.VMEM((2, 1, cols), F32),
            pltpu.VMEM((2, 1, cols), F32),
            pltpu.VMEM((2, blk, y_cols), BF16),
            dma((3,)), dma((2,)), dma((2,)), dma((2, kvh)),
            dma((3, 4)), dma((3, 4)), dma((4,)), dma((3,)), dma((4, 3)), dma((4, 3)), dma((4, 3)), dma((4, 3)),
            dma((2, n_blk, kvh)), dma((n_blk, kvh)), dma((3, n_blk, kvh)), dma((2, n_blk, kvh)), dma((2, 4)), dma((2,)), dma((4, 2)),
        ],
        compiler_params=pltpu.CompilerParams(collective_id=0, has_side_effects=True, vmem_limit_bytes=67043328),
        name="sublayer",
    )(x, gain, w_q, w_k, w_v, w_o, positions, freqs)
    return outs[0], outs[1], outs[2]


def solution(mesh):
    def device_fn(x_in, positions, norm_gain, w_q, w_k, w_v, w_o):
        kv_heads = w_k.shape[1] // HEAD_DIM
        freqs = rope_freqs()
        freqs = jnp.concatenate([freqs, freqs])[None, :]
        gain = norm_gain.reshape(-1, HEAD_DIM)
        y, keys, values = layer(x_in, gain, w_q, w_k, w_v, w_o, positions, freqs)
        shape = (x_in.shape[0], kv_heads, HEAD_DIM)
        return y, keys.reshape(shape), values.reshape(shape)

    row_spec = P(('dp', 'cp'), None)
    cache_spec = P(('dp', 'cp'), 'tp', None)
    return jax.shard_map(device_fn, mesh=mesh, in_specs=(row_spec, P(('dp', 'cp')), P(None), P(None, 'tp'), P(None, 'tp'), P(None, 'tp'), P('tp', None)), out_specs=(row_spec, cache_spec, cache_spec), check_vma=False)
```

```python
import math
import jax
import jax.numpy as jnp
from jax import lax
from jax.experimental import pallas as pl
from jax.experimental.pallas import tpu as pltpu
from jax.sharding import PartitionSpec as P

HEAD_DIM = 128
NORM_EPS = 1e-5
NEG = -0.7 * float(jnp.finfo(jnp.float32).max)
SCALE2 = (1.0 / math.sqrt(HEAD_DIM)) * math.log2(math.e)
BF16 = jnp.bfloat16
F32 = jnp.float32
MESH = pl.DeviceIdType.MESH
LOW, HIGH = range(2)
TOP, BOTTOM = range(2)
FIRST, SECOND, MOVED = SLOTS = range(3)
PARTNER, MID, END, SHIFTED = PIECES = range(4)


def rope_freqs():
    exponent = jnp.arange(0, HEAD_DIM, 2).astype(jnp.float32) / HEAD_DIM
    base_freq = 1.0 / (500000.0 ** exponent)
    wave_len = 2.0 * math.pi / base_freq
    smooth = (8192.0 / wave_len - 1.0) / 3.0
    blended = (1.0 - smooth) * base_freq / 8.0 + smooth * base_freq
    return jnp.where(wave_len < 2048.0, base_freq, jnp.where(wave_len > 8192.0, base_freq / 8.0, blended))


def repeat(n, step, first=0):
    lax.fori_loop(first, first + n, lambda i, carry: (step(i), carry)[1], 0)


def pick(i, values):
    out = values[-1]
    for at, value in enumerate(values[:-1]):
        out = jnp.where(i == at, value, out)
    return out


def rotate(vec_bf, cos, sin):
    vec = vec_bf.astype(F32)
    return (vec * cos + pltpu.roll(vec, HEAD_DIM // 2, axis=1) * sin).astype(BF16)


def layer(x, gain, w_q, w_k, w_v, w_o, positions, freqs):
    rows, width = x.shape
    seg = rows // 2
    d = HEAD_DIM
    kvh = w_k.shape[1] // d
    group = w_q.shape[1] // w_k.shape[1]
    gw = group * d
    qw = kvh * gw
    n_tp = width // qw
    n_groups = n_tp * kvh
    heads = n_groups * group
    n_seg = 8
    blk = 256
    n_blk = rows // blk
    n_lane = width // d
    half_w = width // 2
    bq, bk, bp = 256, 512, 256
    cols = bq * group
    unit_rows = 2 * bq
    w_slice = qw // 8
    s_slice = width // 8
    s_cols = gw + 2 * d
    s_at = qw
    y_cols = 512
    nr = 128
    assert n_blk == n_groups and heads == n_lane

    def kernel(x_ref, gain_ref, wq_ref, wk_ref, wv_ref, wo_ref, pos_ref, freq_ref,
               y_ref, k_ref, v_ref, oall_ref, wall_ref, wsx_ref,
               big, kb, vb, qb, csb, vst, qt, s_a, s_b, acc_a, acc_b, m_run, l_run, m_tile, yb,
               ld_sem, x_sem, vst_sem, kout_sem,
               kv_s, kv_r, wz_s, wz_r, sz_s, sz_r, wp_s, wp_r, wc_s, wc_r,
               o_s, o_l, o_r, f_s, ob_sem, yb_sem, wl_sem):
        dp, z, cp = lax.axis_index("dp"), lax.axis_index("tp"), lax.axis_index("cp")
        cy, cc = cp // 2, cp % 2
        x_nb = {"dp": 1 - dp}
        y_nb = {"cp": (1 - cy) * 2 + cc}
        c_nb = {"cp": cy * 2 + 1 - cc}

        middle = (z == 1) | (z == 2)
        end = jnp.logical_not(middle)
        partner = z + 1 - 2 * (z % 2)
        other_mid = jnp.where(z < 2, 2, 1)
        other_end = jnp.where(z < 2, 3, 0)
        sources = (z, partner, other_mid, other_end)
        slot_out = jnp.where(middle, MID, END)
        keep = jnp.where(z == 1, SECOND, FIRST)
        head_at = lambda slot: jnp.where(middle, keep, slot)
        last_z = n_tp - 1

        def group_of(zz, slot):
            at_far_end = n_groups - len(SLOTS) + (slot + 1) % len(SLOTS) if isinstance(slot, int) else (
                n_groups - len(SLOTS) + lax.rem(slot + 1, len(SLOTS)))
            return jnp.where(zz == 0, slot, jnp.where(zz == last_z, at_far_end, zz + kvh))

        source = lambda piece: sources[piece + 1]

        def remote(src, dst, ss, rs, dev):
            return pltpu.make_async_remote_copy(src_ref=src, dst_ref=dst, send_sem=ss, recv_sem=rs, device_id=dev, device_id_type=MESH)

        def got(region, rs):
            remote(region, region, rs, rs, x_nb).wait_recv()

        def at_rows(n, size):
            return pl.ds(pl.multiple_of(n, size), size)

        barrier = pltpu.get_barrier_semaphore()
        for dev in (x_nb, y_nb, c_nb, {"tp": partner}, {"tp": other_mid}, {"tp": other_end}):
            pl.semaphore_signal(barrier, inc=1, device_id=dev, device_id_type=MESH)
        pl.semaphore_wait(barrier, 6)

        place = dp * 4 + cp

        def place_of(fx, fy, fc):
            px = 1 - dp if fx else dp
            py = 1 - cy if fy else cy
            pc = 1 - cc if fc else cc
            return px * 4 + py * 2 + pc

        def piece(o, fx, fy, fc, part=None):
            size = s_slice if o == SHIFTED else w_slice
            base = place_of(fx, fy, fc) * size
            if o != SHIFTED:
                base = base + source(o) * qw
            n = size if part is None else size // 2
            base = pl.multiple_of(base + (n if part == BOTTOM else 0), n)
            return (wsx_ref if o == SHIFTED else wall_ref).at[pl.ds(base, n), :]

        here = lambda o: piece(o, 0, 0, 0)
        next_x = lambda o, part=None: piece(o, 1, 0, 0, part)
        next_y = lambda o, part=None: piece(o, 0, 1, 0, part)
        next_xy = lambda o, part=None: piece(o, 1, 1, 0, part)
        at_core = lambda o: (here(o), next_x(o), next_y(o), next_xy(o))

        def z_copy(o):
            src = wo_ref.at[at_rows(place * w_slice, w_slice), :]
            dst = wall_ref.at[at_rows(z * qw + place * w_slice, w_slice), :]
            return remote(src, dst, wz_s.at[o], wz_r.at[PARTNER if o == PARTNER else slot_out], {"tp": source(o)})

        def z_forward():
            return remote(here(END), here(END), wz_s.at[SHIFTED], wz_r.at[END], {"tp": partner})

        s_parts = ((wq_ref, 0, gw), (wk_ref, gw, d), (wv_ref, gw + d, d))

        def s_dst(i):
            _, lane, n = s_parts[i]
            return wsx_ref.at[at_rows(place * s_slice, s_slice), pl.ds(lane, n)]

        def s_copy(i):
            ref, _, n = s_parts[i]
            src = ref.at[at_rows(place * s_slice, s_slice), at_rows((1 - keep) * n, n)]
            return remote(src, s_dst(i), sz_s.at[i], sz_r.at[i], {"tp": partner})

        OWN_X, OWN_Y, X_TO_Y, Y_TO_X = kinds = range(4)

        def w_send(kind, o):
            if kind == OWN_X:
                region, dev = here(o), x_nb
            elif kind == OWN_Y:
                region, dev = here(o), y_nb
            elif kind == X_TO_Y:
                region, dev = next_x(o, TOP), y_nb
            else:
                region, dev = next_y(o, None if o == SHIFTED else BOTTOM), x_nb
            return remote(region, region, wp_s.at[kind, o], wp_r.at[kind, o], dev)

        def c_send(i, o):
            region = at_core(o)[i]
            return remote(region, region, wc_s.at[i, o], wc_r.at[i, o], c_nb)

        def w_stage1(o):
            if o == SHIFTED:
                for i in range(len(s_parts)):
                    got(s_dst(i), sz_r.at[i])
            elif o != END:
                got(here(o), wz_r.at[o])
            else:
                @pl.when(end)
                def _():
                    got(here(o), wz_r.at[o])

            w_send(OWN_X, o).start()
            w_send(OWN_Y, o).start()
            c_send(0, o).start()

        def w_stage2(o):
            got(next_x(o), wp_r.at[OWN_X, o])
            if o != SHIFTED:
                w_send(X_TO_Y, o).start()
            c_send(1, o).start()
            got(next_y(o), wp_r.at[OWN_Y, o])
            w_send(Y_TO_X, o).start()
            c_send(2, o).start()

        def w_stage3(o):
            if o != SHIFTED:
                got(next_xy(o, TOP), wp_r.at[X_TO_Y, o])
            got(next_xy(o, None if o == SHIFTED else BOTTOM), wp_r.at[Y_TO_X, o])
            c_send(3, o).start()

        def w_gathered(o):
            for i, (fx, fy) in enumerate(((0, 0), (1, 0), (0, 1), (1, 1))):
                got(piece(o, fx, fy, 1), wc_r.at[i, o])

        def w_load(zs, src, i):
            return [pltpu.make_async_copy(
                src.at[:, pl.ds(n * half_w, half_w)], big.at[n, at_rows(zs * qw, qw), :], wl_sem.at[i, n]) for n in range(2)]

        def w_load_own():
            return w_load(z, wo_ref, SHIFTED)

        def w_load_other(o):
            return w_load(source(o), wall_ref.at[at_rows(source(o) * qw, qw), :], o)

        def w_stage4(o):
            w_gathered(o)
            for c in w_load_other(o):
                c.start()

        def load_weights(i, ref, lane, n):
            return pltpu.make_async_copy(ref, big.at[0, :, pl.ds(lane, n)], ld_sem.at[i])

        load_q, load_k, load_v, load_s = (load_weights(i, *args) for i, args in enumerate((
            (wq_ref, 0, qw), (wk_ref, qw, kvh * d), (wv_ref, qw + kvh * d, kvh * d), (wsx_ref, s_at, s_cols))))

        def x_start(b, slot):
            for i in range(n_lane):
                pltpu.make_async_copy(x_ref.at[at_rows(b * blk, blk), pl.ds(i * d, d)], kb.at[2 + slot, i], x_sem.at[slot]).start()

        def x_wait(slot):
            pltpu.make_async_copy(kb.at[2 + slot], kb.at[2 + slot], x_sem.at[slot]).wait()

        def v_copy(b):
            return pltpu.make_async_copy(vst, v_ref.at[at_rows(b * blk, blk), :], vst_sem.at[0])

        low_lanes = lax.broadcasted_iota(jnp.int32, (blk, d), 1) < d // 2

        def make_angles(b):
            first = pos_ref[b * blk]
            pos = (lax.broadcasted_iota(jnp.int32, (blk, d), 0) + first).astype(F32)
            angle = pos * freq_ref[...]
            csb[at_rows(b * blk, blk), :] = jnp.where(low_lanes, jnp.cos(angle), jnp.sin(angle))

        def cos_sin(b):
            both = csb[at_rows(b * blk, blk), :]
            turned = pltpu.roll(both, d // 2, axis=1)
            return jnp.where(low_lanes, both, turned), jnp.where(low_lanes, -turned, both)

        x_start(0, 0)
        load_k.start()
        load_v.start()
        load_q.start()

        @pl.when(middle)
        def _():
            for i in range(len(s_parts)):
                s_copy(i).start()

        z_copy(PARTNER).start()
        z_copy(MID).start()

        @pl.when(middle)
        def _():
            z_copy(END).start()

        seg_at = lambda half, c: jnp.where(half == LOW, c, n_seg - 1 - c) * seg
        y_cp = (1 - cy) * 2 + cc
        c_cp = cy * 2 + 1 - cc
        yc_cp = (1 - cy) * 2 + 1 - cc

        def kv_region(half, c, which, slot):
            at = pl.multiple_of(seg_at(half, c), seg)
            h = head_at(slot)
            return kb.at[h, pl.ds(at // blk, seg // blk)] if which == 0 else vb.at[h, :, pl.ds(at, seg)]

        TO_CORE, TO_Y, Y_TO_CORE = kv_kinds = range(3)
        kv_both = range(2)
        n_kv = len(kv_both) * len(SLOTS)
        kv_at = lambda half, which, slot: half * n_kv + which * len(SLOTS) + slot

        def kv_send(kind, half, which, slot):
            region = kv_region(half, y_cp if kind == Y_TO_CORE else cp, which, slot)
            i = kv_at(half, which, slot)
            return remote(region, region, kv_s.at[kind, i], kv_r.at[kind, i], y_nb if kind == TO_Y else c_nb)

        def for_slots(slots, f):
            for slot in slots:
                if slot == FIRST:
                    f(slot)
                else:
                    @pl.when(end)
                    def _():
                        f(slot)

        own = (FIRST, SECOND)
        moved = (MOVED,)

        def kv_start(half, slots):
            def f(slot):
                for which in kv_both:
                    kv_send(TO_Y, half, which, slot).start()
                    kv_send(TO_CORE, half, which, slot).start()
            for_slots(slots, f)

        def kv_relay(half, slots):
            def f(slot):
                for which in kv_both:
                    got(kv_region(half, y_cp, which, slot), kv_r.at[TO_Y, kv_at(half, which, slot)])
                    kv_send(Y_TO_CORE, half, which, slot).start()
            for_slots(slots, f)

        def kv_arrived(half, slots):
            def f(slot):
                for which in kv_both:
                    i = kv_at(half, which, slot)
                    got(kv_region(half, c_cp, which, slot), kv_r.at[TO_CORE, i])
                    got(kv_region(half, yc_cp, which, slot), kv_r.at[Y_TO_CORE, i])
            for_slots(slots, f)

        def kv_sent():
            def f(slot):
                for half in (LOW, HIGH):
                    for which in kv_both:
                        for kind in kv_kinds:
                            kv_send(kind, half, which, slot).wait_send()
            for_slots(SLOTS, f)

        def k_copy(half, hh):
            at = pl.multiple_of(seg_at(half, cp), seg)
            n = seg // blk
            return pltpu.make_async_copy(kb.at[hh, pl.ds(at // blk, n)], k_ref.at[pl.ds(half * n, n), :, pl.ds(hh * d, d)], kout_sem.at[half, hh])

        def h_rows(b):
            h0 = big[1, at_rows(b * blk, blk), :]
            h1 = big[1, at_rows(rows + b * blk, blk), :]
            return jnp.concatenate([h0, h1], axis=1)

        load_k.wait()
        load_v.wait()

        half_blk = n_blk // 2

        def at_half_end(b, f):
            for half in (LOW, HIGH):
                @pl.when(b == half * half_blk + half_blk - 1)
                def _():
                    f(half)

        def kv_rows(b):
            return pl.multiple_of(seg_at(b // half_blk, cp) + lax.rem(b, half_blk) * blk, blk)

        def kv_block(b):
            slot = b % 2
            x_wait(slot)

            @pl.when(b + 1 < n_blk)
            def _():
                x_start(b + 1, 1 - slot)

            def norm_rows(i):
                at = at_rows(i * nr, nr)
                square = 0.0
                for j in range(n_lane):
                    xf = kb[2 + slot, j, at, :].astype(F32)
                    square = square + xf * xf
                inv = lax.rsqrt(jnp.sum(square, axis=-1, keepdims=True) / width + NORM_EPS)
                for j in range(n_lane):
                    xf = kb[2 + slot, j, at, :].astype(F32)
                    h = ((xf * inv) * gain_ref[j:j + 1, :].astype(F32)).astype(BF16)
                    row = b * blk + (0 if j * d < half_w else rows) + i * nr
                    lane = (j * d) % half_w
                    big[1, at_rows(row, nr), lane:lane + d] = h

            repeat(blk // nr, norm_rows)
            make_angles(b)
            kv = jnp.dot(h_rows(b), big[0, :, qw:qw + 2 * kvh * d], preferred_element_type=F32).astype(BF16)
            cos, sin = cos_sin(b)
            at = kv_rows(b)

            @pl.when(b > 0)
            def _():
                v_copy(b - 1).wait()

            for hh in range(kvh):
                kb[hh, at // blk] = rotate(kv[:, hh * d:(hh + 1) * d], cos, sin)
                vb[hh, :, pl.ds(at, blk)] = kv[:, (kvh + hh) * d:(kvh + hh + 1) * d].T
            vst[...] = kv[:, kvh * d:]
            v_copy(b).start()

            def send(half):
                kv_start(half, own)
                for hh in range(kvh):
                    k_copy(half, hh).start()

            at_half_end(b, send)

        repeat(n_blk, kv_block)
        v_copy(n_blk - 1).wait()
        load_q.wait()

        @pl.when(end)
        def _():
            w_stage1(SHIFTED)

        def q_half(half):
            def q_block(b):
                cos, sin = cos_sin(b)

                def project(i):
                    head = head_at(i)
                    q = jnp.dot(h_rows(b), big[0, :, at_rows(head * gw, gw)], preferred_element_type=F32).astype(BF16)
                    for j in range(group):
                        qb[head * group + j, at_rows(b * blk, blk), :] = rotate(q[:, j * d:(j + 1) * d], cos, sin)

                repeat(jnp.where(middle, 1, kvh), project)

            repeat(half_blk, q_block, half * half_blk)

        def moved_block(b):
            cos, sin = cos_sin(b)
            qkv = jnp.dot(h_rows(b), big[0, :, s_at:s_at + s_cols], preferred_element_type=F32).astype(BF16)
            for j in range(group):
                qb[MOVED * group + j, at_rows(b * blk, blk), :] = rotate(qkv[:, j * d:(j + 1) * d], cos, sin)
            at = kv_rows(b)
            kb[MOVED, at // blk] = rotate(qkv[:, gw:gw + d], cos, sin)
            vb[MOVED, :, pl.ds(at, blk)] = qkv[:, gw + d:].T
            at_half_end(b, lambda half: kv_start(half, moved))

        def o_region(g, rb):
            return oall_ref.at[pl.ds(g * group, group), at_rows(rb * blk, blk), :]

        def o_own(slot, rb):
            return qb.at[pl.ds(head_at(slot) * group, group), at_rows(rb * blk, blk), :]

        def o_local(slot, rb):
            return pltpu.make_async_copy(o_own(slot, rb), o_region(group_of(z, slot), rb), o_l.at[rb, slot])

        def o_send(to, slot, rb):
            g = group_of(z, slot)
            return remote(o_own(slot, rb), o_region(g, rb), o_s.at[to, rb, slot], o_r.at[rb, g], {"tp": source(to)})

        others = ((MID, FIRST), (END, FIRST), (END, SECOND), (END, MOVED))
        ends_own = ((PARTNER, FIRST), (PARTNER, SECOND), (PARTNER, MOVED))
        passed = others + ends_own

        def o_pass(what, rb):
            g = group_of(source(what[0]), what[1])
            region = o_region(g, rb)
            to = {"tp": partner if what in others else other_mid}
            return remote(region, region, f_s.at[rb, passed.index(what)], o_r.at[rb, g], to)

        def o_wait(what, rb):
            g = group_of(source(what[0]), what[1])
            got(o_region(g, rb), o_r.at[rb, g])

        def pass_on(what, blocks):
            def step(rb):
                for item in what:
                    o_wait(item, rb)
                    o_pass(item, rb).start()

            repeat(len(blocks), step, blocks[0])

        def own_outward(blocks):
            repeat(len(blocks), lambda rb: o_send(PARTNER, FIRST, rb).start(), blocks[0])

        scores = (s_a, s_b)
        accs = (acc_a, acc_b)

        def unit(half, c, slot):
            hl = head_at(slot)
            r0 = pl.multiple_of(half * seg + c * unit_rows, unit_rows)
            g0 = seg_at(half, cp) + c * unit_rows
            for st in range(2):
                for j in range(group):
                    qs = qb[hl * group + j, pl.ds(r0 + st * bq, bq), :].T.astype(F32) * SCALE2
                    top = qs.astype(BF16)
                    span = slice(j * bq, (j + 1) * bq)
                    qt[st, 0:d, span] = top
                    qt[st, d:2 * d, span] = (qs - top.astype(F32)).astype(BF16)
            k_idx = lax.broadcasted_iota(jnp.int32, (bk, cols), 0)
            q_idx = lax.broadcasted_iota(jnp.int32, (bk, cols), 1) % bq

            def qk(st, t, mask=None):
                kt = kb[hl, pl.ds(t * (bk // blk), bk // blk)].reshape(bk, d)
                s = jnp.dot(jnp.concatenate([kt, kt], axis=1), qt[st], preferred_element_type=F32)
                if mask is not None:
                    s = jnp.where(mask, s, NEG)
                scores[st][...] = s
                m_tile[st] = jnp.max(s, axis=0, keepdims=True)

            def soft(st, t):
                m_old = m_run[st]
                m_new = jnp.maximum(m_old, m_tile[st])
                m_run[st] = m_new
                alpha = jnp.exp2(m_old - m_new)
                total, pv = 0.0, 0.0
                for i in range(bk // bp):
                    p = jnp.exp2(scores[st][i * bp:(i + 1) * bp, :] - m_new)
                    total = total + jnp.sum(p, axis=0, keepdims=True)
                    v = vb[hl, :, at_rows(t * bk + i * bp, bp)]
                    pv = pv + jnp.dot(v, p.astype(BF16), preferred_element_type=F32)
                l_run[st] = l_run[st] * alpha + total
                accs[st][...] = accs[st][...] * alpha + pv

            m_run[...] = jnp.full_like(m_run, NEG)
            l_run[...] = jnp.zeros_like(l_run)
            acc_a[...] = jnp.zeros_like(acc_a)
            acc_b[...] = jnp.zeros_like(acc_b)
            n_full = g0 // bk

            @pl.when(n_full > 0)
            def _():
                qk(0, 0)

            @pl.when(n_full == 0)
            def _():
                qk(0, 0, k_idx <= q_idx)

            def body(t):
                qk(1, t)
                soft(0, t)
                qk(0, t + 1)
                soft(1, t)

            repeat(n_full - 1, body)

            @pl.when(n_full > 0)
            def _():
                qk(1, n_full - 1)
                soft(0, n_full - 1)
                qk(0, n_full, k_idx <= q_idx)
                soft(1, n_full - 1)

            qk(1, n_full, k_idx <= q_idx + bq)
            soft(0, n_full)
            soft(1, n_full)
            for st in range(2):
                o = accs[st][...] * (1.0 / l_run[st])
                for j in range(group):
                    qb[hl * group + j, pl.ds(r0 + st * bq, bq), :] = o[:, j * bq:(j + 1) * bq].T.astype(BF16)
            for st in range(2):
                rb = half * half_blk + c * 2 + st

                @pl.when(middle)
                def _():
                    o_send(MID, slot, rb).start()

                @pl.when(end | (half == LOW))
                def _():
                    o_send(PARTNER, slot, rb).start()

                o_local(slot, rb).start()

        q_half(LOW)
        kv_relay(LOW, own)
        kv_arrived(LOW, own)

        def when_cp(which, f):
            @pl.when(which)
            def _():
                f()

        def nothing():
            pass

        def start_all(copies):
            for c in copies:
                c.start()

        def second_half():
            when_cp(cp > 0, lambda: kv_relay(HIGH, own))
            when_cp(cp == 3, lambda: w_stage2(SHIFTED))
            q_half(HIGH)
            when_cp(cp == 0, lambda: kv_relay(HIGH, own))
            kv_arrived(HIGH, own)
            when_cp(cp == 2, lambda: w_stage2(SHIFTED))
            when_cp(cp >= 2, lambda: w_stage1(PARTNER))

        def moved_head():
            w_gathered(SHIFTED)
            load_s.start()
            load_s.wait()
            repeat(n_blk, moved_block)
            start_all(w_load_own())
            when_cp(cp >= 2, lambda: w_stage2(PARTNER))
            w_stage1(END)

        def after_e():
            when_cp(cp < 2, lambda: w_stage2(SHIFTED))
            when_cp(cp == 3, lambda: w_stage3(SHIFTED))
            w_stage1(MID)

        def after_f():
            when_cp(cp < 3, lambda: w_stage3(SHIFTED))
            when_cp(cp < 2, lambda: w_stage2(PARTNER))

        def after_g():
            kv_relay(LOW, moved)
            w_stage2(MID)
            kv_arrived(LOW, moved)

        def after_h():
            kv_relay(HIGH, moved)

        def after_i():
            kv_arrived(HIGH, moved)

        def after_j():
            w_stage3(PARTNER)
            w_stage2(END)

        def after_k():
            w_stage3(MID)
            w_stage4(PARTNER)

        def after_l():
            w_stage3(END)
            w_stage4(MID)
            w_stage4(END)

        end_units = (
            (LOW, TOP, FIRST, nothing, nothing),
            (LOW, TOP, SECOND, nothing, nothing),
            (LOW, BOTTOM, FIRST, nothing, nothing),
            (LOW, BOTTOM, SECOND, nothing, lambda: when_cp(cp < 2, lambda: w_stage1(PARTNER))),
            (HIGH, TOP, FIRST, second_half, after_e),
            (HIGH, TOP, SECOND, nothing, after_f),
            (HIGH, BOTTOM, FIRST, moved_head, after_g),
            (LOW, TOP, MOVED, nothing, after_h),
            (LOW, BOTTOM, MOVED, nothing, after_i),
            (HIGH, TOP, MOVED, nothing, after_j),
            (HIGH, BOTTOM, SECOND, nothing, after_k),
            (HIGH, BOTTOM, MOVED, nothing, after_l),
        )

        low_blocks, high_blocks = range(half_blk), range(half_blk, n_blk)
        top = lambda blocks: blocks[:half_blk // 2]
        bottom = lambda blocks: blocks[half_blk // 2:]
        mids, end_first, end_both, end_moved = others[:1], others[1:2], others[1:3], others[3:]
        own_both, own_moved = ends_own[:2], ends_own[2:]

        def middle_high():
            got(here(END), wz_r.at[END])
            z_forward().start()
            kv_relay(HIGH, own)
            q_half(HIGH)
            kv_arrived(HIGH, own)
            start_all(w_load_own())
            for o in (PARTNER, MID, END):
                w_stage1(o)

        middle_units = (
            (LOW, TOP, FIRST, nothing, nothing),
            (LOW, BOTTOM, FIRST, nothing, nothing),
            (HIGH, TOP, FIRST, middle_high, lambda: pass_on(own_both, top(low_blocks))),
            (HIGH, BOTTOM, FIRST, nothing, nothing),
        )

        def unit_loop(s):
            half, c, slot = (
                jnp.where(middle, pick(s, [u[i] for u in middle_units]), pick(s, [u[i] for u in end_units])) for i in range(3))

            def events(i):
                for role, units in ((middle, middle_units), (end, end_units)):
                    for step, what in enumerate(units):
                        if what[i] is not nothing:
                            @pl.when(role & (s == step))
                            def _():
                                what[i]()

            events(-2)
            unit(half, c, slot)
            events(-1)

        repeat(jnp.where(middle, len(middle_units), len(end_units)), unit_loop)

        @pl.when(middle)
        def _():
            pass_on(own_both, bottom(low_blocks))
            pass_on(mids, low_blocks)
            w_stage2(PARTNER)
            pass_on(end_both, top(low_blocks))
            own_outward(top(high_blocks))
            w_stage2(MID)
            w_stage2(END)
            w_stage3(PARTNER)
            pass_on(end_both, bottom(low_blocks))
            w_stage3(MID)
            w_stage4(PARTNER)
            w_stage3(END)
            w_stage4(MID)
            pass_on(own_moved, low_blocks)
            w_stage4(END)
            pass_on(end_moved, low_blocks)
            pass_on(own_both, top(high_blocks))
            pass_on(mids, top(high_blocks))

        def middle_0():
            pass_on(own_moved, top(high_blocks))
            pass_on(end_both, top(high_blocks))

        def middle_1():
            pass_on(end_moved, top(high_blocks))
            own_outward(bottom(high_blocks))
            pass_on(mids, bottom(high_blocks))
            pass_on(own_both, bottom(high_blocks))

        def middle_2():
            pass_on(own_moved, bottom(high_blocks))
            pass_on(end_both, bottom(high_blocks))

        middle_events = (middle_0, middle_1, middle_2, lambda: pass_on(end_moved, bottom(high_blocks)))

        kv_sent()
        for half in range(2):
            for hh in range(kvh):
                k_copy(half, hh).wait()

        def early_landed(rb):
            for_slots(SLOTS, lambda slot: o_local(slot, rb).wait())

            @pl.when(end)
            def _():
                for what in (ends_own[0], others[0]):
                    o_wait(what, rb)

        def late_landed(rb):
            @pl.when(end)
            def _():
                for what in others[1:]:
                    o_wait(what, rb)

        def ob_copy(rb, slot, first, n, i):
            return pltpu.make_async_copy(
                oall_ref.at[pl.ds(first, n), at_rows(rb * blk, blk), :], kb.at[slot, pl.ds(first, n)], ob_sem.at[slot, i])

        def ob_all(rb, slot):
            return ob_copy(rb, slot, 0, heads, 0)

        def o_fetch(rb, slot):
            early_landed(rb)
            late_landed(rb)
            ob_all(rb, slot).start()

        n_y = width // y_cols
        n_h = half_w // y_cols

        def y_copy(rb, n, slot):
            return pltpu.make_async_copy(yb.at[slot], y_ref.at[at_rows(rb * blk, blk), at_rows(n * y_cols, y_cols)], yb_sem.at[slot])

        def product(slot, first, n_heads, n):
            o = jnp.concatenate([kb[slot, first + i] for i in range(n_heads)], axis=1)
            row = first * d if isinstance(first, int) else pl.multiple_of(first * d, gw)
            w = big[n // n_h, pl.ds(row, n_heads * d), at_rows((n % n_h) * y_cols, y_cols)]
            return jnp.dot(o, w, preferred_element_type=F32)

        def x_cols(slot, n):
            n_in = y_cols // d
            return jnp.concatenate([kb[2 + slot, n * n_in + i] for i in range(n_in)], axis=1).astype(F32)

        x_start(0, 0)
        o_fetch(0, 0)
        for c in sum((w_load_other(o) for o in (PARTNER, MID, END)), w_load_own()):
            c.wait()

        n_full_blocks = n_blk - 2

        def out_block(rb):
            slot = rb % 2
            x_wait(slot)
            ob_all(rb, slot).wait()
            x_start(rb + 1, 1 - slot)

            @pl.when(rb + 1 < n_full_blocks)
            def _():
                o_fetch(rb + 1, 1 - slot)

            def out_cols(n):
                ys = n % 2

                @pl.when(rb * n_y + n >= 2)
                def _():
                    y_copy(rb, n, ys).wait()

                yb[ys] = (x_cols(slot, n) + product(slot, 0, heads, n)).astype(BF16)
                y_copy(rb, n, ys).start()

            repeat(n_y, out_cols)
            for i, event in enumerate(middle_events):
                @pl.when(middle & (rb == i))
                def _():
                    event()

        repeat(n_full_blocks, out_block)

        n_late = len(SLOTS) * group
        n_early = heads - n_late
        early = jnp.where(z < 2, 0, n_late)
        late = jnp.where(z < 2, n_early, 0)
        blocks = (n_full_blocks, n_full_blocks + 1)

        def part(n):
            return (at_rows((n % n_h) // 2 * blk, blk), at_rows(n % 2 * y_cols, y_cols))

        def lanes_of(n, half):
            return at_rows(n * 2 * y_cols + half * y_cols, y_cols)

        def early_sum(slot, n):
            return x_cols(slot, n) + product(slot, early, n_early, n)

        def finish(slot, n, total):
            ys = n % 2
            y_copy(blocks[slot], n, ys).wait()
            yb[ys] = (total + product(slot, late, n_late, n)).astype(BF16)
            y_copy(blocks[slot], n, ys).start()

        early_copies = [ob_copy(rb, slot, early, n_early, 0) for slot, rb in enumerate(blocks)]
        late_copies = [ob_copy(rb, slot, late, n_late, 1) for slot, rb in enumerate(blocks)]
        for slot, rb in enumerate(blocks):
            early_landed(rb)
            if slot > 0:
                x_start(rb, slot)
            early_copies[slot].start()
        for i in range(2):
            if i == 0:
                x_wait(0)
                early_copies[0].wait()

            def first_terms(n):
                scores[i][part(n)] = early_sum(0, n)

            repeat(n_h, first_terms, i * n_h)
        x_wait(1)
        early_copies[1].wait()
        half_rows = blk // 2

        def second_terms(n):
            total = early_sum(1, n)
            for i in range(len(SLOTS)):
                term = total.astype(BF16)
                for half in range(2):
                    vb[i, :, lanes_of(n, half)] = term[half * half_rows:(half + 1) * half_rows]
                total = total - term.astype(F32)

        repeat(n_y, second_terms)
        late_landed(blocks[0])
        late_copies[0].start()
        late_copies[0].wait()
        for i in range(2):
            repeat(n_h, lambda n: finish(0, n, scores[i][part(n)]), i * n_h)
        late_landed(blocks[1])
        late_copies[1].start()
        late_copies[1].wait()

        def last_terms(n):
            terms = [jnp.concatenate([vb[i, :, lanes_of(n, half)] for half in range(2)], axis=0).astype(F32) for i in range(len(SLOTS))]
            finish(1, n, (terms[0] + terms[1]) + terms[2])

        repeat(n_y, last_terms)
        for n in (n_y - 2, n_y - 1):
            y_copy(blocks[1], n, n % 2).wait()

        def drain(rb):
            for_slots(SLOTS, lambda slot: o_send(PARTNER, slot, rb).wait_send())

            @pl.when(middle)
            def _():
                o_send(MID, FIRST, rb).wait_send()
                for what in passed:
                    o_pass(what, rb).wait_send()

        repeat(n_blk, drain)
        z_copy(PARTNER).wait_send()
        z_copy(MID).wait_send()

        @pl.when(middle)
        def _():
            z_copy(END).wait_send()
            z_forward().wait_send()
            for i in range(len(s_parts)):
                s_copy(i).wait_send()

        def w_sent(o):
            for kind in kinds:
                if (kind, o) != (X_TO_Y, SHIFTED):
                    w_send(kind, o).wait_send()
                c_send(kind, o).wait_send()

        for o in (PARTNER, MID, END):
            w_sent(o)

        @pl.when(end)
        def _():
            w_sent(SHIFTED)

    any_spec = pl.BlockSpec(memory_space=pl.ANY)
    vmem_spec = pl.BlockSpec(memory_space=pltpu.VMEM)
    dma = pltpu.SemaphoreType.DMA
    outs = pl.pallas_call(
        kernel,
        in_specs=[any_spec, vmem_spec] + [any_spec] * 4 + [pl.BlockSpec(memory_space=pltpu.SMEM), vmem_spec],
        out_specs=[any_spec] * 6,
        out_shape=[
            jax.ShapeDtypeStruct((rows, width), BF16),
            jax.ShapeDtypeStruct((n_blk, blk, kvh * d), BF16),
            jax.ShapeDtypeStruct((rows, kvh * d), BF16),
            jax.ShapeDtypeStruct((heads, rows, d), BF16),
            jax.ShapeDtypeStruct((width, width), BF16),
            jax.ShapeDtypeStruct((width, s_cols), BF16),
        ],
        scratch_shapes=[
            pltpu.VMEM((2, width, half_w), BF16),
            pltpu.VMEM((4, n_lane, blk, d), BF16),
            pltpu.VMEM((3, d, n_seg * seg), BF16),
            pltpu.VMEM((3 * group, rows, d), BF16),
            pltpu.VMEM((rows, d), F32),
            pltpu.VMEM((blk, kvh * d), BF16),
            pltpu.VMEM((2, 2 * d, cols), BF16),
            pltpu.VMEM((bk, cols), F32),
            pltpu.VMEM((bk, cols), F32),
            pltpu.VMEM((d, cols), F32),
            pltpu.VMEM((d, cols), F32),
            pltpu.VMEM((2, 1, cols), F32),
            pltpu.VMEM((2, 1, cols), F32),
            pltpu.VMEM((2, 1, cols), F32),
            pltpu.VMEM((2, blk, y_cols), BF16),
            dma((4,)), dma((2,)), dma((1,)), dma((2, kvh)),
            dma((3, 12)), dma((3, 12)), dma((4,)), dma((3,)), dma((3,)), dma((3,)), dma((4, 4)), dma((4, 4)), dma((4, 4)), dma((4, 4)),
            dma((2, n_blk, 3)), dma((n_blk, 3)), dma((n_blk, n_groups)), dma((n_blk, 7)), dma((2, 2)), dma((2,)), dma((4, 2)),
        ],
        compiler_params=pltpu.CompilerParams(collective_id=0, has_side_effects=True, vmem_limit_bytes=67043328),
        name="sublayer",
    )(x, gain, w_q, w_k, w_v, w_o, positions, freqs)
    return outs[0], outs[1], outs[2]


def solution(mesh):
    def device_fn(x_in, positions, norm_gain, w_q, w_k, w_v, w_o):
        kv_heads = w_k.shape[1] // HEAD_DIM
        freqs = rope_freqs()
        freqs = jnp.concatenate([freqs, freqs])[None, :]
        gain = norm_gain.reshape(-1, HEAD_DIM)
        y, keys, values = layer(x_in, gain, w_q, w_k, w_v, w_o, positions, freqs)
        shape = (x_in.shape[0], kv_heads, HEAD_DIM)
        return y, keys.reshape(shape), values.reshape(shape)

    row_spec = P(('dp', 'cp'), None)
    cache_spec = P(('dp', 'cp'), 'tp', None)
    return jax.shard_map(device_fn, mesh=mesh, in_specs=(row_spec, P(('dp', 'cp')), P(None), P(None, 'tp'), P(None, 'tp'), P(None, 'tp'), P('tp', None)), out_specs=(row_spec, cache_spec, cache_spec), check_vma=False)
```

```python
import math
import jax
import jax.numpy as jnp
from jax import lax
from jax.experimental import pallas as pl
from jax.experimental.pallas import tpu as pltpu
from jax.sharding import PartitionSpec as P

HEAD_DIM = 128
NORM_EPS = 1e-5
NEG = -0.7 * float(jnp.finfo(jnp.float32).max)
SCALE2 = (1.0 / math.sqrt(HEAD_DIM)) * math.log2(math.e)
BF16 = jnp.bfloat16
F32 = jnp.float32
MESH = pl.DeviceIdType.MESH
LOW, HIGH = range(2)
TOP, BOTTOM = range(2)
FIRST, SECOND, MOVED = SLOTS = range(3)
PARTNER, MID, END, SHIFTED = PIECES = range(4)


def rope_freqs():
    exponent = jnp.arange(0, HEAD_DIM, 2).astype(jnp.float32) / HEAD_DIM
    base_freq = 1.0 / (500000.0 ** exponent)
    wave_len = 2.0 * math.pi / base_freq
    smooth = (8192.0 / wave_len - 1.0) / 3.0
    blended = (1.0 - smooth) * base_freq / 8.0 + smooth * base_freq
    return jnp.where(wave_len < 2048.0, base_freq, jnp.where(wave_len > 8192.0, base_freq / 8.0, blended))


def repeat(n, step, first=0):
    lax.fori_loop(first, first + n, lambda i, carry: (step(i), carry)[1], 0)


def pick(i, values):
    out = values[-1]
    for at, value in enumerate(values[:-1]):
        out = jnp.where(i == at, value, out)
    return out


def rotate(vec_bf, cos, sin):
    vec = vec_bf.astype(F32)
    return (vec * cos + pltpu.roll(vec, HEAD_DIM // 2, axis=1) * sin).astype(BF16)


def layer(x, gain, w_q, w_k, w_v, w_o, positions, freqs):
    rows, width = x.shape
    seg = rows // 2
    d = HEAD_DIM
    kvh = w_k.shape[1] // d
    group = w_q.shape[1] // w_k.shape[1]
    gw = group * d
    qw = kvh * gw
    n_tp = width // qw
    n_groups = n_tp * kvh
    heads = n_groups * group
    n_seg = 8
    blk = 256
    n_blk = rows // blk
    n_lane = width // d
    half_w = width // 2
    bq, bk, bp = 256, 512, 256
    cols = bq * group
    unit_rows = 2 * bq
    w_slice = qw // 8
    s_slice = width // 8
    s_cols = gw + 2 * d
    s_at = qw
    y_cols = 512
    nr = 128
    assert n_blk == n_groups and heads == n_lane

    def kernel(x_ref, gain_ref, wq_ref, wk_ref, wv_ref, wo_ref, pos_ref, freq_ref,
               y_ref, k_ref, v_ref, oall_ref, wall_ref, wsx_ref,
               big, kb, vb, qb, csb, vst, qt, s_a, s_b, acc_a, acc_b, m_run, l_run, m_tile, yb,
               ld_sem, x_sem, vst_sem, kout_sem,
               kv_s, kv_r, wz_s, wz_r, sz_s, sz_r, wp_s, wp_r, wc_s, wc_r,
               o_s, o_l, o_r, f_s, ob_sem, yb_sem, wl_sem):
        dp, z, cp = lax.axis_index("dp"), lax.axis_index("tp"), lax.axis_index("cp")
        cy, cc = cp // 2, cp % 2
        x_nb = {"dp": 1 - dp}
        y_nb = {"cp": (1 - cy) * 2 + cc}
        c_nb = {"cp": cy * 2 + 1 - cc}

        middle = (z == 1) | (z == 2)
        end = jnp.logical_not(middle)
        partner = z + 1 - 2 * (z % 2)
        other_mid = jnp.where(z < 2, 2, 1)
        other_end = jnp.where(z < 2, 3, 0)
        sources = (z, partner, other_mid, other_end)
        slot_out = jnp.where(middle, MID, END)
        keep = jnp.where(z == 1, SECOND, FIRST)
        head_at = lambda slot: jnp.where(middle, keep, slot)
        last_z = n_tp - 1

        def group_of(zz, slot):
            at_far_end = n_groups - len(SLOTS) + (slot + 1) % len(SLOTS) if isinstance(slot, int) else (
                n_groups - len(SLOTS) + lax.rem(slot + 1, len(SLOTS)))
            return jnp.where(zz == 0, slot, jnp.where(zz == last_z, at_far_end, zz + kvh))

        source = lambda piece: sources[piece + 1]

        def remote(src, dst, ss, rs, dev):
            return pltpu.make_async_remote_copy(src_ref=src, dst_ref=dst, send_sem=ss, recv_sem=rs, device_id=dev, device_id_type=MESH)

        def got(region, rs):
            remote(region, region, rs, rs, x_nb).wait_recv()

        def at_rows(n, size):
            return pl.ds(pl.multiple_of(n, size), size)

        barrier = pltpu.get_barrier_semaphore()
        for dev in (x_nb, y_nb, c_nb, {"tp": partner}, {"tp": other_mid}, {"tp": other_end}):
            pl.semaphore_signal(barrier, inc=1, device_id=dev, device_id_type=MESH)
        pl.semaphore_wait(barrier, 6)

        place = dp * 4 + cp

        def place_of(fx, fy, fc):
            px = 1 - dp if fx else dp
            py = 1 - cy if fy else cy
            pc = 1 - cc if fc else cc
            return px * 4 + py * 2 + pc

        def piece(o, fx, fy, fc, part=None):
            size = s_slice if o == SHIFTED else w_slice
            base = place_of(fx, fy, fc) * size
            if o != SHIFTED:
                base = base + source(o) * qw
            n = size if part is None else size // 2
            base = pl.multiple_of(base + (n if part == BOTTOM else 0), n)
            return (wsx_ref if o == SHIFTED else wall_ref).at[pl.ds(base, n), :]

        here = lambda o: piece(o, 0, 0, 0)
        next_x = lambda o, part=None: piece(o, 1, 0, 0, part)
        next_y = lambda o, part=None: piece(o, 0, 1, 0, part)
        next_xy = lambda o, part=None: piece(o, 1, 1, 0, part)
        at_core = lambda o: (here(o), next_x(o), next_y(o), next_xy(o))

        def z_copy(o):
            src = wo_ref.at[at_rows(place * w_slice, w_slice), :]
            dst = wall_ref.at[at_rows(z * qw + place * w_slice, w_slice), :]
            return remote(src, dst, wz_s.at[o], wz_r.at[PARTNER if o == PARTNER else slot_out], {"tp": source(o)})

        def z_forward():
            return remote(here(END), here(END), wz_s.at[SHIFTED], wz_r.at[END], {"tp": partner})

        s_parts = ((wq_ref, 0, gw), (wk_ref, gw, d), (wv_ref, gw + d, d))

        def s_dst(i):
            _, lane, n = s_parts[i]
            return wsx_ref.at[at_rows(place * s_slice, s_slice), pl.ds(lane, n)]

        def s_copy(i):
            ref, _, n = s_parts[i]
            src = ref.at[at_rows(place * s_slice, s_slice), at_rows((1 - keep) * n, n)]
            return remote(src, s_dst(i), sz_s.at[i], sz_r.at[i], {"tp": partner})

        OWN_X, OWN_Y, X_TO_Y, Y_TO_X = kinds = range(4)

        def w_send(kind, o):
            if kind == OWN_X:
                region, dev = here(o), x_nb
            elif kind == OWN_Y:
                region, dev = here(o), y_nb
            elif kind == X_TO_Y:
                region, dev = next_x(o, TOP), y_nb
            else:
                region, dev = next_y(o, None if o == SHIFTED else BOTTOM), x_nb
            return remote(region, region, wp_s.at[kind, o], wp_r.at[kind, o], dev)

        def c_send(i, o):
            region = at_core(o)[i]
            return remote(region, region, wc_s.at[i, o], wc_r.at[i, o], c_nb)

        def w_stage1(o):
            if o == SHIFTED:
                for i in range(len(s_parts)):
                    got(s_dst(i), sz_r.at[i])
            elif o != END:
                got(here(o), wz_r.at[o])
            else:
                @pl.when(end)
                def _():
                    got(here(o), wz_r.at[o])

            w_send(OWN_X, o).start()
            w_send(OWN_Y, o).start()
            c_send(0, o).start()

        def w_stage2(o):
            got(next_x(o), wp_r.at[OWN_X, o])
            if o != SHIFTED:
                w_send(X_TO_Y, o).start()
            c_send(1, o).start()
            got(next_y(o), wp_r.at[OWN_Y, o])
            w_send(Y_TO_X, o).start()
            c_send(2, o).start()

        def w_stage3(o):
            if o != SHIFTED:
                got(next_xy(o, TOP), wp_r.at[X_TO_Y, o])
            got(next_xy(o, None if o == SHIFTED else BOTTOM), wp_r.at[Y_TO_X, o])
            c_send(3, o).start()

        def w_gathered(o):
            for i, (fx, fy) in enumerate(((0, 0), (1, 0), (0, 1), (1, 1))):
                got(piece(o, fx, fy, 1), wc_r.at[i, o])

        def w_load(zs, src, i):
            return [pltpu.make_async_copy(
                src.at[:, pl.ds(n * half_w, half_w)], big.at[n, at_rows(zs * qw, qw), :], wl_sem.at[i, n]) for n in range(2)]

        def w_load_own():
            return w_load(z, wo_ref, SHIFTED)

        def w_load_other(o):
            return w_load(source(o), wall_ref.at[at_rows(source(o) * qw, qw), :], o)

        def w_stage4(o):
            w_gathered(o)
            for c in w_load_other(o):
                c.start()

        def load_weights(i, ref, lane, n):
            return pltpu.make_async_copy(ref, big.at[0, :, pl.ds(lane, n)], ld_sem.at[i])

        load_q, load_k, load_v, load_s = (load_weights(i, *args) for i, args in enumerate((
            (wq_ref, 0, qw), (wk_ref, qw, kvh * d), (wv_ref, qw + kvh * d, kvh * d), (wsx_ref, s_at, s_cols))))

        def x_start(b, slot):
            for i in range(n_lane):
                pltpu.make_async_copy(x_ref.at[at_rows(b * blk, blk), pl.ds(i * d, d)], kb.at[2 + slot, i], x_sem.at[slot]).start()

        def x_wait(slot):
            pltpu.make_async_copy(kb.at[2 + slot], kb.at[2 + slot], x_sem.at[slot]).wait()

        def v_copy(b):
            return pltpu.make_async_copy(vst, v_ref.at[at_rows(b * blk, blk), :], vst_sem.at[0])

        low_lanes = lax.broadcasted_iota(jnp.int32, (blk, d), 1) < d // 2

        def make_angles(b):
            first = pos_ref[b * blk]
            pos = (lax.broadcasted_iota(jnp.int32, (blk, d), 0) + first).astype(F32)
            angle = pos * freq_ref[...]
            csb[at_rows(b * blk, blk), :] = jnp.where(low_lanes, jnp.cos(angle), jnp.sin(angle))

        def cos_sin(b):
            both = csb[at_rows(b * blk, blk), :]
            turned = pltpu.roll(both, d // 2, axis=1)
            return jnp.where(low_lanes, both, turned), jnp.where(low_lanes, -turned, both)

        x_start(0, 0)
        load_k.start()
        load_v.start()
        load_q.start()

        @pl.when(middle)
        def _():
            for i in range(len(s_parts)):
                s_copy(i).start()

        z_copy(PARTNER).start()
        z_copy(MID).start()

        @pl.when(middle)
        def _():
            z_copy(END).start()

        seg_at = lambda half, c: jnp.where(half == LOW, c, n_seg - 1 - c) * seg
        y_cp = (1 - cy) * 2 + cc
        c_cp = cy * 2 + 1 - cc
        yc_cp = (1 - cy) * 2 + 1 - cc

        def kv_region(half, c, which, slot):
            at = pl.multiple_of(seg_at(half, c), seg)
            h = head_at(slot)
            return kb.at[h, pl.ds(at // blk, seg // blk)] if which == 0 else vb.at[h, :, pl.ds(at, seg)]

        TO_CORE, TO_Y, Y_TO_CORE = kv_kinds = range(3)
        kv_both = range(2)
        n_kv = len(kv_both) * len(SLOTS)
        kv_at = lambda half, which, slot: half * n_kv + which * len(SLOTS) + slot

        def kv_send(kind, half, which, slot):
            region = kv_region(half, y_cp if kind == Y_TO_CORE else cp, which, slot)
            i = kv_at(half, which, slot)
            return remote(region, region, kv_s.at[kind, i], kv_r.at[kind, i], y_nb if kind == TO_Y else c_nb)

        def for_slots(slots, f):
            for slot in slots:
                if slot == FIRST:
                    f(slot)
                else:
                    @pl.when(end)
                    def _():
                        f(slot)

        own = (FIRST, SECOND)
        moved = (MOVED,)

        def kv_start(half, slots):
            def f(slot):
                for which in kv_both:
                    kv_send(TO_Y, half, which, slot).start()
                    kv_send(TO_CORE, half, which, slot).start()
            for_slots(slots, f)

        def kv_relay(half, slots):
            def f(slot):
                for which in kv_both:
                    got(kv_region(half, y_cp, which, slot), kv_r.at[TO_Y, kv_at(half, which, slot)])
                    kv_send(Y_TO_CORE, half, which, slot).start()
            for_slots(slots, f)

        def kv_arrived(half, slots):
            def f(slot):
                for which in kv_both:
                    i = kv_at(half, which, slot)
                    got(kv_region(half, c_cp, which, slot), kv_r.at[TO_CORE, i])
                    got(kv_region(half, yc_cp, which, slot), kv_r.at[Y_TO_CORE, i])
            for_slots(slots, f)

        def kv_sent():
            def f(slot):
                for half in (LOW, HIGH):
                    for which in kv_both:
                        for kind in kv_kinds:
                            kv_send(kind, half, which, slot).wait_send()
            for_slots(SLOTS, f)

        def k_copy(half, hh):
            at = pl.multiple_of(seg_at(half, cp), seg)
            n = seg // blk
            return pltpu.make_async_copy(kb.at[hh, pl.ds(at // blk, n)], k_ref.at[pl.ds(half * n, n), :, pl.ds(hh * d, d)], kout_sem.at[half, hh])

        def h_rows(b):
            h0 = big[1, at_rows(b * blk, blk), :]
            h1 = big[1, at_rows(rows + b * blk, blk), :]
            return jnp.concatenate([h0, h1], axis=1)

        load_k.wait()
        load_v.wait()

        half_blk = n_blk // 2

        def at_half_end(b, f):
            for half in (LOW, HIGH):
                @pl.when(b == half * half_blk + half_blk - 1)
                def _():
                    f(half)

        def kv_rows(b):
            return pl.multiple_of(seg_at(b // half_blk, cp) + lax.rem(b, half_blk) * blk, blk)

        def kv_block(b):
            slot = b % 2
            x_wait(slot)

            @pl.when(b + 1 < n_blk)
            def _():
                x_start(b + 1, 1 - slot)

            def norm_rows(i):
                at = at_rows(i * nr, nr)
                square = 0.0
                for j in range(n_lane):
                    xf = kb[2 + slot, j, at, :].astype(F32)
                    square = square + xf * xf
                inv = lax.rsqrt(jnp.sum(square, axis=-1, keepdims=True) / width + NORM_EPS)
                for j in range(n_lane):
                    xf = kb[2 + slot, j, at, :].astype(F32)
                    h = ((xf * inv) * gain_ref[j:j + 1, :].astype(F32)).astype(BF16)
                    row = b * blk + (0 if j * d < half_w else rows) + i * nr
                    lane = (j * d) % half_w
                    big[1, at_rows(row, nr), lane:lane + d] = h

            repeat(blk // nr, norm_rows)
            make_angles(b)
            kv = jnp.dot(h_rows(b), big[0, :, qw:qw + 2 * kvh * d], preferred_element_type=F32).astype(BF16)
            cos, sin = cos_sin(b)
            at = kv_rows(b)

            @pl.when(b > 0)
            def _():
                v_copy(b - 1).wait()

            for hh in range(kvh):
                kb[hh, at // blk] = rotate(kv[:, hh * d:(hh + 1) * d], cos, sin)
                vb[hh, :, pl.ds(at, blk)] = kv[:, (kvh + hh) * d:(kvh + hh + 1) * d].T
            vst[...] = kv[:, kvh * d:]
            v_copy(b).start()

            def send(half):
                kv_start(half, own)
                for hh in range(kvh):
                    k_copy(half, hh).start()

            at_half_end(b, send)

        repeat(n_blk, kv_block)
        v_copy(n_blk - 1).wait()
        load_q.wait()

        @pl.when(end)
        def _():
            w_stage1(SHIFTED)

        def q_half(half):
            def q_block(b):
                cos, sin = cos_sin(b)

                def project(i):
                    head = head_at(i)
                    q = jnp.dot(h_rows(b), big[0, :, at_rows(head * gw, gw)], preferred_element_type=F32).astype(BF16)
                    for j in range(group):
                        qb[head * group + j, at_rows(b * blk, blk), :] = rotate(q[:, j * d:(j + 1) * d], cos, sin)

                repeat(jnp.where(middle, 1, kvh), project)

            repeat(half_blk, q_block, half * half_blk)

        def moved_block(b):
            cos, sin = cos_sin(b)
            qkv = jnp.dot(h_rows(b), big[0, :, s_at:s_at + s_cols], preferred_element_type=F32).astype(BF16)
            for j in range(group):
                qb[MOVED * group + j, at_rows(b * blk, blk), :] = rotate(qkv[:, j * d:(j + 1) * d], cos, sin)
            at = kv_rows(b)
            kb[MOVED, at // blk] = rotate(qkv[:, gw:gw + d], cos, sin)
            vb[MOVED, :, pl.ds(at, blk)] = qkv[:, gw + d:].T
            at_half_end(b, lambda half: kv_start(half, moved))

        def o_region(g, rb):
            return oall_ref.at[pl.ds(g * group, group), at_rows(rb * blk, blk), :]

        def o_own(slot, rb):
            return qb.at[pl.ds(head_at(slot) * group, group), at_rows(rb * blk, blk), :]

        def o_local(slot, rb):
            return pltpu.make_async_copy(o_own(slot, rb), o_region(group_of(z, slot), rb), o_l.at[rb, slot])

        def o_send(to, slot, rb):
            g = group_of(z, slot)
            return remote(o_own(slot, rb), o_region(g, rb), o_s.at[to, rb, slot], o_r.at[rb, g], {"tp": source(to)})

        others = ((MID, FIRST), (END, FIRST), (END, SECOND), (END, MOVED))
        ends_own = ((PARTNER, FIRST), (PARTNER, SECOND), (PARTNER, MOVED))
        passed = others + ends_own

        def o_pass(what, rb):
            g = group_of(source(what[0]), what[1])
            region = o_region(g, rb)
            to = {"tp": partner if what in others else other_mid}
            return remote(region, region, f_s.at[rb, passed.index(what)], o_r.at[rb, g], to)

        def o_wait(what, rb):
            g = group_of(source(what[0]), what[1])
            got(o_region(g, rb), o_r.at[rb, g])

        def pass_on(what, blocks):
            def step(rb):
                for item in what:
                    o_wait(item, rb)
                    o_pass(item, rb).start()

            repeat(len(blocks), step, blocks[0])

        def own_outward(blocks):
            repeat(len(blocks), lambda rb: o_send(PARTNER, FIRST, rb).start(), blocks[0])

        scores = (s_a, s_b)
        accs = (acc_a, acc_b)

        def unit(half, c, slot):
            hl = head_at(slot)
            r0 = pl.multiple_of(half * seg + c * unit_rows, unit_rows)
            g0 = seg_at(half, cp) + c * unit_rows
            for st in range(2):
                for j in range(group):
                    qs = qb[hl * group + j, pl.ds(r0 + st * bq, bq), :].T.astype(F32) * SCALE2
                    top = qs.astype(BF16)
                    span = slice(j * bq, (j + 1) * bq)
                    qt[st, 0:d, span] = top
                    qt[st, d:2 * d, span] = (qs - top.astype(F32)).astype(BF16)
            k_idx = lax.broadcasted_iota(jnp.int32, (bk, cols), 0)
            q_idx = lax.broadcasted_iota(jnp.int32, (bk, cols), 1) % bq

            def qk(st, t, mask=None):
                kt = kb[hl, pl.ds(t * (bk // blk), bk // blk)].reshape(bk, d)
                s = jnp.dot(jnp.concatenate([kt, kt], axis=1), qt[st], preferred_element_type=F32)
                if mask is not None:
                    s = jnp.where(mask, s, NEG)
                scores[st][...] = s
                m_tile[st] = jnp.max(s, axis=0, keepdims=True)

            def soft(st, t):
                m_old = m_run[st]
                m_new = jnp.maximum(m_old, m_tile[st])
                m_run[st] = m_new
                alpha = jnp.exp2(m_old - m_new)
                total, pv = 0.0, 0.0
                for i in range(bk // bp):
                    p = jnp.exp2(scores[st][i * bp:(i + 1) * bp, :] - m_new)
                    total = total + jnp.sum(p, axis=0, keepdims=True)
                    v = vb[hl, :, at_rows(t * bk + i * bp, bp)]
                    pv = pv + jnp.dot(v, p.astype(BF16), preferred_element_type=F32)
                l_run[st] = l_run[st] * alpha + total
                accs[st][...] = accs[st][...] * alpha + pv

            m_run[...] = jnp.full_like(m_run, NEG)
            l_run[...] = jnp.zeros_like(l_run)
            acc_a[...] = jnp.zeros_like(acc_a)
            acc_b[...] = jnp.zeros_like(acc_b)
            n_full = g0 // bk

            qk(0, 0, k_idx <= q_idx + g0)

            def body(t):
                qk(1, t)
                soft(0, t)
                qk(0, t + 1)
                soft(1, t)

            repeat(n_full - 1, body)

            def finish_unit(tail):
                if tail:
                    qk(1, n_full - 1)
                    soft(0, n_full - 1)
                    qk(0, n_full, k_idx <= q_idx)
                    soft(1, n_full - 1)
                qk(1, n_full, k_idx <= q_idx + bq)
                soft(0, n_full)
                soft(1, n_full)
                for st in range(2):
                    o = accs[st][...] * (1.0 / l_run[st])
                    for j in range(group):
                        qb[hl * group + j, pl.ds(r0 + st * bq, bq), :] = o[:, j * bq:(j + 1) * bq].T.astype(BF16)

            @pl.when(n_full > 0)
            def _():
                finish_unit(True)

            @pl.when(n_full == 0)
            def _():
                finish_unit(False)

            for st in range(2):
                rb = half * half_blk + c * 2 + st

                @pl.when(middle)
                def _():
                    o_send(MID, slot, rb).start()

                @pl.when(end | (half == LOW))
                def _():
                    o_send(PARTNER, slot, rb).start()

                o_local(slot, rb).start()

        q_half(LOW)
        kv_relay(LOW, own)
        kv_arrived(LOW, own)

        def when_cp(which, f):
            @pl.when(which)
            def _():
                f()

        def nothing():
            pass

        def start_all(copies):
            for c in copies:
                c.start()

        def second_half():
            when_cp(cp > 0, lambda: kv_relay(HIGH, own))
            when_cp(cp == 3, lambda: w_stage2(SHIFTED))
            q_half(HIGH)
            when_cp(cp == 0, lambda: kv_relay(HIGH, own))
            kv_arrived(HIGH, own)
            when_cp(cp == 2, lambda: w_stage2(SHIFTED))
            when_cp(cp >= 2, lambda: w_stage1(PARTNER))

        def moved_head():
            w_gathered(SHIFTED)
            load_s.start()
            load_s.wait()
            repeat(n_blk, moved_block)
            start_all(w_load_own())
            when_cp(cp >= 2, lambda: w_stage2(PARTNER))
            w_stage1(END)

        def after_e():
            when_cp(cp < 2, lambda: w_stage2(SHIFTED))
            when_cp(cp == 3, lambda: w_stage3(SHIFTED))
            w_stage1(MID)

        def after_f():
            when_cp(cp < 3, lambda: w_stage3(SHIFTED))
            when_cp(cp < 2, lambda: w_stage2(PARTNER))

        def after_g():
            kv_relay(LOW, moved)
            w_stage2(MID)
            kv_arrived(LOW, moved)

        def after_h():
            kv_relay(HIGH, moved)

        def after_i():
            kv_arrived(HIGH, moved)

        def after_j():
            w_stage3(PARTNER)
            w_stage2(END)

        def after_k():
            w_stage3(MID)
            w_stage3(END)
            w_stage4(PARTNER)

        def after_l():
            w_stage4(MID)
            w_stage4(END)

        end_units = (
            (LOW, TOP, FIRST, nothing, nothing),
            (LOW, TOP, SECOND, nothing, nothing),
            (LOW, BOTTOM, FIRST, nothing, nothing),
            (LOW, BOTTOM, SECOND, nothing, lambda: when_cp(cp < 2, lambda: w_stage1(PARTNER))),
            (HIGH, TOP, FIRST, second_half, after_e),
            (HIGH, TOP, SECOND, nothing, after_f),
            (HIGH, BOTTOM, FIRST, moved_head, after_g),
            (LOW, TOP, MOVED, nothing, after_h),
            (LOW, BOTTOM, MOVED, nothing, after_i),
            (HIGH, TOP, MOVED, nothing, after_j),
            (HIGH, BOTTOM, SECOND, nothing, after_k),
            (HIGH, BOTTOM, MOVED, nothing, after_l),
        )

        low_blocks, high_blocks = range(half_blk), range(half_blk, n_blk)
        top = lambda blocks: blocks[:half_blk // 2]
        bottom = lambda blocks: blocks[half_blk // 2:]
        mids, end_first, end_both, end_moved = others[:1], others[1:2], others[1:3], others[3:]
        own_both, own_moved = ends_own[:2], ends_own[2:]

        def middle_high():
            got(here(END), wz_r.at[END])
            z_forward().start()
            kv_relay(HIGH, own)
            q_half(HIGH)
            kv_arrived(HIGH, own)
            start_all(w_load_own())
            for o in (PARTNER, MID, END):
                w_stage1(o)

        middle_units = (
            (LOW, TOP, FIRST, nothing, nothing),
            (LOW, BOTTOM, FIRST, nothing, nothing),
            (HIGH, TOP, FIRST, middle_high, lambda: pass_on(own_both, top(low_blocks))),
            (HIGH, BOTTOM, FIRST, nothing, nothing),
        )

        def unit_loop(s):
            half, c, slot = (
                jnp.where(middle, pick(s, [u[i] for u in middle_units]), pick(s, [u[i] for u in end_units])) for i in range(3))

            def events(i):
                for role, units in ((middle, middle_units), (end, end_units)):
                    for step, what in enumerate(units):
                        if what[i] is not nothing:
                            @pl.when(role & (s == step))
                            def _():
                                what[i]()

            events(-2)
            unit(half, c, slot)
            events(-1)

        repeat(jnp.where(middle, len(middle_units), len(end_units)), unit_loop)

        @pl.when(middle)
        def _():
            pass_on(own_both, bottom(low_blocks))
            pass_on(mids, low_blocks)
            w_stage2(PARTNER)
            pass_on(end_both, top(low_blocks))
            own_outward(top(high_blocks))
            w_stage2(MID)
            w_stage2(END)
            w_stage3(PARTNER)
            pass_on(end_both, bottom(low_blocks))
            w_stage3(MID)
            w_stage4(PARTNER)
            w_stage3(END)
            w_stage4(MID)
            pass_on(own_moved, low_blocks)
            w_stage4(END)
            pass_on(end_moved, low_blocks)
            pass_on(own_both, top(high_blocks))
            pass_on(mids, top(high_blocks))

        def middle_0():
            pass_on(own_moved, top(high_blocks))
            pass_on(end_both, top(high_blocks))

        def middle_1():
            pass_on(end_moved, top(high_blocks))
            own_outward(bottom(high_blocks))
            pass_on(mids, bottom(high_blocks))
            pass_on(own_both, bottom(high_blocks))

        def middle_2():
            pass_on(own_moved, bottom(high_blocks))
            pass_on(end_both, bottom(high_blocks))

        middle_events = (middle_0, middle_1, middle_2, lambda: pass_on(end_moved, bottom(high_blocks)))

        kv_sent()
        for half in range(2):
            for hh in range(kvh):
                k_copy(half, hh).wait()

        def early_landed(rb):
            for_slots(SLOTS, lambda slot: o_local(slot, rb).wait())

            @pl.when(end)
            def _():
                for what in (ends_own[0], others[0]):
                    o_wait(what, rb)

        def late_landed(rb):
            @pl.when(end)
            def _():
                for what in others[1:]:
                    o_wait(what, rb)

        def ob_copy(rb, slot, first, n, i):
            return pltpu.make_async_copy(
                oall_ref.at[pl.ds(first, n), at_rows(rb * blk, blk), :], kb.at[slot, pl.ds(first, n)], ob_sem.at[slot, i])

        def ob_all(rb, slot):
            return ob_copy(rb, slot, 0, heads, 0)

        def o_fetch(rb, slot):
            early_landed(rb)
            late_landed(rb)
            ob_all(rb, slot).start()

        n_y = width // y_cols
        n_h = half_w // y_cols

        def y_copy(rb, n, slot):
            return pltpu.make_async_copy(yb.at[slot], y_ref.at[at_rows(rb * blk, blk), at_rows(n * y_cols, y_cols)], yb_sem.at[slot])

        def product(slot, first, n_heads, n):
            o = jnp.concatenate([kb[slot, first + i] for i in range(n_heads)], axis=1)
            row = first * d if isinstance(first, int) else pl.multiple_of(first * d, gw)
            w = big[n // n_h, pl.ds(row, n_heads * d), at_rows((n % n_h) * y_cols, y_cols)]
            return jnp.dot(o, w, preferred_element_type=F32)

        def x_cols(slot, n):
            n_in = y_cols // d
            return jnp.concatenate([kb[2 + slot, n * n_in + i] for i in range(n_in)], axis=1).astype(F32)

        x_start(0, 0)
        o_fetch(0, 0)
        for c in sum((w_load_other(o) for o in (PARTNER, MID, END)), w_load_own()):
            c.wait()

        n_full_blocks = n_blk - 2

        def out_block(rb):
            slot = rb % 2
            x_wait(slot)
            ob_all(rb, slot).wait()
            x_start(rb + 1, 1 - slot)

            @pl.when(rb + 1 < n_full_blocks)
            def _():
                o_fetch(rb + 1, 1 - slot)

            def out_cols(n):
                ys = n % 2

                @pl.when(rb * n_y + n >= 2)
                def _():
                    y_copy(rb, n, ys).wait()

                yb[ys] = (x_cols(slot, n) + product(slot, 0, heads, n)).astype(BF16)
                y_copy(rb, n, ys).start()

            repeat(n_y, out_cols)
            for i, event in enumerate(middle_events):
                @pl.when(middle & (rb == i))
                def _():
                    event()

        repeat(n_full_blocks, out_block)

        n_late = len(SLOTS) * group
        n_early = heads - n_late
        early = jnp.where(z < 2, 0, n_late)
        late = jnp.where(z < 2, n_early, 0)
        blocks = (n_full_blocks, n_full_blocks + 1)

        def part(n):
            return (at_rows((n % n_h) // 2 * blk, blk), at_rows(n % 2 * y_cols, y_cols))

        def lanes_of(n, half):
            return at_rows(n * 2 * y_cols + half * y_cols, y_cols)

        def early_sum(slot, n):
            return x_cols(slot, n) + product(slot, early, n_early, n)

        def finish(slot, n, total):
            ys = n % 2
            y_copy(blocks[slot], n, ys).wait()
            yb[ys] = (total + product(slot, late, n_late, n)).astype(BF16)
            y_copy(blocks[slot], n, ys).start()

        early_copies = [ob_copy(rb, slot, early, n_early, 0) for slot, rb in enumerate(blocks)]
        late_copies = [ob_copy(rb, slot, late, n_late, 1) for slot, rb in enumerate(blocks)]
        for slot, rb in enumerate(blocks):
            early_landed(rb)
            if slot > 0:
                x_start(rb, slot)
            early_copies[slot].start()
        for i in range(2):
            if i == 0:
                x_wait(0)
                early_copies[0].wait()

            def first_terms(n):
                scores[i][part(n)] = early_sum(0, n)

            repeat(n_h, first_terms, i * n_h)
        x_wait(1)
        early_copies[1].wait()
        half_rows = blk // 2

        def second_terms(n):
            total = early_sum(1, n)
            for i in range(len(SLOTS)):
                term = total.astype(BF16)
                for half in range(2):
                    vb[i, :, lanes_of(n, half)] = term[half * half_rows:(half + 1) * half_rows]
                total = total - term.astype(F32)

        repeat(n_y, second_terms)
        late_landed(blocks[0])
        late_copies[0].start()
        late_copies[0].wait()
        for i in range(2):
            repeat(n_h, lambda n: finish(0, n, scores[i][part(n)]), i * n_h)
        late_landed(blocks[1])
        late_copies[1].start()
        late_copies[1].wait()

        def last_terms(n):
            terms = [jnp.concatenate([vb[i, :, lanes_of(n, half)] for half in range(2)], axis=0).astype(F32) for i in range(len(SLOTS))]
            finish(1, n, (terms[0] + terms[1]) + terms[2])

        repeat(n_y, last_terms)
        for n in (n_y - 2, n_y - 1):
            y_copy(blocks[1], n, n % 2).wait()

        def drain(rb):
            for_slots(SLOTS, lambda slot: o_send(PARTNER, slot, rb).wait_send())

            @pl.when(middle)
            def _():
                o_send(MID, FIRST, rb).wait_send()
                for what in passed:
                    o_pass(what, rb).wait_send()

        repeat(n_blk, drain)
        z_copy(PARTNER).wait_send()
        z_copy(MID).wait_send()

        @pl.when(middle)
        def _():
            z_copy(END).wait_send()
            z_forward().wait_send()
            for i in range(len(s_parts)):
                s_copy(i).wait_send()

        def w_sent(o):
            for kind in kinds:
                if (kind, o) != (X_TO_Y, SHIFTED):
                    w_send(kind, o).wait_send()
                c_send(kind, o).wait_send()

        for o in (PARTNER, MID, END):
            w_sent(o)

        @pl.when(end)
        def _():
            w_sent(SHIFTED)

    any_spec = pl.BlockSpec(memory_space=pl.ANY)
    vmem_spec = pl.BlockSpec(memory_space=pltpu.VMEM)
    dma = pltpu.SemaphoreType.DMA
    outs = pl.pallas_call(
        kernel,
        in_specs=[any_spec, vmem_spec] + [any_spec] * 4 + [pl.BlockSpec(memory_space=pltpu.SMEM), vmem_spec],
        out_specs=[any_spec] * 6,
        out_shape=[
            jax.ShapeDtypeStruct((rows, width), BF16),
            jax.ShapeDtypeStruct((n_blk, blk, kvh * d), BF16),
            jax.ShapeDtypeStruct((rows, kvh * d), BF16),
            jax.ShapeDtypeStruct((heads, rows, d), BF16),
            jax.ShapeDtypeStruct((width, width), BF16),
            jax.ShapeDtypeStruct((width, s_cols), BF16),
        ],
        scratch_shapes=[
            pltpu.VMEM((2, width, half_w), BF16),
            pltpu.VMEM((4, n_lane, blk, d), BF16),
            pltpu.VMEM((3, d, n_seg * seg), BF16),
            pltpu.VMEM((3 * group, rows, d), BF16),
            pltpu.VMEM((rows, d), F32),
            pltpu.VMEM((blk, kvh * d), BF16),
            pltpu.VMEM((2, 2 * d, cols), BF16),
            pltpu.VMEM((bk, cols), F32),
            pltpu.VMEM((bk, cols), F32),
            pltpu.VMEM((d, cols), F32),
            pltpu.VMEM((d, cols), F32),
            pltpu.VMEM((2, 1, cols), F32),
            pltpu.VMEM((2, 1, cols), F32),
            pltpu.VMEM((2, 1, cols), F32),
            pltpu.VMEM((2, blk, y_cols), BF16),
            dma((4,)), dma((2,)), dma((1,)), dma((2, kvh)),
            dma((3, 12)), dma((3, 12)), dma((4,)), dma((3,)), dma((3,)), dma((3,)), dma((4, 4)), dma((4, 4)), dma((4, 4)), dma((4, 4)),
            dma((2, n_blk, 3)), dma((n_blk, 3)), dma((n_blk, n_groups)), dma((n_blk, 7)), dma((2, 2)), dma((2,)), dma((4, 2)),
        ],
        compiler_params=pltpu.CompilerParams(collective_id=0, has_side_effects=True, vmem_limit_bytes=67043328),
        name="sublayer",
    )(x, gain, w_q, w_k, w_v, w_o, positions, freqs)
    return outs[:3]


def results(y):
    rows, width = y.shape
    n = 8
    blk = rows // n

    def kernel(y_in, y_out, buf, sems):
        def copy_in(i):
            return pltpu.make_async_copy(y_in.at[pl.ds(i * blk, blk), :], buf.at[pl.ds(i * blk, blk), :], sems.at[0, i])

        def copy_out(i):
            return pltpu.make_async_copy(buf.at[pl.ds(i * blk, blk), :], y_out.at[pl.ds(i * blk, blk), :], sems.at[1, i])

        for i in range(n):
            copy_in(i).start()
        for i in range(n):
            copy_in(i).wait()
            copy_out(i).start()
        for i in range(n):
            copy_out(i).wait()

    any_spec = pl.BlockSpec(memory_space=pl.ANY)
    return pl.pallas_call(
        kernel,
        in_specs=[any_spec],
        out_specs=any_spec,
        out_shape=jax.ShapeDtypeStruct(y.shape, BF16),
        scratch_shapes=[pltpu.VMEM(y.shape, BF16), pltpu.SemaphoreType.DMA((2, n))],
        compiler_params=pltpu.CompilerParams(vmem_limit_bytes=60 * 2 ** 20),
        name="results",
    )(y)


def solution(mesh):
    def device_fn(x_in, positions, norm_gain, w_q, w_k, w_v, w_o):
        kv_heads = w_k.shape[1] // HEAD_DIM
        freqs = rope_freqs()
        freqs = jnp.concatenate([freqs, freqs])[None, :]
        gain = norm_gain.reshape(-1, HEAD_DIM)
        y, keys, values = layer(x_in, gain, w_q, w_k, w_v, w_o, positions, freqs)
        shape = (x_in.shape[0], kv_heads, HEAD_DIM)
        return results(y), keys.reshape(shape), values.reshape(shape)

    row_spec = P(('dp', 'cp'), None)
    cache_spec = P(('dp', 'cp'), 'tp', None)
    return jax.shard_map(device_fn, mesh=mesh, in_specs=(row_spec, P(('dp', 'cp')), P(None), P(None, 'tp'), P(None, 'tp'), P(None, 'tp'), P('tp', None)), out_specs=(row_spec, cache_spec, cache_spec), check_vma=False)
```

```python
import math
import jax
import jax.numpy as jnp
from jax import lax
from jax.experimental import pallas as pl
from jax.experimental.pallas import tpu as pltpu
from jax.sharding import PartitionSpec as P

HEAD_DIM = 128
NORM_EPS = 1e-5
NEG = -0.7 * float(jnp.finfo(jnp.float32).max)
SCALE2 = (1.0 / math.sqrt(HEAD_DIM)) * math.log2(math.e)
BF16 = jnp.bfloat16
F32 = jnp.float32
MESH = pl.DeviceIdType.MESH
LOW, HIGH = range(2)
TOP, BOTTOM = range(2)
FIRST, SECOND, MOVED = SLOTS = range(3)
PARTNER, MID, END, SHIFTED = PIECES = range(4)


def rope_freqs():
    exponent = jnp.arange(0, HEAD_DIM, 2).astype(jnp.float32) / HEAD_DIM
    base_freq = 1.0 / (500000.0 ** exponent)
    wave_len = 2.0 * math.pi / base_freq
    smooth = (8192.0 / wave_len - 1.0) / 3.0
    blended = (1.0 - smooth) * base_freq / 8.0 + smooth * base_freq
    return jnp.where(wave_len < 2048.0, base_freq, jnp.where(wave_len > 8192.0, base_freq / 8.0, blended))


def repeat(n, step, first=0):
    lax.fori_loop(first, first + n, lambda i, carry: (step(i), carry)[1], 0)


def pick(i, values):
    out = values[-1]
    for at, value in enumerate(values[:-1]):
        out = jnp.where(i == at, value, out)
    return out


def rotate(vec_bf, cos, sin):
    vec = vec_bf.astype(F32)
    return (vec * cos + pltpu.roll(vec, HEAD_DIM // 2, axis=1) * sin).astype(BF16)


def layer(x, gain, w_q, w_k, w_v, w_o, positions, freqs):
    rows, width = x.shape
    seg = rows // 2
    d = HEAD_DIM
    kvh = w_k.shape[1] // d
    group = w_q.shape[1] // w_k.shape[1]
    gw = group * d
    qw = kvh * gw
    n_tp = width // qw
    n_groups = n_tp * kvh
    heads = n_groups * group
    n_seg = 8
    blk = 256
    n_blk = rows // blk
    n_lane = width // d
    half_w = width // 2
    bq, bk, bp = 256, 512, 256
    cols = bq * group
    unit_rows = 2 * bq
    w_slice = qw // 8
    s_slice = width // 8
    s_cols = gw + 2 * d
    s_at = qw
    y_cols = 512
    nr = 128
    assert n_blk == n_groups and heads == n_lane

    def kernel(x_ref, gain_ref, wq_ref, wk_ref, wv_ref, wo_ref, pos_ref, freq_ref,
               y_ref, k_ref, v_ref, oall_ref, wall_ref, wsx_ref,
               big, kb, vb, qb, csb, vst, qt, s_a, s_b, acc_a, acc_b, m_run, l_run, m_tile, yb,
               ld_sem, x_sem, vst_sem, kout_sem,
               kv_s, kv_r, wz_s, wz_r, sz_s, sz_r, wp_s, wp_r, wc_s, wc_r,
               o_s, o_l, o_r, f_s, ob_sem, yb_sem, wl_sem):
        dp, z, cp = lax.axis_index("dp"), lax.axis_index("tp"), lax.axis_index("cp")
        cy, cc = cp // 2, cp % 2
        x_nb = {"dp": 1 - dp}
        y_nb = {"cp": (1 - cy) * 2 + cc}
        c_nb = {"cp": cy * 2 + 1 - cc}

        middle = (z == 1) | (z == 2)
        end = jnp.logical_not(middle)
        partner = z + 1 - 2 * (z % 2)
        other_mid = jnp.where(z < 2, 2, 1)
        other_end = jnp.where(z < 2, 3, 0)
        sources = (z, partner, other_mid, other_end)
        slot_out = jnp.where(middle, MID, END)
        keep = jnp.where(z == 1, SECOND, FIRST)
        head_at = lambda slot: jnp.where(middle, keep, slot)
        last_z = n_tp - 1

        def group_of(zz, slot):
            at_far_end = n_groups - len(SLOTS) + (slot + 1) % len(SLOTS) if isinstance(slot, int) else (
                n_groups - len(SLOTS) + lax.rem(slot + 1, len(SLOTS)))
            return jnp.where(zz == 0, slot, jnp.where(zz == last_z, at_far_end, zz + kvh))

        source = lambda piece: sources[piece + 1]

        def remote(src, dst, ss, rs, dev):
            return pltpu.make_async_remote_copy(src_ref=src, dst_ref=dst, send_sem=ss, recv_sem=rs, device_id=dev, device_id_type=MESH)

        def got(region, rs):
            remote(region, region, rs, rs, x_nb).wait_recv()

        def at_rows(n, size):
            return pl.ds(pl.multiple_of(n, size), size)

        place = dp * 4 + cp

        def place_of(fx, fy, fc):
            px = 1 - dp if fx else dp
            py = 1 - cy if fy else cy
            pc = 1 - cc if fc else cc
            return px * 4 + py * 2 + pc

        def piece(o, fx, fy, fc, part=None):
            size = s_slice if o == SHIFTED else w_slice
            base = place_of(fx, fy, fc) * size
            if o != SHIFTED:
                base = base + source(o) * qw
            n = size if part is None else size // 2
            base = pl.multiple_of(base + (n if part == BOTTOM else 0), n)
            return (wsx_ref if o == SHIFTED else wall_ref).at[pl.ds(base, n), :]

        here = lambda o: piece(o, 0, 0, 0)
        next_x = lambda o, part=None: piece(o, 1, 0, 0, part)
        next_y = lambda o, part=None: piece(o, 0, 1, 0, part)
        next_xy = lambda o, part=None: piece(o, 1, 1, 0, part)
        at_core = lambda o: (here(o), next_x(o), next_y(o), next_xy(o))

        def z_copy(o):
            src = wo_ref.at[at_rows(place * w_slice, w_slice), :]
            dst = wall_ref.at[at_rows(z * qw + place * w_slice, w_slice), :]
            return remote(src, dst, wz_s.at[o], wz_r.at[PARTNER if o == PARTNER else slot_out], {"tp": source(o)})

        def z_forward():
            return remote(here(END), here(END), wz_s.at[SHIFTED], wz_r.at[END], {"tp": partner})

        s_parts = ((wq_ref, 0, gw), (wk_ref, gw, d), (wv_ref, gw + d, d))

        def s_dst(i):
            _, lane, n = s_parts[i]
            return wsx_ref.at[at_rows(place * s_slice, s_slice), pl.ds(lane, n)]

        def s_copy(i):
            ref, _, n = s_parts[i]
            src = ref.at[at_rows(place * s_slice, s_slice), at_rows((1 - keep) * n, n)]
            return remote(src, s_dst(i), sz_s.at[i], sz_r.at[i], {"tp": partner})

        OWN_X, OWN_Y, X_TO_Y, Y_TO_X = kinds = range(4)

        def w_send(kind, o):
            if kind == OWN_X:
                region, dev = here(o), x_nb
            elif kind == OWN_Y:
                region, dev = here(o), y_nb
            elif kind == X_TO_Y:
                region, dev = next_x(o, TOP), y_nb
            else:
                region, dev = next_y(o, None if o == SHIFTED else BOTTOM), x_nb
            return remote(region, region, wp_s.at[kind, o], wp_r.at[kind, o], dev)

        def c_send(i, o):
            region = at_core(o)[i]
            return remote(region, region, wc_s.at[i, o], wc_r.at[i, o], c_nb)

        def w_stage1(o):
            if o == SHIFTED:
                for i in range(len(s_parts)):
                    got(s_dst(i), sz_r.at[i])
            elif o != END:
                got(here(o), wz_r.at[o])
            else:
                @pl.when(end)
                def _():
                    got(here(o), wz_r.at[o])

            w_send(OWN_X, o).start()
            w_send(OWN_Y, o).start()
            c_send(0, o).start()

        def w_stage2(o):
            got(next_x(o), wp_r.at[OWN_X, o])
            if o != SHIFTED:
                w_send(X_TO_Y, o).start()
            c_send(1, o).start()
            got(next_y(o), wp_r.at[OWN_Y, o])
            w_send(Y_TO_X, o).start()
            c_send(2, o).start()

        def w_stage3(o):
            if o != SHIFTED:
                got(next_xy(o, TOP), wp_r.at[X_TO_Y, o])
            got(next_xy(o, None if o == SHIFTED else BOTTOM), wp_r.at[Y_TO_X, o])
            c_send(3, o).start()

        def w_gathered(o):
            for i, (fx, fy) in enumerate(((0, 0), (1, 0), (0, 1), (1, 1))):
                got(piece(o, fx, fy, 1), wc_r.at[i, o])

        def w_load(zs, src, i):
            return [pltpu.make_async_copy(
                src.at[:, pl.ds(n * half_w, half_w)], big.at[n, at_rows(zs * qw, qw), :], wl_sem.at[i, n]) for n in range(2)]

        def w_load_own():
            return w_load(z, wo_ref, SHIFTED)

        def w_load_other(o):
            return w_load(source(o), wall_ref.at[at_rows(source(o) * qw, qw), :], o)

        def w_stage4(o):
            w_gathered(o)
            for c in w_load_other(o):
                c.start()

        def load_weights(i, ref, lane, n):
            return pltpu.make_async_copy(ref, big.at[0, :, pl.ds(lane, n)], ld_sem.at[i])

        load_q, load_k, load_v, load_s = (load_weights(i, *args) for i, args in enumerate((
            (wq_ref, 0, qw), (wk_ref, qw, kvh * d), (wv_ref, qw + kvh * d, kvh * d), (wsx_ref, s_at, s_cols))))

        def x_start(b, slot):
            for i in range(n_lane):
                pltpu.make_async_copy(x_ref.at[at_rows(b * blk, blk), pl.ds(i * d, d)], kb.at[2 + slot, i], x_sem.at[slot]).start()

        def x_wait(slot):
            pltpu.make_async_copy(kb.at[2 + slot], kb.at[2 + slot], x_sem.at[slot]).wait()

        def v_copy(b):
            return pltpu.make_async_copy(vst, v_ref.at[at_rows(b * blk, blk), :], vst_sem.at[0])

        low_lanes = lax.broadcasted_iota(jnp.int32, (blk, d), 1) < d // 2

        def make_angles(b):
            first = pos_ref[b * blk]
            pos = (lax.broadcasted_iota(jnp.int32, (blk, d), 0) + first).astype(F32)
            angle = pos * freq_ref[...]
            csb[at_rows(b * blk, blk), :] = jnp.where(low_lanes, jnp.cos(angle), jnp.sin(angle))

        def cos_sin(b):
            both = csb[at_rows(b * blk, blk), :]
            turned = pltpu.roll(both, d // 2, axis=1)
            return jnp.where(low_lanes, both, turned), jnp.where(low_lanes, -turned, both)

        x_start(0, 0)
        load_k.start()
        load_v.start()
        load_q.start()

        barrier = pltpu.get_barrier_semaphore()
        for dev in (x_nb, y_nb, c_nb, {"tp": partner}, {"tp": other_mid}, {"tp": other_end}):
            pl.semaphore_signal(barrier, inc=1, device_id=dev, device_id_type=MESH)
        pl.semaphore_wait(barrier, 6)

        @pl.when(middle)
        def _():
            for i in range(len(s_parts)):
                s_copy(i).start()

        z_copy(PARTNER).start()
        z_copy(MID).start()

        @pl.when(middle)
        def _():
            z_copy(END).start()

        seg_at = lambda half, c: jnp.where(half == LOW, c, n_seg - 1 - c) * seg
        y_cp = (1 - cy) * 2 + cc
        c_cp = cy * 2 + 1 - cc
        yc_cp = (1 - cy) * 2 + 1 - cc

        def kv_region(half, c, which, slot):
            at = pl.multiple_of(seg_at(half, c), seg)
            h = head_at(slot)
            return kb.at[h, pl.ds(at // blk, seg // blk)] if which == 0 else vb.at[h, :, pl.ds(at, seg)]

        TO_CORE, TO_Y, Y_TO_CORE = kv_kinds = range(3)
        kv_both = range(2)
        n_kv = len(kv_both) * len(SLOTS)
        kv_at = lambda half, which, slot: half * n_kv + which * len(SLOTS) + slot

        def kv_send(kind, half, which, slot):
            region = kv_region(half, y_cp if kind == Y_TO_CORE else cp, which, slot)
            i = kv_at(half, which, slot)
            return remote(region, region, kv_s.at[kind, i], kv_r.at[kind, i], y_nb if kind == TO_Y else c_nb)

        def for_slots(slots, f):
            for slot in slots:
                if slot == FIRST:
                    f(slot)
                else:
                    @pl.when(end)
                    def _():
                        f(slot)

        own = (FIRST, SECOND)
        moved = (MOVED,)

        def kv_start(half, slots):
            def f(slot):
                for which in kv_both:
                    kv_send(TO_Y, half, which, slot).start()
                    kv_send(TO_CORE, half, which, slot).start()
            for_slots(slots, f)

        def kv_relay(half, slots):
            def f(slot):
                for which in kv_both:
                    got(kv_region(half, y_cp, which, slot), kv_r.at[TO_Y, kv_at(half, which, slot)])
                    kv_send(Y_TO_CORE, half, which, slot).start()
            for_slots(slots, f)

        def kv_arrived(half, slots):
            def f(slot):
                for which in kv_both:
                    i = kv_at(half, which, slot)
                    got(kv_region(half, c_cp, which, slot), kv_r.at[TO_CORE, i])
                    got(kv_region(half, yc_cp, which, slot), kv_r.at[Y_TO_CORE, i])
            for_slots(slots, f)

        def kv_sent():
            def f(slot):
                for half in (LOW, HIGH):
                    for which in kv_both:
                        for kind in kv_kinds:
                            kv_send(kind, half, which, slot).wait_send()
            for_slots(SLOTS, f)

        def k_copy(half, hh):
            at = pl.multiple_of(seg_at(half, cp), seg)
            n = seg // blk
            return pltpu.make_async_copy(kb.at[hh, pl.ds(at // blk, n)], k_ref.at[pl.ds(half * n, n), :, pl.ds(hh * d, d)], kout_sem.at[half, hh])

        def h_rows(b):
            h0 = big[1, at_rows(b * blk, blk), :]
            h1 = big[1, at_rows(rows + b * blk, blk), :]
            return jnp.concatenate([h0, h1], axis=1)

        load_k.wait()
        load_v.wait()

        half_blk = n_blk // 2

        def at_half_end(b, f):
            for half in (LOW, HIGH):
                @pl.when(b == half * half_blk + half_blk - 1)
                def _():
                    f(half)

        def kv_rows(b):
            return pl.multiple_of(seg_at(b // half_blk, cp) + lax.rem(b, half_blk) * blk, blk)

        def kv_block(b):
            slot = b % 2
            x_wait(slot)

            @pl.when(b + 1 < n_blk)
            def _():
                x_start(b + 1, 1 - slot)

            def norm_rows(i):
                at = at_rows(i * nr, nr)
                square = 0.0
                for j in range(n_lane):
                    xf = kb[2 + slot, j, at, :].astype(F32)
                    square = square + xf * xf
                inv = lax.rsqrt(jnp.sum(square, axis=-1, keepdims=True) / width + NORM_EPS)
                for j in range(n_lane):
                    xf = kb[2 + slot, j, at, :].astype(F32)
                    h = ((xf * inv) * gain_ref[j:j + 1, :].astype(F32)).astype(BF16)
                    row = b * blk + (0 if j * d < half_w else rows) + i * nr
                    lane = (j * d) % half_w
                    big[1, at_rows(row, nr), lane:lane + d] = h

            repeat(blk // nr, norm_rows)
            make_angles(b)
            kv = jnp.dot(h_rows(b), big[0, :, qw:qw + 2 * kvh * d], preferred_element_type=F32).astype(BF16)
            cos, sin = cos_sin(b)
            at = kv_rows(b)

            @pl.when(b > 0)
            def _():
                v_copy(b - 1).wait()

            for hh in range(kvh):
                kb[hh, at // blk] = rotate(kv[:, hh * d:(hh + 1) * d], cos, sin)
                vb[hh, :, pl.ds(at, blk)] = kv[:, (kvh + hh) * d:(kvh + hh + 1) * d].T
            vst[...] = kv[:, kvh * d:]
            v_copy(b).start()

            def send(half):
                kv_start(half, own)
                for hh in range(kvh):
                    k_copy(half, hh).start()

            at_half_end(b, send)

        repeat(n_blk, kv_block)
        v_copy(n_blk - 1).wait()
        load_q.wait()

        @pl.when(end)
        def _():
            w_stage1(SHIFTED)

        def q_half(half):
            def q_block(b):
                cos, sin = cos_sin(b)

                def project(i):
                    head = head_at(i)
                    q = jnp.dot(h_rows(b), big[0, :, at_rows(head * gw, gw)], preferred_element_type=F32).astype(BF16)
                    for j in range(group):
                        qb[head * group + j, at_rows(b * blk, blk), :] = rotate(q[:, j * d:(j + 1) * d], cos, sin)

                repeat(jnp.where(middle, 1, kvh), project)

            repeat(half_blk, q_block, half * half_blk)

        def moved_block(b):
            cos, sin = cos_sin(b)
            qkv = jnp.dot(h_rows(b), big[0, :, s_at:s_at + s_cols], preferred_element_type=F32).astype(BF16)
            for j in range(group):
                qb[MOVED * group + j, at_rows(b * blk, blk), :] = rotate(qkv[:, j * d:(j + 1) * d], cos, sin)
            at = kv_rows(b)
            kb[MOVED, at // blk] = rotate(qkv[:, gw:gw + d], cos, sin)
            vb[MOVED, :, pl.ds(at, blk)] = qkv[:, gw + d:].T
            at_half_end(b, lambda half: kv_start(half, moved))

        def o_region(g, rb):
            return oall_ref.at[pl.ds(g * group, group), at_rows(rb * blk, blk), :]

        def o_own(slot, rb):
            return qb.at[pl.ds(head_at(slot) * group, group), at_rows(rb * blk, blk), :]

        def o_local(slot, rb):
            return pltpu.make_async_copy(o_own(slot, rb), o_region(group_of(z, slot), rb), o_l.at[rb, slot])

        def o_send(to, slot, rb):
            g = group_of(z, slot)
            return remote(o_own(slot, rb), o_region(g, rb), o_s.at[to, rb, slot], o_r.at[rb, g], {"tp": source(to)})

        others = ((MID, FIRST), (END, FIRST), (END, SECOND), (END, MOVED))
        ends_own = ((PARTNER, FIRST), (PARTNER, SECOND), (PARTNER, MOVED))
        passed = others + ends_own

        def o_pass(what, rb):
            g = group_of(source(what[0]), what[1])
            region = o_region(g, rb)
            to = {"tp": partner if what in others else other_mid}
            return remote(region, region, f_s.at[rb, passed.index(what)], o_r.at[rb, g], to)

        def o_wait(what, rb):
            g = group_of(source(what[0]), what[1])
            got(o_region(g, rb), o_r.at[rb, g])

        def pass_on(what, blocks):
            def step(rb):
                for item in what:
                    o_wait(item, rb)
                    o_pass(item, rb).start()

            repeat(len(blocks), step, blocks[0])

        def own_outward(blocks):
            repeat(len(blocks), lambda rb: o_send(PARTNER, FIRST, rb).start(), blocks[0])

        scores = (s_a, s_b)
        accs = (acc_a, acc_b)

        def unit(half, c, slot):
            hl = head_at(slot)
            r0 = pl.multiple_of(half * seg + c * unit_rows, unit_rows)
            g0 = seg_at(half, cp) + c * unit_rows
            for st in range(2):
                for j in range(group):
                    qs = qb[hl * group + j, pl.ds(r0 + st * bq, bq), :].T.astype(F32) * SCALE2
                    top = qs.astype(BF16)
                    span = slice(j * bq, (j + 1) * bq)
                    qt[st, 0:d, span] = top
                    qt[st, d:2 * d, span] = (qs - top.astype(F32)).astype(BF16)
            k_idx = lax.broadcasted_iota(jnp.int32, (bk, cols), 0)
            q_idx = lax.broadcasted_iota(jnp.int32, (bk, cols), 1) % bq

            def qk(st, t, mask=None):
                kt = kb[hl, pl.ds(t * (bk // blk), bk // blk)].reshape(bk, d)
                s = jnp.dot(jnp.concatenate([kt, kt], axis=1), qt[st], preferred_element_type=F32)
                if mask is not None:
                    s = jnp.where(mask, s, NEG)
                scores[st][...] = s
                m_tile[st] = jnp.max(s, axis=0, keepdims=True)

            def soft(st, t):
                m_old = m_run[st]
                m_new = jnp.maximum(m_old, m_tile[st])
                m_run[st] = m_new
                alpha = jnp.exp2(m_old - m_new)
                total, pv = 0.0, 0.0
                for i in range(bk // bp):
                    p = jnp.exp2(scores[st][i * bp:(i + 1) * bp, :] - m_new)
                    total = total + jnp.sum(p, axis=0, keepdims=True)
                    v = vb[hl, :, at_rows(t * bk + i * bp, bp)]
                    pv = pv + jnp.dot(v, p.astype(BF16), preferred_element_type=F32)
                l_run[st] = l_run[st] * alpha + total
                accs[st][...] = accs[st][...] * alpha + pv

            m_run[...] = jnp.full_like(m_run, NEG)
            l_run[...] = jnp.zeros_like(l_run)
            acc_a[...] = jnp.zeros_like(acc_a)
            acc_b[...] = jnp.zeros_like(acc_b)
            n_full = g0 // bk

            qk(0, 0, k_idx <= q_idx + g0)

            def body(t):
                qk(1, t)
                soft(0, t)
                qk(0, t + 1)
                soft(1, t)

            repeat(n_full - 1, body)

            def finish_unit(tail):
                if tail:
                    qk(1, n_full - 1)
                    soft(0, n_full - 1)
                    qk(0, n_full, k_idx <= q_idx)
                    soft(1, n_full - 1)
                qk(1, n_full, k_idx <= q_idx + bq)
                soft(0, n_full)
                soft(1, n_full)
                for st in range(2):
                    o = accs[st][...] * (1.0 / l_run[st])
                    for j in range(group):
                        qb[hl * group + j, pl.ds(r0 + st * bq, bq), :] = o[:, j * bq:(j + 1) * bq].T.astype(BF16)

            @pl.when(n_full > 0)
            def _():
                finish_unit(True)

            @pl.when(n_full == 0)
            def _():
                finish_unit(False)

            for st in range(2):
                rb = half * half_blk + c * 2 + st

                @pl.when(middle)
                def _():
                    o_send(MID, slot, rb).start()

                @pl.when(end | (half == LOW))
                def _():
                    o_send(PARTNER, slot, rb).start()

                o_local(slot, rb).start()

        q_half(LOW)
        kv_relay(LOW, own)
        kv_arrived(LOW, own)

        def when_cp(which, f):
            @pl.when(which)
            def _():
                f()

        def nothing():
            pass

        def start_all(copies):
            for c in copies:
                c.start()

        def second_half():
            when_cp(cp > 0, lambda: kv_relay(HIGH, own))
            when_cp(cp == 3, lambda: w_stage2(SHIFTED))
            q_half(HIGH)
            when_cp(cp == 0, lambda: kv_relay(HIGH, own))
            kv_arrived(HIGH, own)
            when_cp(cp == 2, lambda: w_stage2(SHIFTED))
            when_cp(cp >= 2, lambda: w_stage1(PARTNER))

        def moved_head():
            w_gathered(SHIFTED)
            load_s.start()
            load_s.wait()
            repeat(n_blk, moved_block)
            start_all(w_load_own())
            when_cp(cp >= 2, lambda: w_stage2(PARTNER))
            w_stage1(END)

        def after_e():
            when_cp(cp < 2, lambda: w_stage2(SHIFTED))
            when_cp(cp == 3, lambda: w_stage3(SHIFTED))
            w_stage1(MID)

        def after_f():
            when_cp(cp < 3, lambda: w_stage3(SHIFTED))
            when_cp(cp < 2, lambda: w_stage2(PARTNER))

        def after_g():
            kv_relay(LOW, moved)
            w_stage2(MID)
            kv_arrived(LOW, moved)

        def after_h():
            kv_relay(HIGH, moved)

        def after_i():
            kv_arrived(HIGH, moved)

        def after_j():
            w_stage3(PARTNER)
            w_stage2(END)

        def after_k():
            w_stage3(MID)
            w_stage3(END)
            w_stage4(PARTNER)

        def after_l():
            w_stage4(MID)
            w_stage4(END)

        end_units = (
            (LOW, TOP, FIRST, nothing, nothing),
            (LOW, TOP, SECOND, nothing, nothing),
            (LOW, BOTTOM, FIRST, nothing, nothing),
            (LOW, BOTTOM, SECOND, nothing, lambda: when_cp(cp < 2, lambda: w_stage1(PARTNER))),
            (HIGH, TOP, FIRST, second_half, after_e),
            (HIGH, TOP, SECOND, nothing, after_f),
            (HIGH, BOTTOM, FIRST, moved_head, after_g),
            (LOW, TOP, MOVED, nothing, after_h),
            (LOW, BOTTOM, MOVED, nothing, after_i),
            (HIGH, TOP, MOVED, nothing, after_j),
            (HIGH, BOTTOM, SECOND, nothing, after_k),
            (HIGH, BOTTOM, MOVED, nothing, after_l),
        )

        low_blocks, high_blocks = range(half_blk), range(half_blk, n_blk)
        top = lambda blocks: blocks[:half_blk // 2]
        bottom = lambda blocks: blocks[half_blk // 2:]
        mids, end_first, end_both, end_moved = others[:1], others[1:2], others[1:3], others[3:]
        own_both, own_moved = ends_own[:2], ends_own[2:]

        def middle_high():
            got(here(END), wz_r.at[END])
            z_forward().start()
            kv_relay(HIGH, own)
            q_half(HIGH)
            kv_arrived(HIGH, own)
            start_all(w_load_own())
            for o in (PARTNER, MID, END):
                w_stage1(o)

        middle_units = (
            (LOW, TOP, FIRST, nothing, nothing),
            (LOW, BOTTOM, FIRST, nothing, nothing),
            (HIGH, TOP, FIRST, middle_high, lambda: pass_on(own_both, top(low_blocks))),
            (HIGH, BOTTOM, FIRST, nothing, nothing),
        )

        def unit_loop(s):
            half, c, slot = (
                jnp.where(middle, pick(s, [u[i] for u in middle_units]), pick(s, [u[i] for u in end_units])) for i in range(3))

            def events(i):
                for role, units in ((middle, middle_units), (end, end_units)):
                    for step, what in enumerate(units):
                        if what[i] is not nothing:
                            @pl.when(role & (s == step))
                            def _():
                                what[i]()

            events(-2)
            unit(half, c, slot)
            events(-1)

        repeat(jnp.where(middle, len(middle_units), len(end_units)), unit_loop)

        @pl.when(middle)
        def _():
            pass_on(own_both, bottom(low_blocks))
            pass_on(mids, low_blocks)
            w_stage2(PARTNER)
            pass_on(end_both, top(low_blocks))
            own_outward(top(high_blocks))
            w_stage2(MID)
            w_stage2(END)
            w_stage3(PARTNER)
            pass_on(end_both, bottom(low_blocks))
            w_stage3(MID)
            w_stage4(PARTNER)
            w_stage3(END)
            w_stage4(MID)
            pass_on(own_moved, low_blocks)
            w_stage4(END)
            pass_on(end_moved, low_blocks)
            pass_on(own_both, top(high_blocks))
            pass_on(mids, top(high_blocks))

        def middle_0():
            pass_on(own_moved, top(high_blocks))
            pass_on(end_both, top(high_blocks))

        def middle_1():
            pass_on(end_moved, top(high_blocks))
            own_outward(bottom(high_blocks))
            pass_on(mids, bottom(high_blocks))
            pass_on(own_both, bottom(high_blocks))

        def middle_2():
            pass_on(own_moved, bottom(high_blocks))
            pass_on(end_both, bottom(high_blocks))

        middle_events = (middle_0, middle_1, middle_2, lambda: pass_on(end_moved, bottom(high_blocks)))

        kv_sent()
        for half in range(2):
            for hh in range(kvh):
                k_copy(half, hh).wait()

        def early_landed(rb):
            for_slots(SLOTS, lambda slot: o_local(slot, rb).wait())

            @pl.when(end)
            def _():
                for what in (ends_own[0], others[0]):
                    o_wait(what, rb)

        def late_landed(rb):
            @pl.when(end)
            def _():
                for what in others[1:]:
                    o_wait(what, rb)

        def ob_copy(rb, slot, first, n, i):
            return pltpu.make_async_copy(
                oall_ref.at[pl.ds(first, n), at_rows(rb * blk, blk), :], kb.at[slot, pl.ds(first, n)], ob_sem.at[slot, i])

        def ob_all(rb, slot):
            return ob_copy(rb, slot, 0, heads, 0)

        def o_fetch(rb, slot):
            early_landed(rb)
            late_landed(rb)
            ob_all(rb, slot).start()

        n_y = width // y_cols
        n_h = half_w // y_cols

        def y_copy(rb, n, slot):
            return pltpu.make_async_copy(yb.at[slot], y_ref.at[at_rows(rb * blk, blk), at_rows(n * y_cols, y_cols)], yb_sem.at[slot])

        def product(slot, first, n_heads, n):
            o = jnp.concatenate([kb[slot, first + i] for i in range(n_heads)], axis=1)
            row = first * d if isinstance(first, int) else pl.multiple_of(first * d, gw)
            w = big[n // n_h, pl.ds(row, n_heads * d), at_rows((n % n_h) * y_cols, y_cols)]
            return jnp.dot(o, w, preferred_element_type=F32)

        def x_cols(slot, n):
            n_in = y_cols // d
            return jnp.concatenate([kb[2 + slot, n * n_in + i] for i in range(n_in)], axis=1).astype(F32)

        x_start(0, 0)
        o_fetch(0, 0)
        for c in sum((w_load_other(o) for o in (PARTNER, MID, END)), w_load_own()):
            c.wait()

        n_full_blocks = n_blk - 2

        def out_block(rb):
            slot = rb % 2
            x_wait(slot)
            ob_all(rb, slot).wait()
            x_start(rb + 1, 1 - slot)

            @pl.when(rb + 1 < n_full_blocks)
            def _():
                o_fetch(rb + 1, 1 - slot)

            def out_cols(n):
                ys = n % 2

                @pl.when(rb * n_y + n >= 2)
                def _():
                    y_copy(rb, n, ys).wait()

                yb[ys] = (x_cols(slot, n) + product(slot, 0, heads, n)).astype(BF16)
                y_copy(rb, n, ys).start()

            repeat(n_y, out_cols)
            for i, event in enumerate(middle_events):
                @pl.when(middle & (rb == i))
                def _():
                    event()

        repeat(n_full_blocks, out_block)

        n_late = len(SLOTS) * group
        n_early = heads - n_late
        early = jnp.where(z < 2, 0, n_late)
        late = jnp.where(z < 2, n_early, 0)
        blocks = (n_full_blocks, n_full_blocks + 1)

        def part(n):
            return (at_rows((n % n_h) // 2 * blk, blk), at_rows(n % 2 * y_cols, y_cols))

        def lanes_of(n, half):
            return at_rows(n * 2 * y_cols + half * y_cols, y_cols)

        def early_sum(slot, n):
            return x_cols(slot, n) + product(slot, early, n_early, n)

        def finish(slot, n, total):
            ys = n % 2
            y_copy(blocks[slot], n, ys).wait()
            yb[ys] = (total + product(slot, late, n_late, n)).astype(BF16)
            y_copy(blocks[slot], n, ys).start()

        early_copies = [ob_copy(rb, slot, early, n_early, 0) for slot, rb in enumerate(blocks)]
        late_copies = [ob_copy(rb, slot, late, n_late, 1) for slot, rb in enumerate(blocks)]
        for slot, rb in enumerate(blocks):
            early_landed(rb)
            if slot > 0:
                x_start(rb, slot)
            early_copies[slot].start()
        for i in range(2):
            if i == 0:
                x_wait(0)
                early_copies[0].wait()

            def first_terms(n):
                scores[i][part(n)] = early_sum(0, n)

            repeat(n_h, first_terms, i * n_h)
        x_wait(1)
        early_copies[1].wait()
        half_rows = blk // 2

        def second_terms(n):
            total = early_sum(1, n)
            for i in range(len(SLOTS)):
                term = total.astype(BF16)
                for half in range(2):
                    vb[i, :, lanes_of(n, half)] = term[half * half_rows:(half + 1) * half_rows]
                total = total - term.astype(F32)

        repeat(n_y, second_terms)
        late_landed(blocks[0])
        late_copies[0].start()
        late_copies[0].wait()
        for i in range(2):
            repeat(n_h, lambda n: finish(0, n, scores[i][part(n)]), i * n_h)
        late_landed(blocks[1])
        late_copies[1].start()
        late_copies[1].wait()

        def last_terms(n):
            terms = [jnp.concatenate([vb[i, :, lanes_of(n, half)] for half in range(2)], axis=0).astype(F32) for i in range(len(SLOTS))]
            finish(1, n, (terms[0] + terms[1]) + terms[2])

        repeat(n_y, last_terms)
        for n in (n_y - 2, n_y - 1):
            y_copy(blocks[1], n, n % 2).wait()

        def drain(rb):
            for_slots(SLOTS, lambda slot: o_send(PARTNER, slot, rb).wait_send())

            @pl.when(middle)
            def _():
                o_send(MID, FIRST, rb).wait_send()
                for what in passed:
                    o_pass(what, rb).wait_send()

        repeat(n_blk, drain)
        z_copy(PARTNER).wait_send()
        z_copy(MID).wait_send()

        @pl.when(middle)
        def _():
            z_copy(END).wait_send()
            z_forward().wait_send()
            for i in range(len(s_parts)):
                s_copy(i).wait_send()

        def w_sent(o):
            for kind in kinds:
                if (kind, o) != (X_TO_Y, SHIFTED):
                    w_send(kind, o).wait_send()
                c_send(kind, o).wait_send()

        for o in (PARTNER, MID, END):
            w_sent(o)

        @pl.when(end)
        def _():
            w_sent(SHIFTED)

    any_spec = pl.BlockSpec(memory_space=pl.ANY)
    vmem_spec = pl.BlockSpec(memory_space=pltpu.VMEM)
    dma = pltpu.SemaphoreType.DMA
    outs = pl.pallas_call(
        kernel,
        in_specs=[any_spec, vmem_spec] + [any_spec] * 4 + [pl.BlockSpec(memory_space=pltpu.SMEM), vmem_spec],
        out_specs=[any_spec] * 6,
        out_shape=[
            jax.ShapeDtypeStruct((rows, width), BF16),
            jax.ShapeDtypeStruct((n_blk, blk, kvh * d), BF16),
            jax.ShapeDtypeStruct((rows, kvh * d), BF16),
            jax.ShapeDtypeStruct((heads, rows, d), BF16),
            jax.ShapeDtypeStruct((width, width), BF16),
            jax.ShapeDtypeStruct((width, s_cols), BF16),
        ],
        scratch_shapes=[
            pltpu.VMEM((2, width, half_w), BF16),
            pltpu.VMEM((4, n_lane, blk, d), BF16),
            pltpu.VMEM((3, d, n_seg * seg), BF16),
            pltpu.VMEM((3 * group, rows, d), BF16),
            pltpu.VMEM((rows, d), F32),
            pltpu.VMEM((blk, kvh * d), BF16),
            pltpu.VMEM((2, 2 * d, cols), BF16),
            pltpu.VMEM((bk, cols), F32),
            pltpu.VMEM((bk, cols), F32),
            pltpu.VMEM((d, cols), F32),
            pltpu.VMEM((d, cols), F32),
            pltpu.VMEM((2, 1, cols), F32),
            pltpu.VMEM((2, 1, cols), F32),
            pltpu.VMEM((2, 1, cols), F32),
            pltpu.VMEM((2, blk, y_cols), BF16),
            dma((4,)), dma((2,)), dma((1,)), dma((2, kvh)),
            dma((3, 12)), dma((3, 12)), dma((4,)), dma((3,)), dma((3,)), dma((3,)), dma((4, 4)), dma((4, 4)), dma((4, 4)), dma((4, 4)),
            dma((2, n_blk, 3)), dma((n_blk, 3)), dma((n_blk, n_groups)), dma((n_blk, 7)), dma((2, 2)), dma((2,)), dma((4, 2)),
        ],
        compiler_params=pltpu.CompilerParams(collective_id=0, has_side_effects=True, vmem_limit_bytes=67043328),
        name="sublayer",
    )(x, gain, w_q, w_k, w_v, w_o, positions, freqs)
    return outs[:3]


def results(y):
    rows, width = y.shape
    n = 8
    blk = rows // n

    def kernel(y_in, y_out, buf, sems):
        def copy_in(i):
            return pltpu.make_async_copy(y_in.at[pl.ds(i * blk, blk), :], buf.at[pl.ds(i * blk, blk), :], sems.at[0, i])

        def copy_out(i):
            return pltpu.make_async_copy(buf.at[pl.ds(i * blk, blk), :], y_out.at[pl.ds(i * blk, blk), :], sems.at[1, i])

        for i in range(n):
            copy_in(i).start()
        for i in range(n):
            copy_in(i).wait()
            copy_out(i).start()
        for i in range(n):
            copy_out(i).wait()

    any_spec = pl.BlockSpec(memory_space=pl.ANY)
    return pl.pallas_call(
        kernel,
        in_specs=[any_spec],
        out_specs=any_spec,
        out_shape=jax.ShapeDtypeStruct(y.shape, BF16),
        scratch_shapes=[pltpu.VMEM(y.shape, BF16), pltpu.SemaphoreType.DMA((2, n))],
        compiler_params=pltpu.CompilerParams(vmem_limit_bytes=60 * 2 ** 20),
        name="results",
    )(y)


def solution(mesh):
    def device_fn(x_in, positions, norm_gain, w_q, w_k, w_v, w_o):
        kv_heads = w_k.shape[1] // HEAD_DIM
        freqs = rope_freqs()
        freqs = jnp.concatenate([freqs, freqs])[None, :]
        gain = norm_gain.reshape(-1, HEAD_DIM)
        y, keys, values = layer(x_in, gain, w_q, w_k, w_v, w_o, positions, freqs)
        shape = (x_in.shape[0], kv_heads, HEAD_DIM)
        return results(y), keys.reshape(shape), values.reshape(shape)

    row_spec = P(('dp', 'cp'), None)
    cache_spec = P(('dp', 'cp'), 'tp', None)
    return jax.shard_map(device_fn, mesh=mesh, in_specs=(row_spec, P(('dp', 'cp')), P(None), P(None, 'tp'), P(None, 'tp'), P(None, 'tp'), P('tp', None)), out_specs=(row_spec, cache_spec, cache_spec), check_vma=False)
```

```python
import math
import jax
import jax.numpy as jnp
from jax import lax
from jax.experimental import pallas as pl
from jax.experimental.pallas import tpu as pltpu
from jax.sharding import PartitionSpec as P

HEAD_DIM = 128
NORM_EPS = 1e-5
NEG = -0.7 * float(jnp.finfo(jnp.float32).max)
SCALE2 = (1.0 / math.sqrt(HEAD_DIM)) * math.log2(math.e)
BF16 = jnp.bfloat16
F32 = jnp.float32
MESH = pl.DeviceIdType.MESH
LOW, HIGH = range(2)
TOP, BOTTOM = range(2)
FIRST, SECOND, MOVED = SLOTS = range(3)
PARTNER, MID, END, SHIFTED = PIECES = range(4)


def rope_freqs():
    exponent = jnp.arange(0, HEAD_DIM, 2).astype(jnp.float32) / HEAD_DIM
    base_freq = 1.0 / (500000.0 ** exponent)
    wave_len = 2.0 * math.pi / base_freq
    smooth = (8192.0 / wave_len - 1.0) / 3.0
    blended = (1.0 - smooth) * base_freq / 8.0 + smooth * base_freq
    return jnp.where(wave_len < 2048.0, base_freq, jnp.where(wave_len > 8192.0, base_freq / 8.0, blended))


def repeat(n, step, first=0):
    lax.fori_loop(first, first + n, lambda i, carry: (step(i), carry)[1], 0)


def pick(i, values):
    out = values[-1]
    for at, value in enumerate(values[:-1]):
        out = jnp.where(i == at, value, out)
    return out


def rotate(vec_bf, cos, sin):
    vec = vec_bf.astype(F32)
    return (vec * cos + pltpu.roll(vec, HEAD_DIM // 2, axis=1) * sin).astype(BF16)


def layer(x, gain, w_q, w_k, w_v, w_o, positions, freqs):
    rows, width = x.shape
    seg = rows // 2
    d = HEAD_DIM
    kvh = w_k.shape[1] // d
    group = w_q.shape[1] // w_k.shape[1]
    gw = group * d
    qw = kvh * gw
    n_tp = width // qw
    n_groups = n_tp * kvh
    heads = n_groups * group
    n_seg = 8
    blk = 256
    n_blk = rows // blk
    n_lane = width // d
    half_w = width // 2
    bq, bk, bp = 256, 512, 256
    cols = bq * group
    unit_rows = 2 * bq
    w_slice = qw // 8
    s_slice = width // 8
    s_cols = gw + 2 * d
    s_at = qw
    y_cols = 512
    nr = 128
    assert n_blk == n_groups and heads == n_lane

    def kernel(x_ref, gain_ref, wq_ref, wk_ref, wv_ref, wo_ref, pos_ref, freq_ref,
               y_ref, k_ref, v_ref, oall_ref, wall_ref, wsx_ref,
               big, kb, vb, qb, csb, vst, qt, s_a, s_b, acc_a, acc_b, m_run, l_run, m_tile, yb,
               ld_sem, x_sem, vst_sem, kout_sem,
               kv_s, kv_r, wz_s, wz_r, sz_s, sz_r, wp_s, wp_r, wc_s, wc_r,
               o_s, o_l, o_r, f_s, ob_sem, yb_sem, wl_sem):
        dp, z, cp = lax.axis_index("dp"), lax.axis_index("tp"), lax.axis_index("cp")
        cy, cc = cp // 2, cp % 2
        x_nb = {"dp": 1 - dp}
        y_nb = {"cp": (1 - cy) * 2 + cc}
        c_nb = {"cp": cy * 2 + 1 - cc}

        middle = (z == 1) | (z == 2)
        end = jnp.logical_not(middle)
        partner = z + 1 - 2 * (z % 2)
        other_mid = jnp.where(z < 2, 2, 1)
        other_end = jnp.where(z < 2, 3, 0)
        sources = (z, partner, other_mid, other_end)
        slot_out = jnp.where(middle, MID, END)
        keep = jnp.where(z == 1, SECOND, FIRST)
        head_at = lambda slot: jnp.where(middle, keep, slot)
        last_z = n_tp - 1

        def group_of(zz, slot):
            at_far_end = n_groups - len(SLOTS) + (slot + 1) % len(SLOTS) if isinstance(slot, int) else (
                n_groups - len(SLOTS) + lax.rem(slot + 1, len(SLOTS)))
            return jnp.where(zz == 0, slot, jnp.where(zz == last_z, at_far_end, zz + kvh))

        source = lambda piece: sources[piece + 1]

        def remote(src, dst, ss, rs, dev):
            return pltpu.make_async_remote_copy(src_ref=src, dst_ref=dst, send_sem=ss, recv_sem=rs, device_id=dev, device_id_type=MESH)

        def got(region, rs):
            remote(region, region, rs, rs, x_nb).wait_recv()

        def at_rows(n, size):
            return pl.ds(pl.multiple_of(n, size), size)

        place = dp * 4 + cp

        def place_of(fx, fy, fc):
            px = 1 - dp if fx else dp
            py = 1 - cy if fy else cy
            pc = 1 - cc if fc else cc
            return px * 4 + py * 2 + pc

        def piece(o, fx, fy, fc, part=None):
            size = s_slice if o == SHIFTED else w_slice
            base = place_of(fx, fy, fc) * size
            if o != SHIFTED:
                base = base + source(o) * qw
            n = size if part is None else size // 2
            base = pl.multiple_of(base + (n if part == BOTTOM else 0), n)
            return (wsx_ref if o == SHIFTED else wall_ref).at[pl.ds(base, n), :]

        here = lambda o: piece(o, 0, 0, 0)
        next_x = lambda o, part=None: piece(o, 1, 0, 0, part)
        next_y = lambda o, part=None: piece(o, 0, 1, 0, part)
        next_xy = lambda o, part=None: piece(o, 1, 1, 0, part)
        at_core = lambda o: (here(o), next_x(o), next_y(o), next_xy(o))

        def z_copy(o):
            src = wo_ref.at[at_rows(place * w_slice, w_slice), :]
            dst = wall_ref.at[at_rows(z * qw + place * w_slice, w_slice), :]
            return remote(src, dst, wz_s.at[o], wz_r.at[PARTNER if o == PARTNER else slot_out], {"tp": source(o)})

        def z_forward():
            return remote(here(END), here(END), wz_s.at[SHIFTED], wz_r.at[END], {"tp": partner})

        s_parts = ((wq_ref, 0, gw), (wk_ref, gw, d), (wv_ref, gw + d, d))

        def s_dst(i):
            _, lane, n = s_parts[i]
            return wsx_ref.at[at_rows(place * s_slice, s_slice), pl.ds(lane, n)]

        def s_copy(i):
            ref, _, n = s_parts[i]
            src = ref.at[at_rows(place * s_slice, s_slice), at_rows((1 - keep) * n, n)]
            return remote(src, s_dst(i), sz_s.at[i], sz_r.at[i], {"tp": partner})

        OWN_X, OWN_Y, X_TO_Y, Y_TO_X = kinds = range(4)

        def w_send(kind, o):
            if kind == OWN_X:
                region, dev = here(o), x_nb
            elif kind == OWN_Y:
                region, dev = here(o), y_nb
            elif kind == X_TO_Y:
                region, dev = next_x(o, TOP), y_nb
            else:
                region, dev = next_y(o, None if o == SHIFTED else BOTTOM), x_nb
            return remote(region, region, wp_s.at[kind, o], wp_r.at[kind, o], dev)

        def c_send(i, o):
            region = at_core(o)[i]
            return remote(region, region, wc_s.at[i, o], wc_r.at[i, o], c_nb)

        def w_stage1(o):
            if o == SHIFTED:
                for i in range(len(s_parts)):
                    got(s_dst(i), sz_r.at[i])
            elif o != END:
                got(here(o), wz_r.at[o])
            else:
                @pl.when(end)
                def _():
                    got(here(o), wz_r.at[o])

            w_send(OWN_X, o).start()
            w_send(OWN_Y, o).start()
            c_send(0, o).start()

        def w_stage2(o):
            got(next_x(o), wp_r.at[OWN_X, o])
            if o != SHIFTED:
                w_send(X_TO_Y, o).start()
            c_send(1, o).start()
            got(next_y(o), wp_r.at[OWN_Y, o])
            w_send(Y_TO_X, o).start()
            c_send(2, o).start()

        def w_stage3(o):
            if o != SHIFTED:
                got(next_xy(o, TOP), wp_r.at[X_TO_Y, o])
            got(next_xy(o, None if o == SHIFTED else BOTTOM), wp_r.at[Y_TO_X, o])
            c_send(3, o).start()

        def w_gathered(o):
            for i, (fx, fy) in enumerate(((0, 0), (1, 0), (0, 1), (1, 1))):
                got(piece(o, fx, fy, 1), wc_r.at[i, o])

        def w_load(zs, src, i):
            return [pltpu.make_async_copy(
                src.at[:, pl.ds(n * half_w, half_w)], big.at[n, at_rows(zs * qw, qw), :], wl_sem.at[i, n]) for n in range(2)]

        def w_load_own():
            return w_load(z, wo_ref, SHIFTED)

        def w_load_other(o):
            return w_load(source(o), wall_ref.at[at_rows(source(o) * qw, qw), :], o)

        def w_stage4(o):
            w_gathered(o)
            for c in w_load_other(o):
                c.start()

        def load_weights(i, ref, lane, n):
            return pltpu.make_async_copy(ref, big.at[0, :, pl.ds(lane, n)], ld_sem.at[i])

        load_q, load_k, load_v, load_s = (load_weights(i, *args) for i, args in enumerate((
            (wq_ref, 0, qw), (wk_ref, qw, kvh * d), (wv_ref, qw + kvh * d, kvh * d), (wsx_ref, s_at, s_cols))))

        def x_start(b, slot):
            for i in range(n_lane):
                pltpu.make_async_copy(x_ref.at[at_rows(b * blk, blk), pl.ds(i * d, d)], kb.at[2 + slot, i], x_sem.at[slot]).start()

        def x_wait(slot):
            pltpu.make_async_copy(kb.at[2 + slot], kb.at[2 + slot], x_sem.at[slot]).wait()

        def v_copy(b):
            return pltpu.make_async_copy(vst, v_ref.at[at_rows(b * blk, blk), :], vst_sem.at[0])

        low_lanes = lax.broadcasted_iota(jnp.int32, (blk, d), 1) < d // 2

        def make_angles(b):
            first = pos_ref[b * blk]
            pos = (lax.broadcasted_iota(jnp.int32, (blk, d), 0) + first).astype(F32)
            angle = pos * freq_ref[...]
            csb[at_rows(b * blk, blk), :] = jnp.where(low_lanes, jnp.cos(angle), jnp.sin(angle))

        def cos_sin(b):
            both = csb[at_rows(b * blk, blk), :]
            turned = pltpu.roll(both, d // 2, axis=1)
            return jnp.where(low_lanes, both, turned), jnp.where(low_lanes, -turned, both)

        x_start(0, 0)
        load_k.start()
        load_v.start()
        load_q.start()

        barrier = pltpu.get_barrier_semaphore()
        for dev in (x_nb, y_nb, c_nb, {"tp": partner}, {"tp": other_mid}, {"tp": other_end}):
            pl.semaphore_signal(barrier, inc=1, device_id=dev, device_id_type=MESH)
        pl.semaphore_wait(barrier, 6)

        @pl.when(middle)
        def _():
            for i in range(len(s_parts)):
                s_copy(i).start()

        z_copy(PARTNER).start()
        z_copy(MID).start()

        @pl.when(middle)
        def _():
            z_copy(END).start()

        seg_at = lambda half, c: jnp.where(half == LOW, c, n_seg - 1 - c) * seg
        y_cp = (1 - cy) * 2 + cc
        c_cp = cy * 2 + 1 - cc
        yc_cp = (1 - cy) * 2 + 1 - cc

        def kv_region(half, c, which, slot):
            at = pl.multiple_of(seg_at(half, c), seg)
            h = head_at(slot)
            return kb.at[h, pl.ds(at // blk, seg // blk)] if which == 0 else vb.at[h, :, pl.ds(at, seg)]

        TO_CORE, TO_Y, Y_TO_CORE = kv_kinds = range(3)
        kv_both = range(2)
        n_kv = len(kv_both) * len(SLOTS)
        kv_at = lambda half, which, slot: half * n_kv + which * len(SLOTS) + slot

        def kv_send(kind, half, which, slot):
            region = kv_region(half, y_cp if kind == Y_TO_CORE else cp, which, slot)
            i = kv_at(half, which, slot)
            return remote(region, region, kv_s.at[kind, i], kv_r.at[kind, i], y_nb if kind == TO_Y else c_nb)

        def for_slots(slots, f):
            for slot in slots:
                if slot == FIRST:
                    f(slot)
                else:
                    @pl.when(end)
                    def _():
                        f(slot)

        own = (FIRST, SECOND)
        moved = (MOVED,)

        def kv_start(half, slots):
            def f(slot):
                for which in kv_both:
                    kv_send(TO_Y, half, which, slot).start()
                    kv_send(TO_CORE, half, which, slot).start()
            for_slots(slots, f)

        def kv_relay(half, slots):
            def f(slot):
                for which in kv_both:
                    got(kv_region(half, y_cp, which, slot), kv_r.at[TO_Y, kv_at(half, which, slot)])
                    kv_send(Y_TO_CORE, half, which, slot).start()
            for_slots(slots, f)

        def kv_arrived(half, slots):
            def f(slot):
                for which in kv_both:
                    i = kv_at(half, which, slot)
                    got(kv_region(half, c_cp, which, slot), kv_r.at[TO_CORE, i])
                    got(kv_region(half, yc_cp, which, slot), kv_r.at[Y_TO_CORE, i])
            for_slots(slots, f)

        def kv_sent():
            def f(slot):
                for half in (LOW, HIGH):
                    for which in kv_both:
                        for kind in kv_kinds:
                            kv_send(kind, half, which, slot).wait_send()
            for_slots(SLOTS, f)

        def k_copy(half, hh):
            at = pl.multiple_of(seg_at(half, cp), seg)
            n = seg // blk
            return pltpu.make_async_copy(kb.at[hh, pl.ds(at // blk, n)], k_ref.at[pl.ds(half * n, n), :, pl.ds(hh * d, d)], kout_sem.at[half, hh])

        def h_rows(b):
            h0 = big[1, at_rows(b * blk, blk), :]
            h1 = big[1, at_rows(rows + b * blk, blk), :]
            return jnp.concatenate([h0, h1], axis=1)

        load_k.wait()
        load_v.wait()

        half_blk = n_blk // 2

        def at_half_end(b, f):
            for half in (LOW, HIGH):
                @pl.when(b == half * half_blk + half_blk - 1)
                def _():
                    f(half)

        def kv_rows(b):
            return pl.multiple_of(seg_at(b // half_blk, cp) + lax.rem(b, half_blk) * blk, blk)

        def kv_block(b):
            slot = b % 2
            x_wait(slot)

            @pl.when(b + 1 < n_blk)
            def _():
                x_start(b + 1, 1 - slot)

            def norm_rows(i):
                at = at_rows(i * nr, nr)
                square = 0.0
                for j in range(n_lane):
                    xf = kb[2 + slot, j, at, :].astype(F32)
                    square = square + xf * xf
                inv = lax.rsqrt(jnp.sum(square, axis=-1, keepdims=True) / width + NORM_EPS)
                for j in range(n_lane):
                    xf = kb[2 + slot, j, at, :].astype(F32)
                    h = ((xf * inv) * gain_ref[j:j + 1, :].astype(F32)).astype(BF16)
                    row = b * blk + (0 if j * d < half_w else rows) + i * nr
                    lane = (j * d) % half_w
                    big[1, at_rows(row, nr), lane:lane + d] = h

            repeat(blk // nr, norm_rows)
            make_angles(b)
            kv = jnp.dot(h_rows(b), big[0, :, qw:qw + 2 * kvh * d], preferred_element_type=F32).astype(BF16)
            cos, sin = cos_sin(b)
            at = kv_rows(b)

            @pl.when(b > 0)
            def _():
                v_copy(b - 1).wait()

            for hh in range(kvh):
                kb[hh, at // blk] = rotate(kv[:, hh * d:(hh + 1) * d], cos, sin)
                vb[hh, :, pl.ds(at, blk)] = kv[:, (kvh + hh) * d:(kvh + hh + 1) * d].T
            vst[...] = kv[:, kvh * d:]
            v_copy(b).start()

            def send(half):
                kv_start(half, own)
                for hh in range(kvh):
                    k_copy(half, hh).start()

            at_half_end(b, send)

        repeat(n_blk, kv_block)
        v_copy(n_blk - 1).wait()
        load_q.wait()

        @pl.when(end)
        def _():
            w_stage1(SHIFTED)

        def q_half(half):
            def q_block(b):
                cos, sin = cos_sin(b)

                def project(i):
                    head = head_at(i)
                    q = jnp.dot(h_rows(b), big[0, :, at_rows(head * gw, gw)], preferred_element_type=F32).astype(BF16)
                    for j in range(group):
                        qb[head * group + j, at_rows(b * blk, blk), :] = rotate(q[:, j * d:(j + 1) * d], cos, sin)

                repeat(jnp.where(middle, 1, kvh), project)

            repeat(half_blk, q_block, half * half_blk)

        def moved_block(b):
            cos, sin = cos_sin(b)
            qkv = jnp.dot(h_rows(b), big[0, :, s_at:s_at + s_cols], preferred_element_type=F32).astype(BF16)
            for j in range(group):
                qb[MOVED * group + j, at_rows(b * blk, blk), :] = rotate(qkv[:, j * d:(j + 1) * d], cos, sin)
            at = kv_rows(b)
            kb[MOVED, at // blk] = rotate(qkv[:, gw:gw + d], cos, sin)
            vb[MOVED, :, pl.ds(at, blk)] = qkv[:, gw + d:].T
            at_half_end(b, lambda half: kv_start(half, moved))

        def o_region(g, rb):
            return oall_ref.at[pl.ds(g * group, group), at_rows(rb * blk, blk), :]

        def o_own(slot, rb):
            return qb.at[pl.ds(head_at(slot) * group, group), at_rows(rb * blk, blk), :]

        def o_local(slot, rb):
            return pltpu.make_async_copy(o_own(slot, rb), o_region(group_of(z, slot), rb), o_l.at[rb, slot])

        def o_send(to, slot, rb):
            g = group_of(z, slot)
            return remote(o_own(slot, rb), o_region(g, rb), o_s.at[to, rb, slot], o_r.at[rb, g], {"tp": source(to)})

        others = ((MID, FIRST), (END, FIRST), (END, SECOND), (END, MOVED))
        ends_own = ((PARTNER, FIRST), (PARTNER, SECOND), (PARTNER, MOVED))
        passed = others + ends_own

        def o_pass(what, rb):
            g = group_of(source(what[0]), what[1])
            region = o_region(g, rb)
            to = {"tp": partner if what in others else other_mid}
            return remote(region, region, f_s.at[rb, passed.index(what)], o_r.at[rb, g], to)

        def o_wait(what, rb):
            g = group_of(source(what[0]), what[1])
            got(o_region(g, rb), o_r.at[rb, g])

        def pass_on(what, blocks):
            def step(rb):
                for item in what:
                    o_wait(item, rb)
                    o_pass(item, rb).start()

            repeat(len(blocks), step, blocks[0])

        def own_outward(blocks):
            repeat(len(blocks), lambda rb: o_send(PARTNER, FIRST, rb).start(), blocks[0])

        scores = (s_a, s_b)
        accs = (acc_a, acc_b)

        def unit(half, c, slot):
            hl = head_at(slot)
            r0 = pl.multiple_of(half * seg + c * unit_rows, unit_rows)
            g0 = seg_at(half, cp) + c * unit_rows
            for st in range(2):
                for j in range(group):
                    qs = qb[hl * group + j, pl.ds(r0 + st * bq, bq), :].T.astype(F32) * SCALE2
                    top = qs.astype(BF16)
                    span = slice(j * bq, (j + 1) * bq)
                    qt[st, 0:d, span] = top
                    qt[st, d:2 * d, span] = (qs - top.astype(F32)).astype(BF16)
            k_idx = lax.broadcasted_iota(jnp.int32, (bk, cols), 0)
            q_idx = lax.broadcasted_iota(jnp.int32, (bk, cols), 1) % bq

            def qk(st, t, mask=None):
                kt = kb[hl, pl.ds(t * (bk // blk), bk // blk)].reshape(bk, d)
                s = jnp.dot(jnp.concatenate([kt, kt], axis=1), qt[st], preferred_element_type=F32)
                if mask is not None:
                    s = jnp.where(mask, s, NEG)
                scores[st][...] = s
                m_tile[st] = jnp.max(s, axis=0, keepdims=True)

            def soft(st, t):
                m_old = m_run[st]
                m_new = jnp.maximum(m_old, m_tile[st])
                m_run[st] = m_new
                alpha = jnp.exp2(m_old - m_new)
                total, pv = 0.0, 0.0
                for i in range(bk // bp):
                    p = jnp.exp2(scores[st][i * bp:(i + 1) * bp, :] - m_new)
                    total = total + jnp.sum(p, axis=0, keepdims=True)
                    v = vb[hl, :, at_rows(t * bk + i * bp, bp)]
                    pv = pv + jnp.dot(v, p.astype(BF16), preferred_element_type=F32)
                l_run[st] = l_run[st] * alpha + total
                accs[st][...] = accs[st][...] * alpha + pv

            m_run[...] = jnp.full_like(m_run, NEG)
            l_run[...] = jnp.zeros_like(l_run)
            acc_a[...] = jnp.zeros_like(acc_a)
            acc_b[...] = jnp.zeros_like(acc_b)
            n_full = g0 // bk

            qk(0, 0, k_idx <= q_idx + g0)

            def body(t):
                qk(1, t)
                soft(0, t)
                qk(0, t + 1)
                soft(1, t)

            repeat(n_full - 1, body)

            def finish_unit(tail):
                if tail:
                    qk(1, n_full - 1)
                    soft(0, n_full - 1)
                    qk(0, n_full, k_idx <= q_idx)
                    soft(1, n_full - 1)
                qk(1, n_full, k_idx <= q_idx + bq)
                soft(0, n_full)
                soft(1, n_full)
                for st in range(2):
                    o = accs[st][...] * (1.0 / l_run[st])
                    for j in range(group):
                        qb[hl * group + j, pl.ds(r0 + st * bq, bq), :] = o[:, j * bq:(j + 1) * bq].T.astype(BF16)

            @pl.when(n_full > 0)
            def _():
                finish_unit(True)

            @pl.when(n_full == 0)
            def _():
                finish_unit(False)

            for st in range(2):
                rb = half * half_blk + c * 2 + st

                @pl.when(middle)
                def _():
                    o_send(MID, slot, rb).start()

                @pl.when(end | (half == LOW))
                def _():
                    o_send(PARTNER, slot, rb).start()

                o_local(slot, rb).start()

        q_half(LOW)
        kv_relay(LOW, own)
        kv_arrived(LOW, own)

        def when_cp(which, f):
            @pl.when(which)
            def _():
                f()

        def nothing():
            pass

        def start_all(copies):
            for c in copies:
                c.start()

        def second_half():
            when_cp(cp > 0, lambda: kv_relay(HIGH, own))
            when_cp(cp == 3, lambda: w_stage2(SHIFTED))
            q_half(HIGH)
            when_cp(cp == 0, lambda: kv_relay(HIGH, own))
            kv_arrived(HIGH, own)
            when_cp(cp == 2, lambda: w_stage2(SHIFTED))
            when_cp(cp >= 2, lambda: w_stage1(PARTNER))

        def moved_head():
            w_gathered(SHIFTED)
            load_s.start()
            load_s.wait()
            repeat(n_blk, moved_block)
            start_all(w_load_own())
            when_cp(cp >= 2, lambda: w_stage2(PARTNER))
            w_stage1(END)

        def after_e():
            when_cp(cp < 2, lambda: w_stage2(SHIFTED))
            when_cp(cp == 3, lambda: w_stage3(SHIFTED))
            w_stage1(MID)

        def after_f():
            when_cp(cp < 3, lambda: w_stage3(SHIFTED))
            when_cp(cp < 2, lambda: w_stage2(PARTNER))

        def after_g():
            kv_relay(LOW, moved)
            w_stage2(MID)
            kv_arrived(LOW, moved)

        def after_h():
            kv_relay(HIGH, moved)

        def after_i():
            kv_arrived(HIGH, moved)

        def after_j():
            w_stage3(PARTNER)
            w_stage2(END)

        def after_k():
            w_stage3(MID)
            w_stage3(END)
            w_stage4(PARTNER)
            w_stage4(MID)

        def after_l():
            w_stage4(END)

        end_units = (
            (LOW, TOP, FIRST, nothing, nothing),
            (LOW, TOP, SECOND, nothing, nothing),
            (LOW, BOTTOM, FIRST, nothing, nothing),
            (LOW, BOTTOM, SECOND, nothing, lambda: when_cp(cp < 2, lambda: w_stage1(PARTNER))),
            (HIGH, TOP, FIRST, second_half, after_e),
            (HIGH, TOP, SECOND, nothing, after_f),
            (HIGH, BOTTOM, FIRST, moved_head, after_g),
            (LOW, TOP, MOVED, nothing, after_h),
            (LOW, BOTTOM, MOVED, nothing, after_i),
            (HIGH, TOP, MOVED, nothing, after_j),
            (HIGH, BOTTOM, SECOND, nothing, after_k),
            (HIGH, BOTTOM, MOVED, nothing, after_l),
        )

        low_blocks, high_blocks = range(half_blk), range(half_blk, n_blk)
        top = lambda blocks: blocks[:half_blk // 2]
        bottom = lambda blocks: blocks[half_blk // 2:]
        mids, end_first, end_both, end_moved = others[:1], others[1:2], others[1:3], others[3:]
        own_both, own_moved = ends_own[:2], ends_own[2:]

        def middle_high():
            got(here(END), wz_r.at[END])
            z_forward().start()
            kv_relay(HIGH, own)
            q_half(HIGH)
            kv_arrived(HIGH, own)
            start_all(w_load_own())
            for o in (PARTNER, MID, END):
                w_stage1(o)

        middle_units = (
            (LOW, TOP, FIRST, nothing, nothing),
            (LOW, BOTTOM, FIRST, nothing, nothing),
            (HIGH, TOP, FIRST, middle_high, lambda: pass_on(own_both, top(low_blocks))),
            (HIGH, BOTTOM, FIRST, nothing, nothing),
        )

        def unit_loop(s):
            half, c, slot = (
                jnp.where(middle, pick(s, [u[i] for u in middle_units]), pick(s, [u[i] for u in end_units])) for i in range(3))

            def events(i):
                for role, units in ((middle, middle_units), (end, end_units)):
                    for step, what in enumerate(units):
                        if what[i] is not nothing:
                            @pl.when(role & (s == step))
                            def _():
                                what[i]()

            events(-2)
            unit(half, c, slot)
            events(-1)

        repeat(jnp.where(middle, len(middle_units), len(end_units)), unit_loop)

        @pl.when(middle)
        def _():
            pass_on(own_both, bottom(low_blocks))
            pass_on(mids, low_blocks)
            w_stage2(PARTNER)
            pass_on(end_both, top(low_blocks))
            own_outward(top(high_blocks))
            w_stage2(MID)
            w_stage2(END)
            w_stage3(PARTNER)
            pass_on(end_both, bottom(low_blocks))
            w_stage3(MID)
            w_stage4(PARTNER)
            w_stage3(END)
            w_stage4(MID)
            pass_on(own_moved, low_blocks)
            w_stage4(END)
            pass_on(end_moved, low_blocks)
            pass_on(own_both, top(high_blocks))
            pass_on(mids, top(high_blocks))

        def middle_0():
            pass_on(own_moved, top(high_blocks))
            pass_on(end_both, top(high_blocks))

        def middle_1():
            pass_on(end_moved, top(high_blocks))
            own_outward(bottom(high_blocks))
            pass_on(mids, bottom(high_blocks))
            pass_on(own_both, bottom(high_blocks))

        def middle_2():
            pass_on(own_moved, bottom(high_blocks))
            pass_on(end_both, bottom(high_blocks))

        middle_events = (middle_0, middle_1, middle_2, lambda: pass_on(end_moved, bottom(high_blocks)))

        kv_sent()
        for half in range(2):
            for hh in range(kvh):
                k_copy(half, hh).wait()

        def early_landed(rb):
            for_slots(SLOTS, lambda slot: o_local(slot, rb).wait())

            @pl.when(end)
            def _():
                for what in (ends_own[0], others[0]):
                    o_wait(what, rb)

        def late_landed(rb):
            @pl.when(end)
            def _():
                for what in others[1:]:
                    o_wait(what, rb)

        def ob_copy(rb, slot, first, n, i):
            return pltpu.make_async_copy(
                oall_ref.at[pl.ds(first, n), at_rows(rb * blk, blk), :], kb.at[slot, pl.ds(first, n)], ob_sem.at[slot, i])

        def ob_all(rb, slot):
            return ob_copy(rb, slot, 0, heads, 0)

        def o_fetch(rb, slot):
            early_landed(rb)
            late_landed(rb)
            ob_all(rb, slot).start()

        n_y = width // y_cols
        n_h = half_w // y_cols

        def y_copy(rb, n, slot):
            return pltpu.make_async_copy(yb.at[slot], y_ref.at[at_rows(rb * blk, blk), at_rows(n * y_cols, y_cols)], yb_sem.at[slot])

        def product(slot, first, n_heads, n):
            o = jnp.concatenate([kb[slot, first + i] for i in range(n_heads)], axis=1)
            row = first * d if isinstance(first, int) else pl.multiple_of(first * d, gw)
            w = big[n // n_h, pl.ds(row, n_heads * d), at_rows((n % n_h) * y_cols, y_cols)]
            return jnp.dot(o, w, preferred_element_type=F32)

        def x_cols(slot, n):
            n_in = y_cols // d
            return jnp.concatenate([kb[2 + slot, n * n_in + i] for i in range(n_in)], axis=1).astype(F32)

        x_start(0, 0)
        o_fetch(0, 0)
        for c in sum((w_load_other(o) for o in (PARTNER, MID, END)), w_load_own()):
            c.wait()

        n_full_blocks = n_blk - 2

        def out_block(rb):
            slot = rb % 2
            x_wait(slot)
            ob_all(rb, slot).wait()
            x_start(rb + 1, 1 - slot)

            @pl.when(rb + 1 < n_full_blocks)
            def _():
                o_fetch(rb + 1, 1 - slot)

            def out_cols(n):
                ys = n % 2

                @pl.when(rb * n_y + n >= 2)
                def _():
                    y_copy(rb, n, ys).wait()

                yb[ys] = (x_cols(slot, n) + product(slot, 0, heads, n)).astype(BF16)
                y_copy(rb, n, ys).start()

            repeat(n_y, out_cols)
            for i, event in enumerate(middle_events):
                @pl.when(middle & (rb == i))
                def _():
                    event()

        repeat(n_full_blocks, out_block)

        n_late = len(SLOTS) * group
        n_early = heads - n_late
        early = jnp.where(z < 2, 0, n_late)
        late = jnp.where(z < 2, n_early, 0)
        blocks = (n_full_blocks, n_full_blocks + 1)

        def part(n):
            return (at_rows((n % n_h) // 2 * blk, blk), at_rows(n % 2 * y_cols, y_cols))

        def lanes_of(n, half):
            return at_rows(n * 2 * y_cols + half * y_cols, y_cols)

        def early_sum(slot, n):
            return x_cols(slot, n) + product(slot, early, n_early, n)

        def finish(slot, n, total):
            ys = n % 2
            y_copy(blocks[slot], n, ys).wait()
            yb[ys] = (total + product(slot, late, n_late, n)).astype(BF16)
            y_copy(blocks[slot], n, ys).start()

        early_copies = [ob_copy(rb, slot, early, n_early, 0) for slot, rb in enumerate(blocks)]
        late_copies = [ob_copy(rb, slot, late, n_late, 1) for slot, rb in enumerate(blocks)]
        for slot, rb in enumerate(blocks):
            early_landed(rb)
            if slot > 0:
                x_start(rb, slot)
            early_copies[slot].start()
        for i in range(2):
            if i == 0:
                x_wait(0)
                early_copies[0].wait()

            def first_terms(n):
                scores[i][part(n)] = early_sum(0, n)

            repeat(n_h, first_terms, i * n_h)
        x_wait(1)
        early_copies[1].wait()
        half_rows = blk // 2

        def second_terms(n):
            total = early_sum(1, n)
            for i in range(len(SLOTS)):
                term = total.astype(BF16)
                for half in range(2):
                    vb[i, :, lanes_of(n, half)] = term[half * half_rows:(half + 1) * half_rows]
                total = total - term.astype(F32)

        repeat(n_y, second_terms)
        late_landed(blocks[0])
        late_copies[0].start()
        late_copies[0].wait()
        for i in range(2):
            repeat(n_h, lambda n: finish(0, n, scores[i][part(n)]), i * n_h)
        late_landed(blocks[1])
        late_copies[1].start()
        late_copies[1].wait()

        def last_terms(n):
            terms = [jnp.concatenate([vb[i, :, lanes_of(n, half)] for half in range(2)], axis=0).astype(F32) for i in range(len(SLOTS))]
            finish(1, n, (terms[0] + terms[1]) + terms[2])

        repeat(n_y, last_terms)
        for n in (n_y - 2, n_y - 1):
            y_copy(blocks[1], n, n % 2).wait()

        def drain(rb):
            for_slots(SLOTS, lambda slot: o_send(PARTNER, slot, rb).wait_send())

            @pl.when(middle)
            def _():
                o_send(MID, FIRST, rb).wait_send()
                for what in passed:
                    o_pass(what, rb).wait_send()

        repeat(n_blk, drain)
        z_copy(PARTNER).wait_send()
        z_copy(MID).wait_send()

        @pl.when(middle)
        def _():
            z_copy(END).wait_send()
            z_forward().wait_send()
            for i in range(len(s_parts)):
                s_copy(i).wait_send()

        def w_sent(o):
            for kind in kinds:
                if (kind, o) != (X_TO_Y, SHIFTED):
                    w_send(kind, o).wait_send()
                c_send(kind, o).wait_send()

        for o in (PARTNER, MID, END):
            w_sent(o)

        @pl.when(end)
        def _():
            w_sent(SHIFTED)

    any_spec = pl.BlockSpec(memory_space=pl.ANY)
    vmem_spec = pl.BlockSpec(memory_space=pltpu.VMEM)
    dma = pltpu.SemaphoreType.DMA
    outs = pl.pallas_call(
        kernel,
        in_specs=[any_spec, vmem_spec] + [any_spec] * 4 + [pl.BlockSpec(memory_space=pltpu.SMEM), vmem_spec],
        out_specs=[any_spec] * 6,
        out_shape=[
            jax.ShapeDtypeStruct((rows, width), BF16),
            jax.ShapeDtypeStruct((n_blk, blk, kvh * d), BF16),
            jax.ShapeDtypeStruct((rows, kvh * d), BF16),
            jax.ShapeDtypeStruct((heads, rows, d), BF16),
            jax.ShapeDtypeStruct((width, width), BF16),
            jax.ShapeDtypeStruct((width, s_cols), BF16),
        ],
        scratch_shapes=[
            pltpu.VMEM((2, width, half_w), BF16),
            pltpu.VMEM((4, n_lane, blk, d), BF16),
            pltpu.VMEM((3, d, n_seg * seg), BF16),
            pltpu.VMEM((3 * group, rows, d), BF16),
            pltpu.VMEM((rows, d), F32),
            pltpu.VMEM((blk, kvh * d), BF16),
            pltpu.VMEM((2, 2 * d, cols), BF16),
            pltpu.VMEM((bk, cols), F32),
            pltpu.VMEM((bk, cols), F32),
            pltpu.VMEM((d, cols), F32),
            pltpu.VMEM((d, cols), F32),
            pltpu.VMEM((2, 1, cols), F32),
            pltpu.VMEM((2, 1, cols), F32),
            pltpu.VMEM((2, 1, cols), F32),
            pltpu.VMEM((2, blk, y_cols), BF16),
            dma((4,)), dma((2,)), dma((1,)), dma((2, kvh)),
            dma((3, 12)), dma((3, 12)), dma((4,)), dma((3,)), dma((3,)), dma((3,)), dma((4, 4)), dma((4, 4)), dma((4, 4)), dma((4, 4)),
            dma((2, n_blk, 3)), dma((n_blk, 3)), dma((n_blk, n_groups)), dma((n_blk, 7)), dma((2, 2)), dma((2,)), dma((4, 2)),
        ],
        compiler_params=pltpu.CompilerParams(collective_id=0, has_side_effects=True, vmem_limit_bytes=67043328),
        name="sublayer",
    )(x, gain, w_q, w_k, w_v, w_o, positions, freqs)
    return outs[:3]


def results(y):
    rows, width = y.shape
    n = 8
    blk = rows // n

    def kernel(y_in, y_out, buf, sems):
        def copy_in(i):
            return pltpu.make_async_copy(y_in.at[pl.ds(i * blk, blk), :], buf.at[pl.ds(i * blk, blk), :], sems.at[0, i])

        def copy_out(i):
            return pltpu.make_async_copy(buf.at[pl.ds(i * blk, blk), :], y_out.at[pl.ds(i * blk, blk), :], sems.at[1, i])

        for i in range(n):
            copy_in(i).start()
        for i in range(n):
            copy_in(i).wait()
            copy_out(i).start()
        for i in range(n):
            copy_out(i).wait()

    any_spec = pl.BlockSpec(memory_space=pl.ANY)
    return pl.pallas_call(
        kernel,
        in_specs=[any_spec],
        out_specs=any_spec,
        out_shape=jax.ShapeDtypeStruct(y.shape, BF16),
        scratch_shapes=[pltpu.VMEM(y.shape, BF16), pltpu.SemaphoreType.DMA((2, n))],
        compiler_params=pltpu.CompilerParams(vmem_limit_bytes=60 * 2 ** 20),
        name="results",
    )(y)


def solution(mesh):
    def device_fn(x_in, positions, norm_gain, w_q, w_k, w_v, w_o):
        kv_heads = w_k.shape[1] // HEAD_DIM
        freqs = rope_freqs()
        freqs = jnp.concatenate([freqs, freqs])[None, :]
        gain = norm_gain.reshape(-1, HEAD_DIM)
        y, keys, values = layer(x_in, gain, w_q, w_k, w_v, w_o, positions, freqs)
        shape = (x_in.shape[0], kv_heads, HEAD_DIM)
        return results(y), keys.reshape(shape), values.reshape(shape)

    row_spec = P(('dp', 'cp'), None)
    cache_spec = P(('dp', 'cp'), 'tp', None)
    return jax.shard_map(device_fn, mesh=mesh, in_specs=(row_spec, P(('dp', 'cp')), P(None), P(None, 'tp'), P(None, 'tp'), P(None, 'tp'), P('tp', None)), out_specs=(row_spec, cache_spec, cache_spec), check_vma=False)
```
